32 devices in a mesh: seq: 8 (over z, x), batch: 4 (over y, core).
Axes of the slice: x: 2, y: 2, z: 4, core: 2. Of those that a mesh axis runs over, the one named last changes fastest.
Arguments:
- inputs: bfloat16 [4, 4096, 1024], P('batch', 'seq'), may hold values from -6 to 6
- w_key: bfloat16 [1024, 1024], replicated, may hold values from -0.1875 to 0.1875
- w_value: bfloat16 [1024, 1024], replicated, may hold values from -0.1875 to 0.1875
- w_recept: bfloat16 [1024, 1024], replicated, may hold values from -0.1875 to 0.1875
- w_output: bfloat16 [1024, 1024], replicated, may hold values from -2 to 2
- w_ffn_key: bfloat16 [1024, 4096], replicated, may hold values from -0.1875 to 0.1875
- w_ffn_value: bfloat16 [4096, 1024], replicated, may hold values from -0.09375 to 0.09375
- w_ffn_recept: bfloat16 [1024, 1024], replicated, may hold values from -0.1875 to 0.1875
- ln1_gain: float32 [1024], replicated, may hold values from 0.5 to 1.5
- ln1_bias: float32 [1024], replicated, may hold values from -0.5 to 0.5
- mix_key: float32 [1024], replicated, may hold values from 0 to 1
- mix_value: float32 [1024], replicated, may hold values from 0 to 1
- mix_recept: float32 [1024], replicated, may hold values from 0 to 1
- time_decay: float32 [1024], replicated, as said below
- time_first: float32 [1024], replicated, may hold values from -1 to 1
- ln2_gain: float32 [1024], replicated, may hold values from 0.5 to 1.5
- ln2_bias: float32 [1024], replicated, may hold values from -0.5 to 0.5
- ffn_mix_key: float32 [1024], replicated, may hold values from 0 to 1
- ffn_mix_recept: float32 [1024], replicated, may hold values from 0 to 1
- state_num: float32 [1024, 4], P(None, 'batch'), may hold values from -8 to 8
- state_den: float32 [1024, 4], P(None, 'batch'), may hold values from 1 to 8
- state_max: float32 [1024, 4], P(None, 'batch'), may hold values from 0 to 2
- prev_att: float32 [1024, 4], P(None, 'batch'), may hold values from -6 to 6
- prev_ffn: float32 [1024, 4], P(None, 'batch'), may hold values from -6 to 6
- cotangent: bfloat16 [4, 4096, 1024], P('batch', 'seq'), may hold values from -6 to 6
Outputs:
- block_out: bfloat16 [4, 4096, 1024], P('batch', 'seq')
- input_grad: bfloat16 [4, 4096, 1024], P('batch', 'seq')
- grad_w_key: float32 [1024, 1024], P('seq', 'batch')
- grad_w_value: float32 [1024, 1024], P('seq', 'batch')
- grad_w_recept: float32 [1024, 1024], P('seq', 'batch')
- grad_w_output: float32 [1024, 1024], P('seq', 'batch')
- grad_w_ffn_key: float32 [1024, 4096], P('seq', 'batch')
- grad_w_ffn_value: float32 [4096, 1024], P('seq', 'batch')
- grad_w_ffn_recept: float32 [1024, 1024], P('seq', 'batch')
- grad_ln1_gain: float32 [1024], P('seq')
- grad_ln1_bias: float32 [1024], P('seq')
- grad_mix_key: float32 [1024], P('seq')
- grad_mix_value: float32 [1024], P('seq')
- grad_mix_recept: float32 [1024], P('seq')
- grad_time_decay: float32 [1024], P('seq')
- grad_time_first: float32 [1024], P('seq')
- grad_ln2_gain: float32 [1024], P('seq')
- grad_ln2_bias: float32 [1024], P('seq')
- grad_ffn_mix_key: float32 [1024], P('seq')
- grad_ffn_mix_recept: float32 [1024], P('seq')
- grad_state_num: float32 [1024, 4], P('seq', 'batch')
- grad_state_den: float32 [1024, 4], P('seq', 'batch')
- grad_state_max: float32 [1024, 4], P('seq', 'batch')
- grad_prev_att: float32 [1024, 4], P('seq', 'batch')
- grad_prev_ffn: float32 [1024, 4], P('seq', 'batch')
The draws below stay inside these ranges and needn't reach their ends.
Inputs may be any that keep to these rules, and one draw needn't show every extreme that they name: exp(time_decay) is at most 0.05 in every channel.
All inputs are finite; a program needn't handle non-finite values.
Results may differ from the reference program's by a relative error of at most 0.0095.
Values sent between devices are 32-bit elements; how exact they have to be, the bound alone decides.
A program may use at most 192 MiB of HBM per device.

```python
import math
import jax
import jax.numpy as jnp
from jax import lax

D = 1024
FF = 4096
STRETCH = 512
BLOCK = 64
SEGS = 4
LEN = 4096


def draw_time_decay(key, part):
    pick_key, slow_key, fast_key = jax.random.split(key, 3)
    chain = float(LEN)
    piece = float(STRETCH)
    fast_share = 0.4
    slow_top = 2.0 / piece
    fast_pick = jax.random.uniform(pick_key, (D,), dtype=jnp.float32) < fast_share
    slow_log = jax.random.uniform(slow_key, (D,), dtype=jnp.float32, minval=math.log(0.5 / chain), maxval=math.log(slow_top))
    fast_log = jax.random.uniform(fast_key, (D,), dtype=jnp.float32, minval=math.log(0.02), maxval=math.log(0.05))
    return jnp.where(fast_pick, fast_log, slow_log).astype(jnp.float32)


def block_levels(key, shape, pieces, smallest, top_value):
    loudness = 1.0
    for dim, shards_of in pieces:
        draws = jax.random.uniform(jax.random.fold_in(jax.random.fold_in(key, 6), dim), (shards_of,), jnp.float32, smallest / len(pieces), top_value / len(pieces))
        loudness = loudness * jnp.repeat(jnp.exp(draws), shape[dim] // shards_of).reshape((-1,) + (1,) * (len(shape) - 1 - dim))
    return loudness


def noise(stream_key, dims, deviation, limit, cuts=(), held_as=jnp.bfloat16):
    values = jax.random.normal(stream_key, dims, jnp.float32) * deviation
    if len(cuts) > 0:
        values = block_levels(stream_key, dims, cuts, -0.22, 0.18) * values
    return jnp.clip(values, min=-limit, max=limit).astype(held_as)


def setup_inputs(seed: int = 0) -> dict:
    splits = jax.random.split(jax.random.key(seed), 26)
    return {
        "inputs": noise(splits[0], (SEGS, LEN, D), 1.0, 6.0, ((0, 4), (1, 8))),
        "w_key": noise(splits[1], (D, D), D ** -0.5, 0.1875),
        "w_value": noise(splits[2], (D, D), D ** -0.5, 0.1875),
        "w_recept": noise(splits[3], (D, D), D ** -0.5, 0.1875),
        "w_output": noise(splits[4], (D, D), 8 ** -0.5, 2.0),
        "w_ffn_key": noise(splits[5], (D, FF), D ** -0.5, 0.1875),
        "w_ffn_value": noise(splits[6], (FF, D), FF ** -0.5, 0.09375),
        "w_ffn_recept": noise(splits[7], (D, D), D ** -0.5, 0.1875),
        "ln1_gain": jnp.clip(1.0 + 0.1 * jax.random.normal(splits[8], (D,), jnp.float32), 0.5, 1.5),
        "ln1_bias": jnp.clip(jax.random.uniform(splits[9], (D,), jnp.float32, -0.5, 0.5), -0.5, 0.5),
        "mix_key": jnp.clip(jax.random.uniform(splits[10], (D,), jnp.float32, 0.0, 1.0), 0.0, 1.0),
        "mix_value": jnp.clip(jax.random.uniform(splits[11], (D,), jnp.float32, 0.0, 1.0), 0.0, 1.0),
        "mix_recept": jnp.clip(jax.random.uniform(splits[12], (D,), jnp.float32, 0.0, 1.0), 0.0, 1.0),
        "time_decay": draw_time_decay(jax.random.fold_in(splits[25], 71), 0),
        "time_first": jnp.clip(jax.random.uniform(splits[14], (D,), jnp.float32, -1.0, 1.0), -1.0, 1.0),
        "ln2_gain": jnp.clip(1.0 + 0.1 * jax.random.normal(splits[15], (D,), jnp.float32), 0.5, 1.5),
        "ln2_bias": jnp.clip(jax.random.uniform(splits[16], (D,), jnp.float32, -0.5, 0.5), -0.5, 0.5),
        "ffn_mix_key": jnp.clip(jax.random.uniform(splits[17], (D,), jnp.float32, 0.0, 1.0), 0.0, 1.0),
        "ffn_mix_recept": jnp.clip(jax.random.uniform(splits[18], (D,), jnp.float32, 0.0, 1.0), 0.0, 1.0),
        "state_num": noise(splits[19], (D, SEGS), 2.0, 8.0, ((1, 4),), jnp.float32),
        "state_den": jnp.clip(1.0 + 7.0 * jax.random.uniform(splits[20], (D, SEGS), jnp.float32) ** block_levels(splits[20], (D, SEGS), ((1, 4),), -0.2, 0.2), 1.0, 8.0),
        "state_max": jnp.clip(2.0 * jax.random.uniform(splits[21], (D, SEGS), jnp.float32) ** block_levels(splits[21], (D, SEGS), ((1, 4),), -0.2, 0.2), 0.0, 2.0),
        "prev_att": noise(splits[22], (D, SEGS), 1.0, 6.0, ((1, 4),), jnp.float32),
        "prev_ffn": noise(splits[23], (D, SEGS), 1.0, 6.0, ((1, 4),), jnp.float32),
        "cotangent": noise(splits[24], (SEGS, LEN, D), 1.0, 6.0, ((0, 4), (1, 8))),
    }


highest = lax.Precision.HIGHEST

@jax.custom_vjp
def low(v):
    return lax.optimization_barrier(v.astype(jnp.bfloat16)).astype(jnp.float32)

@jax.custom_vjp
def low_back(v):
    return v

def low_keep(v):
    return (low(v), None)

def low_pass(kept, grad):
    return (grad,)

def back_keep(v):
    return (v, None)

def back_low(kept, grad):
    return (low(grad),)
low.defvjp(low_keep, low_pass)
low_back.defvjp(back_keep, back_low)

def layer_norm(values, ln_gain, ln_bias):
    centred = values - lax.optimization_barrier(jnp.mean(values, axis=-1, keepdims=True))
    spread = lax.optimization_barrier(jnp.mean(centred * centred, axis=-1, keepdims=True))
    return centred * lax.rsqrt(spread + 1e-05) * ln_gain + ln_bias

def matmul(operand, matrix):
    return jnp.dot(operand, matrix, precision=highest, preferred_element_type=jnp.float32)

def shifted(normed, edge_row):
    return jnp.concatenate([edge_row[None, :], normed[:-1]], axis=0)

def wkv_tokens(key_rows, value_rows, decay_rate, time_first, start_state):

    def token_step(state_in, inputs_now):
        numerator, denominator, running_max = state_in
        key_now, value_now = inputs_now
        current = time_first + key_now
        highest_now = jnp.maximum(running_max, current)
        weight_old = jnp.exp(running_max - highest_now)
        weight_new = jnp.exp(current - highest_now)
        mixed_now = (weight_old * numerator + weight_new * value_now) / (weight_old * denominator + weight_new)
        decayed = running_max + decay_rate
        highest_next = jnp.maximum(decayed, key_now)
        weight_old = jnp.exp(decayed - highest_next)
        weight_new = jnp.exp(key_now - highest_next)
        new_state = (weight_old * numerator + weight_new * value_now, weight_old * denominator + weight_new, highest_next)
        return (new_state, mixed_now)

    def block_step(state_in, inputs_now):
        return lax.scan(token_step, state_in, inputs_now)
    blocks = key_rows.shape[0] // BLOCK
    shaped = (key_rows.reshape(blocks, BLOCK, key_rows.shape[1]), value_rows.reshape(blocks, BLOCK, value_rows.shape[1]))
    final_state, mixed_rows = lax.scan(jax.checkpoint(block_step), start_state, shaped)
    return mixed_rows.reshape(key_rows.shape)

def forward(rows_in, matrix_set, vector_set, start_set):
    w_key, w_value, w_recept, w_output, w_ffn_key, w_ffn_value, w_ffn_recept = matrix_set
    ln1_gain, ln1_bias, mix_key, mix_value, mix_recept, time_decay, time_first, ln2_gain, ln2_bias, ffn_mix_key, ffn_mix_recept = vector_set
    start_num, start_den, start_max, edge_att, edge_ffn = start_set
    normed = layer_norm(rows_in, ln1_gain, ln1_bias)
    before = shifted(normed, edge_att)
    key_in = low(normed * mix_key + before * (1.0 - mix_key))
    value_in = low(normed * mix_value + before * (1.0 - mix_value))
    recept_in = low(normed * mix_recept + before * (1.0 - mix_recept))
    key_rows = low_back(matmul(key_in, w_key))
    value_rows = low_back(matmul(value_in, w_value))
    recept_rows = low_back(matmul(recept_in, w_recept))
    mixed_rows = wkv_tokens(key_rows, value_rows, -jnp.exp(time_decay), time_first, (start_num, start_den, start_max))
    gated = low(jax.nn.sigmoid(recept_rows) * mixed_rows)
    attended = low_back(matmul(gated, w_output))
    middle = rows_in + attended
    normed_ffn = layer_norm(middle, ln2_gain, ln2_bias)
    before_ffn = shifted(normed_ffn, edge_ffn)
    ffn_key_in = low(normed_ffn * ffn_mix_key + before_ffn * (1.0 - ffn_mix_key))
    ffn_recept_in = low(normed_ffn * ffn_mix_recept + before_ffn * (1.0 - ffn_mix_recept))
    hidden_pre = low_back(matmul(ffn_key_in, w_ffn_key))
    hidden = low(jnp.square(jax.nn.relu(hidden_pre)))
    ffn_values = low_back(matmul(hidden, w_ffn_value))
    gate_pre = low_back(matmul(ffn_recept_in, w_ffn_recept))
    return middle + jax.nn.sigmoid(gate_pre) * ffn_values

def reference(inputs, w_key, w_value, w_recept, w_output, w_ffn_key, w_ffn_value, w_ffn_recept, ln1_gain, ln1_bias, mix_key, mix_value, mix_recept, time_decay, time_first, ln2_gain, ln2_bias, ffn_mix_key, ffn_mix_recept, state_num, state_den, state_max, prev_att, prev_ffn, cotangent):
    matrices = (w_key.astype(jnp.float32), w_value.astype(jnp.float32), w_recept.astype(jnp.float32), w_output.astype(jnp.float32), w_ffn_key.astype(jnp.float32), w_ffn_value.astype(jnp.float32), w_ffn_recept.astype(jnp.float32))
    vectors = (ln1_gain, ln1_bias, mix_key, mix_value, mix_recept, time_decay, time_first, ln2_gain, ln2_bias, ffn_mix_key, ffn_mix_recept)
    starts = (state_num.T, state_den.T, state_max.T, prev_att.T, prev_ffn.T)

    def segment_step(totals, segment):
        seg_rows, grad_rows, start_num, start_den, start_max, edge_att, edge_ffn = segment
        result, pullback = jax.vjp(forward, seg_rows.astype(jnp.float32), matrices, vectors, (start_num, start_den, start_max, edge_att, edge_ffn))
        grad_in, grad_matrices, grad_vectors, grad_starts = pullback(grad_rows.astype(jnp.float32))
        totals = jax.tree.map(jnp.add, totals, (grad_matrices, grad_vectors))
        return (totals, (result.astype(jnp.bfloat16), grad_in.astype(jnp.bfloat16), grad_starts))
    initial_sums = jax.tree.map(jnp.zeros_like, (matrices, vectors))
    totals, per_segment = lax.scan(segment_step, initial_sums, (inputs, cotangent) + starts)
    grad_matrices, grad_vectors = totals
    block_out, input_grad, grad_starts = per_segment
    return (block_out, input_grad, grad_matrices[0], grad_matrices[1], grad_matrices[2], grad_matrices[3], grad_matrices[4], grad_matrices[5], grad_matrices[6], grad_vectors[0], grad_vectors[1], grad_vectors[2], grad_vectors[3], grad_vectors[4], grad_vectors[5], grad_vectors[6], grad_vectors[7], grad_vectors[8], grad_vectors[9], grad_vectors[10], grad_starts[0].T, grad_starts[1].T, grad_starts[2].T, grad_starts[3].T, grad_starts[4].T)
```

```python
import functools
from functools import partial

import jax
import jax.numpy as jnp
from jax import lax
from jax.experimental import pallas as pl
from jax.experimental.pallas import tpu as pltpu
from jax.sharding import PartitionSpec as P

MESH = pl.DeviceIdType.MESH
F32 = jnp.float32
BF = jnp.bfloat16


def contract0(a, b):
    return lax.dot_general(a, b, (((0,), (0,)), ((), ())), preferred_element_type=F32)


class Place:
    def __init__(self, nz, nx, ny):
        s, b = lax.axis_index("seq"), lax.axis_index("batch")
        self.nz, self.nx, self.ny = nz, nx, ny
        self.z, self.x = s // nx, s % nx
        self.y, self.c = b // 2, b % 2

    def at(self, z=None, x=None, y=None, c=None):
        z = self.z if z is None else z
        x = self.x if x is None else x
        y = self.y if y is None else y
        c = self.c if c is None else c
        return (z * self.nx + x, y * 2 + c)


NZ = 4
LAG = 4
SLOTF = 8


def rs_kernel(nm, *refs):
    lhs = refs[:7]
    rhs = refs[7:14]
    sm_in = refs[14]
    outs = refs[15:22]
    sm_out = refs[22]
    (lbuf, rbuf, acc, sbuf, rF, rS, rZ, smb, smr, lsem, rsem, s0s, s0r, sFs, sFr, sSs, sSr, sZs, sZr, osem, msem, mss, msr) = refs[23:]
    nk = 2 * nm
    me = Place(NZ, 2, 2)
    z, x, y, c = me.z, me.x, me.y, me.c

    bar = pltpu.get_barrier_semaphore()

    def sig(dev):
        pl.semaphore_signal(bar, inc=1, device_id=dev, device_id_type=MESH)

    sig(me.at(c=1 - c))
    sig(me.at(x=1 - x))
    sig(me.at(y=1 - y))

    @pl.when(z > 0)
    def _():
        sig(me.at(z=z - 1))

    @pl.when(z < NZ - 1)
    def _():
        sig(me.at(z=z + 1))

    def fs(h):
        f = jnp.where(h == 0, x, y)
        s = jnp.where(h == 0, y, x)
        return f, s

    def partnerF(h):
        a, b = me.at(x=1 - x), me.at(y=1 - y)
        return (jnp.where(h == 0, a[0], b[0]), jnp.where(h == 0, a[1], b[1]))

    def partnerS(h):
        return partnerF(1 - h)

    def rcopy(src, dst, ss, rs, dev):
        return pltpu.make_async_remote_copy(src_ref=src, dst_ref=dst, send_sem=ss, recv_sem=rs, device_id=dev, device_id_type=MESH)

    def copy0(k):
        return rcopy(sbuf.at[lax.rem(k, 3)], acc.at[k], s0s.at[k], s0r.at[k], me.at(c=1 - c))

    def copyF(k):
        h = lax.rem(k, 2)
        f, s = fs(h)
        return rcopy(acc.at[k, 1 - f], rF.at[lax.rem(k, SLOTF)], sFs.at[k], sFr.at[k], partnerF(h))

    def copySA(k):
        h = lax.rem(k, 2)
        f, s = fs(h)
        return rcopy(acc.at[k, f, 1 - s], rS.at[k], sSs.at[k], sSr.at[k], partnerS(h))

    def copySE(k):
        h = lax.rem(k, 2)
        f, s = fs(h)
        return rcopy(acc.at[k, f, 1 - s, z], rS.at[k, 0], sSs.at[k], sSr.at[k], partnerS(h))

    def unit(k, q, late):
        f, s = fs(lax.rem(k, 2))
        if late:
            return acc.at[k, f, s, q]
        return acc.at[k, f, :, q]

    def zbuf(k, slot, late):
        if late:
            return rZ.at[k, slot, 0]
        return rZ.at[k, slot]

    def copyR(k, q, late):
        return rcopy(unit(k, q, late), zbuf(k, q + 1, late), sZs.at[k, q], sZr.at[k, q + 1], me.at(z=z + 1))

    def copyL(k, q, late):
        return rcopy(unit(k, q, late), zbuf(k, q, late), sZs.at[k, q], sZr.at[k, q], me.at(z=z - 1))

    def add_into(dst, src):
        dst[...] = dst[...] + src[...]

    def zadd(k, q, slot, late):
        f, s = fs(lax.rem(k, 2))
        if late:
            add_into(acc.at[k, f, s, q], rZ.at[k, slot, 0])
        else:
            for i in range(2):
                add_into(acc.at[k, f, i, q], rZ.at[k, slot, i])

    def zsub(k, tau, late):
        n = NZ

        @pl.when(z <= tau)
        def _():
            q = n - 1 - tau + z

            @pl.when(z > 0)
            def _():
                copyR(k, q, late).wait_recv()
                zadd(k, q, q + 1, late)

            copyR(k, q, late).start()

        @pl.when(n - 1 - z <= tau)
        def _():
            q = tau - (n - 1 - z)

            @pl.when(z < n - 1)
            def _():
                copyL(k, q, late).wait_recv()
                zadd(k, q, q, late)

            copyL(k, q, late).start()

    def zfin(k, late):
        @pl.when(z > 0)
        def _():
            copyR(k, z, late).wait_recv()
            zadd(k, z, z + 1, late)

        @pl.when(z < NZ - 1)
        def _():
            copyL(k, z, late).wait_recv()
            zadd(k, z, z, late)

    def operands(m, slot):
        return (pltpu.make_async_copy(lhs[0], lbuf.at[slot], lsem.at[slot]),
                pltpu.make_async_copy(rhs[0], rbuf.at[slot], rsem.at[slot]))

    def fetch(m, slot):
        for j in range(4):
            @pl.when(m == j)
            def _(j=j):
                for s in range(8):
                    pltpu.make_async_copy(lhs[5].at[:, pl.ds(s * 512 + j * 128, 128)], lbuf.at[slot, :, pl.ds(s * 128, 128)], lsem.at[slot]).start()
                pltpu.make_async_copy(rhs[5], rbuf.at[slot], rsem.at[slot]).start()

            @pl.when(m == 4 + j)
            def _(j=j):
                for s in range(8):
                    pltpu.make_async_copy(rhs[4].at[:, pl.ds(s * 512 + j * 128, 128)], rbuf.at[slot, :, pl.ds(s * 128, 128)], rsem.at[slot]).start()
                pltpu.make_async_copy(lhs[4], lbuf.at[slot], lsem.at[slot]).start()

        for mm, i in ((8, 6), (9, 3), (10, 2), (11, 1), (12, 0)):
            @pl.when(m == mm)
            def _(i=i):
                pltpu.make_async_copy(lhs[i], lbuf.at[slot], lsem.at[slot]).start()
                pltpu.make_async_copy(rhs[i], rbuf.at[slot], rsem.at[slot]).start()

    def wait_fetch(slot):
        for cp in operands(0, slot):
            cp.wait()

    def columns(slot, h, core):
        parts = []
        for yy in range(2):
            start = pl.multiple_of((2 * yy + core) * 256 + h * 128, 128)
            parts.append(rbuf[slot, :, pl.ds(start, 128)])
        return jnp.concatenate(parts, axis=1)

    def gradient(k, core, write):
        h = lax.rem(k, 2)
        slot = lax.rem(k // 2, 2)
        cols = columns(slot, h, core)

        def group(g, _):
            rows = lbuf[slot, :, pl.ds(pl.multiple_of(g * 512, 512), 512)]
            res = contract0(rows, cols)
            for i in range(4):
                zz, xx = g * 2 + i // 2, i % 2
                for yy in range(2):
                    f = jnp.where(h == 0, xx, yy)
                    s = jnp.where(h == 0, yy, xx)
                    write(f, s, zz, res[i * 128:(i + 1) * 128, yy * 128:(yy + 1) * 128])
            return 0

        lax.fori_loop(0, 2, group, 0)

    def taskP(k):
        slot = lax.rem(k, 3)

        @pl.when(k >= 3)
        def _():
            copy0(k - 3).wait_send()

        def write(f, s, zz, v):
            sbuf[slot, f, s, zz] = v

        gradient(k, 1 - c, write)
        copy0(k).start()

    def task1(k):
        copy0(k).wait_recv()

        def write(f, s, zz, v):
            acc[k, f, s, zz] = acc[k, f, s, zz] + v

        gradient(k, c, write)
        copyF(k).start()

    def is_late(k):
        return lax.rem(k // 2, 3) == 0

    def task2(k):
        copyF(k).wait_recv()
        f, s = fs(lax.rem(k, 2))
        slot = lax.rem(k, SLOTF)

        def body(i, _):
            add_into(acc.at[k, f, i // NZ, lax.rem(i, NZ)], rF.at[slot, i // NZ, lax.rem(i, NZ)])
            return 0

        lax.fori_loop(0, 2 * NZ, body, 0)

        @pl.when(is_late(k))
        def _():
            copySA(k).start()

        @pl.when(jnp.logical_not(is_late(k)))
        def _():
            zsub(k, 0, False)

    def taskSA(k):
        @pl.when(is_late(k))
        def _():
            copySA(k).wait_recv()
            f, s = fs(lax.rem(k, 2))

            def body(i, _):
                add_into(acc.at[k, f, s, i], rS.at[k, i])
                return 0

            lax.fori_loop(0, NZ, body, 0)
            zsub(k, 0, True)

    def taskZA(tau, k):
        @pl.when(is_late(k))
        def _():
            zsub(k, tau, True)

    def taskZE(tau, k):
        @pl.when(jnp.logical_not(is_late(k)))
        def _():
            zsub(k, tau, False)

    def finish(k):
        f, s = fs(lax.rem(k, 2))
        h = lax.rem(k, 2)
        m = k // 2
        src = acc.at[k, f, s, z]
        for j in range(4):
            @pl.when(m == j)
            def _(j=j):
                pltpu.make_async_copy(src, outs[5].at[pl.ds(j * 128, 128), pl.ds(pl.multiple_of(h * 128, 128), 128)], osem.at[k]).start()

            @pl.when(m == 4 + j)
            def _(j=j):
                pltpu.make_async_copy(src, outs[4].at[:, pl.ds(pl.multiple_of(h * 512 + j * 128, 128), 128)], osem.at[k]).start()
        for mm, i in ((8, 6), (9, 3), (10, 2), (11, 1), (12, 0)):
            @pl.when(m == mm)
            def _(i=i):
                pltpu.make_async_copy(src, outs[i].at[:, pl.ds(pl.multiple_of(h * 128, 128), 128)], osem.at[k]).start()

    def taskFinA(k):
        @pl.when(is_late(k))
        def _():
            zfin(k, True)
            finish(k)

    def taskFinE(k):
        @pl.when(jnp.logical_not(is_late(k)))
        def _():
            zfin(k, False)
            copySE(k).start()

    def taskSE(k):
        @pl.when(jnp.logical_not(is_late(k)))
        def _():
            copySE(k).wait_recv()
            f, s = fs(lax.rem(k, 2))
            add_into(acc.at[k, f, s, z], rS.at[k, 0])
            finish(k)

    L = LAG
    stages = [
        (0, taskP),
        (1, task1),
        (1 + L, task2),
        (1 + 2 * L, taskSA),
        (2 + L, functools.partial(taskZE, 1)),
        (3 + L, functools.partial(taskZE, 2)),
        (4 + L, taskFinE),
        (2 + 2 * L, functools.partial(taskZA, 1)),
        (3 + 2 * L, functools.partial(taskZA, 2)),
        (4 + 2 * L, taskFinA),
        (5 + L, taskSE),
    ]
    stages = stages[::-1]
    last = max(lag for lag, _ in stages)

    def sm_copy(step):
        if step == 0:
            return rcopy(smb.at[0], smr.at[0], mss.at[0], msr.at[0], me.at(c=1 - c))
        if step == 1:
            return rcopy(smb.at[0], smr.at[1], mss.at[1], msr.at[1], me.at(y=1 - y))
        return rcopy(smb.at[1, 1 - x], smr.at[2, 0], mss.at[2], msr.at[2], me.at(x=1 - x))

    def sm_z(q, right):
        if right:
            return rcopy(smb.at[1, x, q], smr.at[3, 0, q], mss.at[3 + q], msr.at[3 + q], me.at(z=z + 1))
        return rcopy(smb.at[1, x, q], smr.at[3, 1, q], mss.at[3 + q], msr.at[3 + NZ + q], me.at(z=z - 1))

    vec = lax.broadcasted_iota(jnp.int32, (2, NZ, 16, 128), 2) < 11

    def sm0():
        pltpu.make_async_copy(sm_in, smb.at[0], msem).wait()
        sm_copy(0).start()

    def sm1():
        sm_copy(0).wait_recv()
        smb[1] = smb[0] + jnp.where(vec, smr[0], 0.0)
        sm_copy(0).wait_send()
        smb[0] = smb[1]
        sm_copy(1).start()

    def sm2():
        sm_copy(1).wait_recv()
        smb[1] = smb[0] + jnp.where(vec, smr[1], 0.0)
        sm_copy(2).start()

    def sm3():
        sm_copy(2).wait_recv()
        smb[1, x] = smb[1, x] + smr[2, 0]

    def smz(tau):
        n = NZ

        @pl.when(z <= tau)
        def _():
            q = n - 1 - tau + z

            @pl.when(z > 0)
            def _():
                sm_z(q, True).wait_recv()
                smb[1, x, q] = smb[1, x, q] + smr[3, 0, q]

            sm_z(q, True).start()

        @pl.when(n - 1 - z <= tau)
        def _():
            q = tau - (n - 1 - z)

            @pl.when(z < n - 1)
            def _():
                sm_z(q, False).wait_recv()
                smb[1, x, q] = smb[1, x, q] + smr[3, 1, q]

            sm_z(q, False).start()

    def sm_fin():
        @pl.when(z > 0)
        def _():
            sm_z(z, True).wait_recv()
            smb[1, x, z] = smb[1, x, z] + smr[3, 0, z]

        @pl.when(z < NZ - 1)
        def _():
            sm_z(z, False).wait_recv()
            smb[1, x, z] = smb[1, x, z] + smr[3, 1, z]

        pltpu.make_async_copy(smb.at[1, x, z], sm_out, msem).start()

    small = [sm0, sm1, sm2, sm3, lambda: smz(0), lambda: smz(1), lambda: smz(2), sm_fin]

    pltpu.make_async_copy(sm_in, smb.at[0], msem).start()
    fetch(0, 0)
    pl.semaphore_wait(bar, 3 + jnp.where(z > 0, 1, 0) + jnp.where(z < NZ - 1, 1, 0))

    def tick(t, _):
        @pl.when(jnp.logical_and(lax.rem(t, 2) == 0, t < nk))
        def _():
            wait_fetch(lax.rem(t // 2, 2))

        for lag, task in stages:
            k = t - lag

            @pl.when(jnp.logical_and(k >= 0, k < nk))
            def _(k=k, task=task):
                task(k)

            if task is taskP:
                @pl.when(jnp.logical_and(lax.rem(t, 2) == 0, t + 2 < nk))
                def _():
                    fetch(t // 2 + 1, lax.rem(t // 2 + 1, 2))

        for i, step in enumerate(small):
            @pl.when(t == 8 + i)
            def _(step=step):
                step()
        return 0

    lax.fori_loop(0, nk + last, tick, 0)

    def drain(k, _):
        @pl.when(k >= nk - 3)
        def _():
            copy0(k).wait_send()

        copyF(k).wait_send()
        pltpu.make_async_copy(acc.at[k, 0, 0, 0], outs[0].at[:, pl.ds(0, 128)], osem.at[k]).wait()

        @pl.when(is_late(k))
        def _():
            copySA(k).wait_send()
            for q in range(NZ):
                @pl.when(q != z)
                def _(q=q):
                    rcopy(unit(k, q, True), zbuf(k, q, True), sZs.at[k, q], sZr.at[k, q], me.at(c=1 - c)).wait_send()

        @pl.when(jnp.logical_not(is_late(k)))
        def _():
            copySE(k).wait_send()
            for q in range(NZ):
                @pl.when(q != z)
                def _(q=q):
                    rcopy(unit(k, q, False), zbuf(k, q, False), sZs.at[k, q], sZr.at[k, q], me.at(c=1 - c)).wait_send()
        return 0

    lax.fori_loop(0, nk, drain, 0)
    sm_copy(1).wait_send()
    sm_copy(2).wait_send()
    for q in range(NZ):
        @pl.when(q != z)
        def _(q=q):
            sm_z(q, True).wait_send()
    pltpu.make_async_copy(smb.at[1, x, z], sm_out, msem).wait()


def rs_call(lhs, rhs, small):
    nm = 13
    nk = 26
    anyspec = pl.BlockSpec(memory_space=pl.ANY)
    d = [jax.ShapeDtypeStruct((128, 256), F32)] * 4 + [jax.ShapeDtypeStruct((128, 1024), F32), jax.ShapeDtypeStruct((512, 256), F32), jax.ShapeDtypeStruct((128, 256), F32)]
    sem = pltpu.SemaphoreType.DMA
    return pl.pallas_call(
        functools.partial(rs_kernel, nm),
        out_shape=d + [jax.ShapeDtypeStruct((16, 128), F32)],
        in_specs=[anyspec] * 15,
        out_specs=[anyspec] * 8,
        scratch_shapes=[
            pltpu.VMEM((2, 512, 1024), BF), pltpu.VMEM((2, 512, 1024), BF),
            pltpu.VMEM((nk, 2, 2, NZ, 128, 128), F32),
            pltpu.VMEM((3, 2, 2, NZ, 128, 128), F32),
            pltpu.VMEM((SLOTF, 2, NZ, 128, 128), F32),
            pltpu.VMEM((nk, NZ, 128, 128), F32),
            pltpu.VMEM((nk, NZ + 1, 2, 128, 128), F32),
            pltpu.VMEM((2, 2, NZ, 16, 128), F32), pltpu.VMEM((4, 2, NZ, 16, 128), F32),
            sem((2,)), sem((2,)),
            sem((nk,)), sem((nk,)), sem((nk,)), sem((nk,)), sem((nk,)), sem((nk,)),
            sem((nk, NZ)), sem((nk, NZ + 1)), sem((nk,)), sem, sem((3 + NZ,)), sem((3 + 2 * NZ,)),
        ],
        compiler_params=pltpu.CompilerParams(collective_id=0, has_side_effects=True, vmem_limit_bytes=67043328),
        name="grad_sums",
    )(*lhs, *rhs, small)


BLOCK = 64


far_below = -1e30


def from_behind(block, axis, distance):
    devices = range(lax.axis_size(axis))
    route = [(i - distance, i) for i in devices if i - distance in devices]
    return lax.ppermute(block, axis, route)


def prefix(value, axis, join, neutral, backward):
    count, mine = (lax.axis_size(axis), lax.axis_index(axis))
    pieces = jax.tree.map(lambda part: lax.all_gather(part, axis), value)
    if backward:
        pieces = jax.tree.map(lambda part: part[::-1], pieces)
        mine = count - 1 - mine
    total = jax.tree.map(
        lambda part, zero: jnp.full_like(part, 0) + jnp.asarray(zero, part.dtype), value, neutral
    )

    def turn(position, total):
        longer = join(total, jax.tree.map(lambda part: part[position], pieces))
        return jax.tree.map(lambda new, old: jnp.where(position < mine, new, old), longer, total)

    return lax.fori_loop(0, count - 1, turn, total)


def layer_norm(values, ln_gain, ln_bias):
    centred = values - jnp.mean(values, axis=-1, keepdims=True)
    spread = jnp.mean(centred * centred, axis=-1, keepdims=True)
    return centred * lax.rsqrt(spread + 1e-05) * ln_gain + ln_bias


def matmul(operand, matrix):
    return lax.dot_general(
        operand, matrix, (((operand.ndim - 1,), (0,)), ((), ())), preferred_element_type=jnp.float32
    )


def matmul_back(gradient, matrix):
    return lax.dot_general(
        gradient,
        matrix,
        (((gradient.ndim - 1,), (1,)), ((), ())),
        preferred_element_type=jnp.float32,
    )


def outer_sum(operand, gradient):
    flat_operand = operand.reshape(-1, operand.shape[-1])
    flat_gradient = gradient.reshape(-1, gradient.shape[-1])
    return lax.dot_general(
        flat_operand, flat_gradient, (((0,), (0,)), ((), ())), preferred_element_type=jnp.float32
    )


def token_mix(normed, edge_row, mix_vectors):
    earlier = jnp.concatenate([edge_row[:, None, :], normed[:, :-1, :]], axis=1)
    return tuple((normed * member + earlier * (1.0 - member) for member in mix_vectors))


def gate_rows(recept_rows, mixed_rows):
    return jax.nn.sigmoid(recept_rows) * mixed_rows


def wkv_block(decay_rate, time_first, state_in, inputs_now):
    numerator, denominator, running_max = state_in
    key_rows, value_rows = inputs_now
    length = key_rows.shape[1]
    places = jnp.arange(length, dtype=jnp.float32)[None, :, None]
    own_terms = time_first + key_rows
    anchor = jnp.maximum(
        jnp.maximum(running_max, jnp.max(key_rows, axis=1)), jnp.max(own_terms, axis=1)
    )
    scaled = jnp.exp(key_rows - anchor[:, None, :] - (places + 1.0) * decay_rate)
    running_num = jnp.cumsum(scaled * value_rows, axis=1)
    running_den = jnp.cumsum(scaled, axis=1)
    past_num = jnp.concatenate([jnp.zeros_like(running_num[:, :1]), running_num[:, :-1]], axis=1)
    past_den = jnp.concatenate([jnp.zeros_like(running_den[:, :1]), running_den[:, :-1]], axis=1)
    fading = jnp.exp(places * decay_rate)
    carried = jnp.exp(running_max[:, None, :] + places * decay_rate - anchor[:, None, :])
    own_weight = jnp.exp(own_terms - anchor[:, None, :])
    top_num = past_num * fading + own_weight * value_rows + carried * numerator[:, None, :]
    top_den = past_den * fading + own_weight + carried * denominator[:, None, :]
    outputs = top_num / top_den
    final_terms = key_rows + (length - 1.0 - places) * decay_rate
    kept_max = running_max + length * decay_rate
    new_max = jnp.maximum(kept_max, jnp.max(final_terms, axis=1))
    final_weights = jnp.exp(final_terms - new_max[:, None, :])
    kept_weight = jnp.exp(kept_max - new_max)
    new_num = jnp.sum(final_weights * value_rows, axis=1) + kept_weight * numerator
    new_den = jnp.sum(final_weights, axis=1) + kept_weight * denominator
    return ((new_num, new_den, new_max), outputs)


def wkv_local(key_rows, value_rows, time_decay, time_first, in_num, in_den, in_max):
    decay_rate = -jnp.exp(time_decay)
    block_count = key_rows.shape[1] // BLOCK

    def arrange(values):
        return jnp.moveaxis(
            values.reshape(values.shape[0], block_count, BLOCK, values.shape[2]), 1, 0
        )

    block_step = jax.checkpoint(partial(wkv_block, decay_rate, time_first))
    state_out, outputs = lax.scan(
        block_step, (in_num, in_den, in_max), (arrange(key_rows), arrange(value_rows))
    )
    outputs = jnp.moveaxis(outputs, 0, 1).reshape(key_rows.shape)
    return (outputs, state_out)


def local_summary(key_rows, value_rows, decay_rate):
    length = key_rows.shape[1]
    places = jnp.arange(length, dtype=jnp.float32)[None, :, None]
    terms = key_rows + (length - 1.0 - places) * decay_rate
    top_term = jnp.max(terms, axis=1)
    weights_now = jnp.exp(terms - top_term[:, None, :])
    return (jnp.sum(weights_now * value_rows, axis=1), jnp.sum(weights_now, axis=1), top_term)


def combine_states(earlier_one, later_one):
    earlier_num, earlier_den, earlier_max, earlier_span = earlier_one
    later_num, later_den, later_max, later_span = later_one
    shifted_max = earlier_max + later_span
    top_both = jnp.maximum(shifted_max, later_max)
    weight_early = jnp.exp(shifted_max - top_both)
    weight_late = jnp.exp(later_max - top_both)
    return (
        earlier_num * weight_early + later_num * weight_late,
        earlier_den * weight_early + later_den * weight_late,
        top_both,
        earlier_span + later_span,
    )


def combine_grads(earlier_one, later_one):
    earlier_num, earlier_den, earlier_span = earlier_one
    later_num, later_den, later_span = later_one
    factor = jnp.exp(later_span)
    return (
        later_num + factor * earlier_num,
        later_den + factor * earlier_den,
        earlier_span + later_span,
    )


def local(
    inputs,
    w_key,
    w_value,
    w_recept,
    w_output,
    w_ffn_key,
    w_ffn_value,
    w_ffn_recept,
    ln1_gain,
    ln1_bias,
    mix_key,
    mix_value,
    mix_recept,
    time_decay,
    time_first,
    ln2_gain,
    ln2_bias,
    ffn_mix_key,
    ffn_mix_recept,
    state_num,
    state_den,
    state_max,
    prev_att,
    prev_ffn,
    cotangent,
):
    position = lax.axis_index("seq")
    is_first = position == 0
    start_num = state_num.T
    start_den = state_den.T
    start_max = state_max.T
    before_att = prev_att.T
    before_ffn = prev_ffn.T
    input_rows = inputs.astype(jnp.float32)
    normed, norm_pull = jax.vjp(layer_norm, input_rows, ln1_gain, ln1_bias)
    from_left = from_behind(normed[:, -1, :], "seq", 1)
    edge_att = jnp.where(is_first, before_att, from_left)
    mixed_inputs, mix_pull = jax.vjp(token_mix, normed, edge_att, (mix_key, mix_value, mix_recept))
    key_in = mixed_inputs[0].astype(jnp.bfloat16)
    value_in = mixed_inputs[1].astype(jnp.bfloat16)
    recept_in = mixed_inputs[2].astype(jnp.bfloat16)
    key_rows = matmul(key_in, w_key)
    value_rows = matmul(value_in, w_value)
    recept_rows = matmul(recept_in, w_recept)
    decay_rate = -jnp.exp(time_decay)
    local_len = key_rows.shape[1]
    device_span = jnp.broadcast_to(local_len * decay_rate, start_num.shape)
    own_num, own_den, own_max = local_summary(key_rows, value_rows, decay_rate)
    first_element = combine_states(
        (start_num, start_den, start_max, jnp.zeros_like(device_span)),
        (own_num, own_den, own_max, device_span),
    )
    element_num = jnp.where(is_first, first_element[0], own_num)
    element_den = jnp.where(is_first, first_element[1], own_den)
    element_max = jnp.where(is_first, first_element[2], own_max)
    zero_rows = jnp.zeros_like(start_num)
    identity = (zero_rows, zero_rows, jnp.full_like(start_num, far_below), zero_rows)
    incoming = prefix(
        (element_num, element_den, element_max, device_span), "seq", combine_states, identity, False
    )
    prior_num, prior_den, prior_max = (incoming[0], incoming[1], incoming[2])
    in_num = jnp.where(is_first, start_num, prior_num)
    in_den = jnp.where(is_first, start_den, prior_den)
    in_max = jnp.where(is_first, start_max, prior_max)
    (mixed_rows, state_out), wkv_pull = jax.vjp(
        wkv_local, key_rows, value_rows, time_decay, time_first, in_num, in_den, in_max
    )
    gated, gate_pull = jax.vjp(gate_rows, recept_rows, mixed_rows)
    gated_low = gated.astype(jnp.bfloat16)
    attended = matmul(gated_low, w_output)
    middle = input_rows + attended
    normed_ffn, norm_ffn_pull = jax.vjp(layer_norm, middle, ln2_gain, ln2_bias)
    from_left_ffn = from_behind(normed_ffn[:, -1, :], "seq", 1)
    edge_ffn = jnp.where(is_first, before_ffn, from_left_ffn)
    ffn_inputs, ffn_mix_pull = jax.vjp(
        token_mix, normed_ffn, edge_ffn, (ffn_mix_key, ffn_mix_recept)
    )
    ffn_key_in = ffn_inputs[0].astype(jnp.bfloat16)
    ffn_recept_in = ffn_inputs[1].astype(jnp.bfloat16)
    hidden_pre = matmul(ffn_key_in, w_ffn_key)
    hidden = jnp.square(jax.nn.relu(hidden_pre)).astype(jnp.bfloat16)
    ffn_values = matmul(hidden, w_ffn_value)
    gate_now = jax.nn.sigmoid(matmul(ffn_recept_in, w_ffn_recept))
    block_out = (middle + gate_now * ffn_values).astype(jnp.bfloat16)
    grad_out = cotangent.astype(jnp.float32)
    grad_values = (grad_out * gate_now).astype(jnp.bfloat16)
    grad_gate = (grad_out * ffn_values * gate_now * (1.0 - gate_now)).astype(jnp.bfloat16)
    grad_hidden = matmul_back(grad_values, w_ffn_value)
    grad_pre = (grad_hidden * 2.0 * jax.nn.relu(hidden_pre)).astype(jnp.bfloat16)
    grad_w_ffn_value = outer_sum(hidden, grad_values)
    grad_w_ffn_key = outer_sum(ffn_key_in, grad_pre)
    grad_w_ffn_recept = outer_sum(ffn_recept_in, grad_gate)
    grad_normed_ffn, grad_edge_ffn, ffn_mix_grads = ffn_mix_pull(
        (matmul_back(grad_pre, w_ffn_key), matmul_back(grad_gate, w_ffn_recept))
    )
    from_right_ffn = from_behind(grad_edge_ffn, "seq", -1)
    grad_normed_ffn = grad_normed_ffn.at[:, -1, :].add(from_right_ffn)
    grad_middle, grad_ln2_gain, grad_ln2_bias = norm_ffn_pull(grad_normed_ffn)
    grad_middle = grad_middle + grad_out
    grad_attended = grad_middle.astype(jnp.bfloat16)
    grad_w_output = outer_sum(gated_low, grad_attended)
    grad_recept_full, grad_mixed = gate_pull(matmul_back(grad_attended, w_output))
    grad_recept = grad_recept_full.astype(jnp.bfloat16)
    zero_state = (zero_rows, zero_rows, zero_rows)
    first_pass = wkv_pull((grad_mixed, zero_state))
    unscale = jnp.exp(-in_max)
    local_grad_num = first_pass[4] * unscale
    local_grad_den = first_pass[5] * unscale
    later_grads = prefix(
        (local_grad_num, local_grad_den, device_span),
        "seq",
        combine_grads,
        (zero_rows, zero_rows, zero_rows),
        True,
    )
    exit_num, exit_den = (later_grads[0], later_grads[1])
    out_num, out_den, out_max = state_out
    lifting = jnp.exp(out_max)
    exit_cotangent = (
        exit_num * lifting,
        exit_den * lifting,
        (exit_num * out_num + exit_den * out_den) * lifting,
    )
    second_pass = wkv_pull((jnp.zeros_like(grad_mixed), exit_cotangent))
    grad_key_rows = (first_pass[0] + second_pass[0]).astype(jnp.bfloat16)
    grad_value_rows = (first_pass[1] + second_pass[1]).astype(jnp.bfloat16)
    grad_time_decay = first_pass[2] + second_pass[2]
    grad_time_first = first_pass[3] + second_pass[3]
    grad_start_num = first_pass[4] + second_pass[4]
    grad_start_den = first_pass[5] + second_pass[5]
    grad_start_max = first_pass[6] + second_pass[6]
    grad_w_key = outer_sum(key_in, grad_key_rows)
    grad_w_value = outer_sum(value_in, grad_value_rows)
    grad_w_recept = outer_sum(recept_in, grad_recept)
    grad_normed, grad_edge_att, mix_grads = mix_pull(
        (
            matmul_back(grad_key_rows, w_key),
            matmul_back(grad_value_rows, w_value),
            matmul_back(grad_recept, w_recept),
        )
    )
    from_right = from_behind(grad_edge_att, "seq", -1)
    grad_normed = grad_normed.at[:, -1, :].add(from_right)
    grad_input_ln, grad_ln1_gain, grad_ln1_bias = norm_pull(grad_normed)
    input_grad = (grad_input_ln + grad_middle).astype(jnp.bfloat16)
    start_num_grad = jnp.where(is_first, grad_start_num, 0.0).T
    start_den_grad = jnp.where(is_first, grad_start_den, 0.0).T
    start_max_grad = jnp.where(is_first, grad_start_max, 0.0).T
    edge_att_grad = jnp.where(is_first, grad_edge_att, 0.0).T
    edge_ffn_grad = jnp.where(is_first, grad_edge_ffn, 0.0).T
    if fits_kernel():
        small = jnp.concatenate(
            [
                part.reshape(1, -1)
                for part in (
                    grad_ln1_gain,
                    grad_ln1_bias,
                    mix_grads[0],
                    mix_grads[1],
                    mix_grads[2],
                    grad_time_decay,
                    grad_time_first,
                    grad_ln2_gain,
                    grad_ln2_bias,
                    ffn_mix_grads[0],
                    ffn_mix_grads[1],
                    start_num_grad,
                    start_den_grad,
                    start_max_grad,
                    edge_att_grad,
                    edge_ffn_grad,
                )
            ],
            axis=0,
        )
        small = small.reshape(16, NZ, 2, 128).transpose(2, 1, 0, 3)
        flat = lambda rows: rows.reshape(-1, rows.shape[-1])
        *matrices, small_sums = rs_call(
            [flat(v) for v in (key_in, value_in, recept_in, gated_low, ffn_key_in, hidden, ffn_recept_in)],
            [flat(v) for v in (grad_key_rows, grad_value_rows, grad_recept, grad_attended, grad_pre, grad_values, grad_gate)],
            small,
        )
        return (
            block_out,
            input_grad,
            *matrices,
            *[small_sums[i] for i in range(11)],
            *[small_sums[i][:, None] for i in range(11, 16)],
        )
    row_parts = (
        lax.psum_scatter(grad_w_key, "seq", scatter_dimension=0, tiled=True),
        lax.psum_scatter(grad_w_value, "seq", scatter_dimension=0, tiled=True),
        lax.psum_scatter(grad_w_recept, "seq", scatter_dimension=0, tiled=True),
        lax.psum_scatter(grad_w_output, "seq", scatter_dimension=0, tiled=True),
        lax.psum_scatter(grad_w_ffn_key, "seq", scatter_dimension=0, tiled=True),
        lax.psum_scatter(grad_w_ffn_value, "seq", scatter_dimension=0, tiled=True),
        lax.psum_scatter(grad_w_ffn_recept, "seq", scatter_dimension=0, tiled=True),
        lax.psum_scatter(grad_ln1_gain, "seq", scatter_dimension=0, tiled=True),
        lax.psum_scatter(grad_ln1_bias, "seq", scatter_dimension=0, tiled=True),
        lax.psum_scatter(mix_grads[0], "seq", scatter_dimension=0, tiled=True),
        lax.psum_scatter(mix_grads[1], "seq", scatter_dimension=0, tiled=True),
        lax.psum_scatter(mix_grads[2], "seq", scatter_dimension=0, tiled=True),
        lax.psum_scatter(grad_time_decay, "seq", scatter_dimension=0, tiled=True),
        lax.psum_scatter(grad_time_first, "seq", scatter_dimension=0, tiled=True),
        lax.psum_scatter(grad_ln2_gain, "seq", scatter_dimension=0, tiled=True),
        lax.psum_scatter(grad_ln2_bias, "seq", scatter_dimension=0, tiled=True),
        lax.psum_scatter(ffn_mix_grads[0], "seq", scatter_dimension=0, tiled=True),
        lax.psum_scatter(ffn_mix_grads[1], "seq", scatter_dimension=0, tiled=True),
        lax.psum_scatter(start_num_grad, "seq", scatter_dimension=0, tiled=True),
        lax.psum_scatter(start_den_grad, "seq", scatter_dimension=0, tiled=True),
        lax.psum_scatter(start_max_grad, "seq", scatter_dimension=0, tiled=True),
        lax.psum_scatter(edge_att_grad, "seq", scatter_dimension=0, tiled=True),
        lax.psum_scatter(edge_ffn_grad, "seq", scatter_dimension=0, tiled=True),
    )
    matrix_parts = (
        lax.psum_scatter(row_parts[0], "batch", scatter_dimension=1, tiled=True),
        lax.psum_scatter(row_parts[1], "batch", scatter_dimension=1, tiled=True),
        lax.psum_scatter(row_parts[2], "batch", scatter_dimension=1, tiled=True),
        lax.psum_scatter(row_parts[3], "batch", scatter_dimension=1, tiled=True),
        lax.psum_scatter(row_parts[4], "batch", scatter_dimension=1, tiled=True),
        lax.psum_scatter(row_parts[5], "batch", scatter_dimension=1, tiled=True),
        lax.psum_scatter(row_parts[6], "batch", scatter_dimension=1, tiled=True),
    )
    vector_parts = lax.psum(
        (
            row_parts[7],
            row_parts[8],
            row_parts[9],
            row_parts[10],
            row_parts[11],
            row_parts[12],
            row_parts[13],
            row_parts[14],
            row_parts[15],
            row_parts[16],
            row_parts[17],
        ),
        "batch",
    )
    start_parts = (row_parts[18], row_parts[19], row_parts[20], row_parts[21], row_parts[22])
    return (
        block_out,
        input_grad,
        matrix_parts[0],
        matrix_parts[1],
        matrix_parts[2],
        matrix_parts[3],
        matrix_parts[4],
        matrix_parts[5],
        matrix_parts[6],
        vector_parts[0],
        vector_parts[1],
        vector_parts[2],
        vector_parts[3],
        vector_parts[4],
        vector_parts[5],
        vector_parts[6],
        vector_parts[7],
        vector_parts[8],
        vector_parts[9],
        vector_parts[10],
        start_parts[0],
        start_parts[1],
        start_parts[2],
        start_parts[3],
        start_parts[4],
    )


def fits_kernel():
    return (lax.axis_size("seq"), lax.axis_size("batch")) == (2 * NZ, 4)


def solution(mesh):
    placed = (
        P("batch", "seq", None),
        P(),
        P(),
        P(),
        P(),
        P(),
        P(),
        P(),
        P(),
        P(),
        P(),
        P(),
        P(),
        P(),
        P(),
        P(),
        P(),
        P(),
        P(),
        P(None, "batch"),
        P(None, "batch"),
        P(None, "batch"),
        P(None, "batch"),
        P(None, "batch"),
        P("batch", "seq", None),
    )
    return jax.shard_map(
        local,
        mesh=mesh,
        in_specs=placed,
        out_specs=(
            P("batch", "seq", None),
            P("batch", "seq", None),
            P("seq", "batch"),
            P("seq", "batch"),
            P("seq", "batch"),
            P("seq", "batch"),
            P("seq", "batch"),
            P("seq", "batch"),
            P("seq", "batch"),
            P("seq"),
            P("seq"),
            P("seq"),
            P("seq"),
            P("seq"),
            P("seq"),
            P("seq"),
            P("seq"),
            P("seq"),
            P("seq"),
            P("seq"),
            P("seq", "batch"),
            P("seq", "batch"),
            P("seq", "batch"),
            P("seq", "batch"),
            P("seq", "batch"),
        ),
        check_vma=False,
    )
```

```python
import functools
from functools import partial

import jax
import jax.numpy as jnp
from jax import lax
from jax.experimental import pallas as pl
from jax.experimental.pallas import tpu as pltpu
from jax.sharding import PartitionSpec as P

MESH = pl.DeviceIdType.MESH
F32 = jnp.float32
BF = jnp.bfloat16
NS = 8
T = 512
D = 1024
SUB = T // 8


def matmul_ref(out, a, b):
    out[...] = jnp.dot(a[...], b[...], preferred_element_type=F32)


def normalize(v, gain, bias):
    mean = jnp.mean(v, axis=-1, keepdims=True)
    cen = v - mean
    var = jnp.mean(cen * cen, axis=-1, keepdims=True)
    return cen * lax.rsqrt(var + 1e-5) * gain + bias


def step_weights(delta):
    e = jnp.exp(-jnp.abs(delta))
    up = delta >= 0
    return jnp.where(up, 1.0, e), jnp.where(up, e, 1.0)


def join(early, late, span):
    em, en, ed = early
    lm, ln, ld = late
    a, b = step_weights(em + span - lm)
    return jnp.maximum(em + span, lm), a * en + b * ln, a * ed + b * ld


def fwd_kernel(*refs):
    (x_hbm, wk_h, wv_h, wr_h, wo_h, g1, b1, mk, mv, mr, td, tf, g2, b2, fmk, fmr, sn, sd, sm, pa, pf) = refs[:21]
    (o_kin, o_vin, o_rin, o_gat, o_fk, o_fr, o_mid, o_k, o_v, o_r, o_mix, o_m, o_n, o_d, o_edge) = refs[21:36]
    (xb, lanes, xf, xp, nb, kin, vin, rin, gat, fki, fri, wbuf, kb, vb, rb, mixb, mb, nmb, db,
     es, er, fs, fr, ss, sr, cur, edges, insem, outsem, esem, fsem, ssem, rsem) = refs[36:]
    s = lax.axis_index("seq")
    b = lax.axis_index("batch")
    bar = pltpu.get_barrier_semaphore()
    for d in range(1, NS):
        pl.semaphore_signal(bar, inc=1, device_id=(lax.rem(s + d, NS), b), device_id_type=MESH)
    loads = [pltpu.make_async_copy(x_hbm, xb, insem.at[0])]
    for i, w in enumerate((wk_h, wv_h, wr_h, wo_h)):
        loads.append(pltpu.make_async_copy(w, wbuf.at[i], insem.at[1 + i]))
    for cp in loads:
        cp.start()
    pending = []

    def put(src, dst):
        cp = pltpu.make_async_copy(src, dst, outsem.at[len(pending)])
        cp.start()
        pending.append(cp)

    def edge(src, dst, i, sem):
        return pltpu.make_async_remote_copy(src_ref=src, dst_ref=dst, send_sem=sem.at[0], recv_sem=sem.at[1], device_id=(i, b), device_id_type=MESH)

    loads[0].wait()
    es[...] = normalize(xb[T - 16:T, :].astype(F32), g1[...], b1[...])[8:16, :]
    pl.semaphore_wait(bar, NS - 1)
    to_next = edge(es, er, jnp.minimum(s + 1, NS - 1), esem)

    @pl.when(s < NS - 1)
    def _():
        to_next.start()

    def widen(i, _):
        rows = pl.ds(pl.multiple_of(i * 64, 64), 64)
        for g in range(8):
            lanes[g, rows, :] = xb[rows, g * 128:g * 128 + 128].astype(F32)
        return 0

    lax.fori_loop(0, T // 64, widen, 0)

    def norm1(j, _):
        rows = pl.ds(pl.multiple_of(j * 8, 8), 8)
        v = jnp.concatenate([lanes[g, pl.ds(j, 8, stride=SUB), :] for g in range(8)], axis=1)
        xp[rows, :] = v
        nb[pl.ds(pl.multiple_of(j * 8 + 8, 8), 8), :] = normalize(v, g1[...], b1[...])
        return 0

    lax.fori_loop(0, SUB, norm1, 0, unroll=4)
    first_row = lax.broadcasted_iota(jnp.int32, (8, D), 0) == 0

    def header(buf, start_row):
        tail = pltpu.roll(buf[T:T + 8, :], 1, 0)
        buf[0:8, :] = jnp.where(first_row, start_row, tail)

    def mix(buf, pairs, i):
        rows = pl.ds(pl.multiple_of(i * 32, 32), 32)
        before = buf[rows, :]
        now = buf[pl.ds(pl.multiple_of(i * 32 + 8, 8), 32), :]
        for dst, w in pairs:
            dst[rows, :] = (now * w[...] + before * (1.0 - w[...])).astype(BF)

    @pl.when(s > 0)
    def _():
        to_next.wait_recv()

    header(nb, jnp.where(s == 0, pa[...], er[7:8, :]))
    edges[0:8, :] = nb[0:8, :]

    def mix1(i, _):
        mix(nb, ((kin, mk), (vin, mv), (rin, mr)), i)
        return 0

    lax.fori_loop(0, T // 32, mix1, 0)
    put(kin, o_kin)
    put(vin, o_vin)
    put(rin, o_rin)
    loads[1].wait()
    matmul_ref(kb, kin, wbuf.at[0])
    loads[2].wait()
    matmul_ref(vb, vin, wbuf.at[1])
    put(kb, o_k)
    put(vb, o_v)
    decay = -jnp.exp(td[...])

    def own(h):
        cols = pl.ds(h * 512, 512)
        w = jnp.broadcast_to(decay[:, h * 512:h * 512 + 512], (8, 512))

        def step(j, state):
            rows = pl.ds(pl.multiple_of(j * 8, 8), 8)
            m, n, d = state
            k, v = kb[rows, cols], vb[rows, cols]
            low = m + w
            a, bb = step_weights(low - k)
            return jnp.maximum(low, k), a * n + bb * v, a * d + bb

        zero = jnp.zeros((8, 512), F32)
        k, v = kb[0:8, cols], vb[0:8, cols]
        return lax.fori_loop(1, SUB, step, (k, v, zero + 1.0), unroll=3)

    halves = [own(h) for h in range(2)]
    total = tuple(jnp.concatenate([halves[0][i], halves[1][i]], axis=1) for i in range(3))
    row = lax.broadcasted_iota(jnp.int32, (8, D), 0)
    span = SUB * decay

    def earlier(state, dist):
        m, n, d = (pltpu.roll(p, dist, 0) for p in state)
        out = row < dist
        return jnp.where(out, -1e30, m), jnp.where(out, 0.0, n), jnp.where(out, 0.0, d)

    for dist in (1, 2, 4):
        total = join(earlier(total, dist), total, dist * span)
    before_own = earlier(total, 1)
    m, n, d = (p[7:8, :] for p in total)
    ss[...] = jnp.where(row == 0, m, jnp.where(row == 1, n, d))

    def state_copy(src, dst):
        return pltpu.make_async_remote_copy(src_ref=ss, dst_ref=sr.at[src], send_sem=ssem.at[dst], recv_sem=rsem.at[src], device_id=(dst, b), device_id_type=MESH)

    for i in range(1, NS):
        @pl.when(s < i)
        def _(i=i):
            state_copy(s, i).start()

    loads[3].wait()
    matmul_ref(rb, rin, wbuf.at[2])
    put(rb, o_r)
    cur[0:1, :] = sm[...]
    cur[1:2, :] = sn[...]
    cur[2:3, :] = sd[...]
    for i in range(NS - 1):
        @pl.when(i < s)
        def _(i=i):
            state_copy(i, NS - 1).wait_recv()
            got = (sr[i, 0:1, :], sr[i, 1:2, :], sr[i, 2:3, :])
            now = join((cur[0:1, :], cur[1:2, :], cur[2:3, :]), got, 8.0 * span)
            for r in range(3):
                cur[r:r + 1, :] = now[r]

    lifted = cur[0:1, :] + row.astype(F32) * span
    wide = tuple(jnp.broadcast_to(cur[r:r + 1, :], (8, D)) for r in (1, 2))
    begin = join((lifted,) + wide, before_own, 0.0)

    def outputs(h):
        cols = pl.ds(h * 512, 512)
        w = jnp.broadcast_to(decay[:, h * 512:h * 512 + 512], (8, 512))
        bonus = jnp.broadcast_to(tf[:, h * 512:h * 512 + 512], (8, 512))

        def one(j, state):
            rows = pl.ds(pl.multiple_of(j * 8, 8), 8)
            m, n, d = state
            k, v = kb[rows, cols], vb[rows, cols]
            mb[rows, cols] = m
            nmb[rows, cols] = n
            db[rows, cols] = d
            p, u = step_weights(m - (bonus + k))
            mixed = (p * n + u * v) / (p * d + u)
            mixb[rows, cols] = mixed
            low = m + w
            a, bb = step_weights(low - k)
            return (jnp.maximum(low, k), a * n + bb * v, a * d + bb), jax.nn.sigmoid(rb[rows, cols]) * mixed

        def two(i, state):
            state, ga = one(2 * i, state)
            state, gb = one(2 * i + 1, state)
            gat[pl.ds(pl.multiple_of(i * 16, 16), 16), cols] = jnp.concatenate([ga, gb], axis=0).astype(BF)
            return state

        lax.fori_loop(0, SUB // 2, two, tuple(p[:, h * 512:h * 512 + 512] for p in begin))

    for h in range(2):
        outputs(h)
    put(gat, o_gat)
    put(mixb, o_mix)
    put(mb, o_m)
    put(nmb, o_n)
    put(db, o_d)
    loads[4].wait()
    matmul_ref(xf, gat, wbuf.at[3])

    def norm2(i):
        rows = pl.ds(pl.multiple_of(i * 32, 32), 32)
        v = xp[rows, :] + xf[rows, :]
        xp[rows, :] = v
        nb[pl.ds(pl.multiple_of(i * 32 + 8, 8), 32), :] = normalize(v, g2[...], b2[...])

    norm2(T // 32 - 1)
    fs[...] = nb[T:T + 8, :]
    to_next2 = edge(fs, fr, jnp.minimum(s + 1, NS - 1), fsem)

    @pl.when(s < NS - 1)
    def _():
        to_next2.start()

    def norm2_loop(i, _):
        norm2(i)
        return 0

    lax.fori_loop(0, T // 32 - 1, norm2_loop, 0)
    put(xp, o_mid)

    def mix2(i, _):
        mix(nb, ((fki, fmk), (fri, fmr)), i)
        return 0

    lax.fori_loop(1, T // 32, mix2, 0)

    @pl.when(s > 0)
    def _():
        to_next2.wait_recv()

    header(nb, jnp.where(s == 0, pf[...], fr[7:8, :]))
    edges[8:16, :] = nb[0:8, :]
    put(edges, o_edge)
    mix2(0, 0)
    put(fki, o_fk)
    put(fri, o_fr)

    @pl.when(s < NS - 1)
    def _():
        to_next.wait_send()
        to_next2.wait_send()

    for i in range(1, NS):
        @pl.when(s < i)
        def _(i=i):
            state_copy(s, i).wait_send()
    for cp in pending:
        cp.wait()


def fwd_call(x, wk, wv, wr, wo, vectors, states):
    anyspec = pl.BlockSpec(memory_space=pl.ANY)
    vm = pl.BlockSpec(memory_space=pltpu.VMEM)
    low, full = jax.ShapeDtypeStruct((T, D), BF), jax.ShapeDtypeStruct((T, D), F32)
    sem = pltpu.SemaphoreType.DMA
    V = pltpu.VMEM
    return pl.pallas_call(
        fwd_kernel,
        out_shape=[low] * 6 + [full] * 8 + [jax.ShapeDtypeStruct((16, D), F32)],
        in_specs=[anyspec] * 5 + [vm] * 16,
        out_specs=[anyspec] * 15,
        scratch_shapes=[
            V((T, D), BF), V((8, T, 128), F32), V((T, D), F32), V((T, D), F32), V((T + 8, D), F32),
            V((T, D), BF), V((T, D), BF), V((T, D), BF), V((T, D), BF), V((T, D), BF), V((T, D), BF),
            V((4, D, D), BF), V((T, D), F32), V((T, D), F32), V((T, D), F32), V((T, D), F32), V((T, D), F32), V((T, D), F32), V((T, D), F32),
            V((8, D), F32), V((8, D), F32), V((8, D), F32), V((8, D), F32), V((8, D), F32), V((NS, 8, D), F32), V((8, D), F32), V((16, D), F32),
            sem((5,)), sem((15,)), sem((2,)), sem((2,)), sem((NS,)), sem((NS,)),
        ],
        compiler_params=pltpu.CompilerParams(collective_id=1, has_side_effects=True, vmem_limit_bytes=67043328),
        name="forward",
    )(x, wk, wv, wr, wo, *vectors, *states)


NZ = 4
NM = 13
NK = 2 * NM
WIN = 12
WINF = 4
RA = 48
RE = 128 - RA
LAGS = [3, 5, 4, 5, 6, 6, 7, 8, 8]
RETIRE = 9


def contract0(a, b):
    return lax.dot_general(a, b, (((0,), (0,)), ((), ())), preferred_element_type=F32)


def contract1(a, b):
    return lax.dot_general(a, b, (((1,), (1,)), ((), ())), preferred_element_type=F32)


def pick(m, table):
    out = jnp.int32(table[0])
    for i, v in enumerate(table[1:], 1):
        out = jnp.where(m == i, v, out)
    return out


LEFT = (0, 9, 1, 9, 2, 9, 3, 9, 10, 4, 5, 8, 7)
RIGHT = (8, 4, 8, 5, 8, 6, 8, 7, 0, 1, 2, 3, 6)


class Place:
    def __init__(self):
        self.s, self.b = lax.axis_index("seq"), lax.axis_index("batch")
        self.z, self.x = self.s // 2, self.s % 2
        self.y, self.c = self.b // 2, self.b % 2

    def at(self, z=None, x=None, y=None, c=None):
        z = self.z if z is None else z
        x = self.x if x is None else x
        y = self.y if y is None else y
        c = self.c if c is None else c
        return (z * 2 + x, y * 2 + c)


def rcopy(src, dst, ss, rs, dev):
    return pltpu.make_async_remote_copy(src_ref=src, dst_ref=dst, send_sem=ss, recv_sem=rs, device_id=dev, device_id_type=MESH)


def bwd_kernel(*refs):
    (cot_h, x_h, wfk_h, wfv_h, wfr_h, wo_h, wr_h, wv_h, wk_h,
     kin_h, vin_h, rin_h, gat_h, fk_h, fr_h, mid_h, k_h, v_h, r_h, mix_h, m_h, n_h, d_h) = refs[:23]
    (edges, g1, b1, mk, mv, mr, td, tf, g2, b2, fmk, fmr, sn, sd) = refs[23:37]
    (o_blk, o_inp) = refs[37:39]
    outs = refs[39:46]
    sm_out = refs[46]
    (ob, wbuf, G, V, K, X, lanes, lanes2, st, sums, RS, es, er, fs, fr, ws, wr,
     acc, sbuf, rF, rSA, rSE, rZA, rZE, smb, smr,
     obsem, wsem, stsem, bigsem, outsem, esem, fsem, wssem, wrsem,
     s0s, s0r, sFs, sFr, sSs, sSr, sZs, sZr, osem, msem, mss, msr) = refs[47:]
    me = Place()
    z, x, y, c, s = me.z, me.x, me.y, me.c, me.s
    left, right = (jnp.maximum(s - 1, 0), me.b), (jnp.minimum(s + 1, NS - 1), me.b)

    bar = pltpu.get_barrier_semaphore()

    def sig(dev):
        pl.semaphore_signal(bar, inc=1, device_id=dev, device_id_type=MESH)

    sig(me.at(c=1 - c))
    sig(me.at(y=1 - y))
    for i in range(1, NS):
        sig((lax.rem(s + i, NS), me.b))

    def local(src, dst, sem):
        return pltpu.make_async_copy(src, dst, sem)

    def op_load(src, slot):
        return local(src, ob.at[slot], obsem.at[slot])

    def slab_columns(src, j, dst, sem):
        return [local(src.at[:, pl.ds(i * 512 + j * 128, 128)], dst.at[:, pl.ds(i * 128, 128)], sem) for i in range(8)]

    def slab_rows(src, j, dst, sem):
        return [local(src.at[pl.ds(i * 512 + j * 128, 128), :], dst.at[pl.ds(i * 128, 128), :], sem) for i in range(8)]

    weights = [("p", wfr_h)]
    for j in range(4):
        weights += [("c", wfk_h, j), ("r", wfv_h, j)]
    weights += [("p", wfr_h), ("p", wo_h), ("p", wr_h), ("p", wv_h), ("p", wk_h)]

    def w_start(i):
        if i >= len(weights):
            return
        kind, src, *j = weights[i]
        dst, sem = wbuf.at[i % 3], wsem.at[i % 3]
        if kind == "p":
            local(src, dst, sem).start()
        else:
            for cp in (slab_columns if kind == "c" else slab_rows)(src, j[0], dst, sem):
                cp.start()

    def w_wait(i):
        local(wo_h, wbuf.at[i % 3], wsem.at[i % 3]).wait()

    def fs_of(k):
        h = lax.rem(k, 2)
        return jnp.where(h == 0, x, y), jnp.where(h == 0, y, x)

    def partner(h):
        a, b = me.at(x=1 - x), me.at(y=1 - y)
        return (jnp.where(h == 0, a[0], b[0]), jnp.where(h == 0, a[1], b[1]))

    def copy0(k):
        return rcopy(sbuf.at[lax.rem(k, 2)], acc.at[lax.rem(k, WIN)], s0s.at[k], s0r.at[k], me.at(c=1 - c))

    def copyF(k):
        f, _ = fs_of(k)
        return rcopy(acc.at[lax.rem(k, WIN), 1 - f], rF.at[lax.rem(k, WINF)], sFs.at[k], sFr.at[k], partner(lax.rem(k, 2)))

    def copySA(k):
        f, g = fs_of(k)
        w = lax.rem(k, WIN)
        return rcopy(acc.at[w, f, 1 - g, :, pl.ds(0, RA)], rSA.at[w], sSs.at[k, 0], sSr.at[k, 0], partner(1 - lax.rem(k, 2)))

    def copySE(k):
        f, g = fs_of(k)
        w = lax.rem(k, WIN)
        return rcopy(acc.at[w, f, 1 - g, z, pl.ds(RA, RE)], rSE.at[w], sSs.at[k, 1], sSr.at[k, 1], partner(1 - lax.rem(k, 2)))

    def unit(k, q, late):
        f, g = fs_of(k)
        w = lax.rem(k, WIN)
        return acc.at[w, f, g, q, pl.ds(0, RA)] if late else acc.at[w, f, :, q, pl.ds(RA, RE)]

    def zbuf(k, slot, late):
        return (rZA if late else rZE).at[lax.rem(k, WIN), slot]

    def copyR(k, q, late):
        i = int(late)
        return rcopy(unit(k, q, late), zbuf(k, q + 1, late), sZs.at[k, i, q], sZr.at[k, i, q + 1], me.at(z=z + 1))

    def copyL(k, q, late):
        i = int(late)
        return rcopy(unit(k, q, late), zbuf(k, q, late), sZs.at[k, i, q], sZr.at[k, i, q], me.at(z=z - 1))

    def add_into(dst, src):
        dst[...] = dst[...] + src[...]

    def zsub(k, tau, late):
        @pl.when(z <= tau)
        def _():
            q = NZ - 1 - tau + z

            @pl.when(z > 0)
            def _():
                copyR(k, q, late).wait_recv()
                add_into(unit(k, q, late), zbuf(k, q + 1, late))

            copyR(k, q, late).start()

        @pl.when(NZ - 1 - z <= tau)
        def _():
            q = tau - (NZ - 1 - z)

            @pl.when(z < NZ - 1)
            def _():
                copyL(k, q, late).wait_recv()
                add_into(unit(k, q, late), zbuf(k, q, late))

            copyL(k, q, late).start()

    def zfin(k, late):
        @pl.when(z > 0)
        def _():
            copyR(k, z, late).wait_recv()
            add_into(unit(k, z, late), zbuf(k, z + 1, late))

        @pl.when(z < NZ - 1)
        def _():
            copyL(k, z, late).wait_recv()
            add_into(unit(k, z, late), zbuf(k, z, late))

    def gradient(k, core, write):
        h, m = lax.rem(k, 2), k // 2
        ls, rs = pick(m, LEFT), pick(m, RIGHT)
        cols = jnp.concatenate(
            [ob[rs, :, pl.ds(pl.multiple_of((2 * yy + core) * 256 + h * 128, 128), 128)] for yy in range(2)], axis=1)

        def group(g, _):
            res = contract0(ob[ls, :, pl.ds(pl.multiple_of(g * 512, 512), 512)], cols)
            for i in range(4):
                zz, xx = g * 2 + i // 2, i % 2
                for yy in range(2):
                    f = jnp.where(h == 0, xx, yy)
                    g2_ = jnp.where(h == 0, yy, xx)
                    write(f, g2_, zz, res[i * 128:(i + 1) * 128, yy * 128:(yy + 1) * 128])
            return 0

        lax.fori_loop(0, 2, group, 0)

    def taskP(k):
        @pl.when(k >= 2)
        def _():
            copy0(k - 2).wait_send()

        slot = lax.rem(k, 2)

        def write(f, g, zz, v):
            sbuf[slot, f, g, zz] = v

        gradient(k, 1 - c, write)
        copy0(k).start()

    def task1(k):
        copy0(k).wait_recv()
        w = lax.rem(k, WIN)

        def write(f, g, zz, v):
            acc[w, f, g, zz] = acc[w, f, g, zz] + v

        gradient(k, c, write)
        copyF(k).start()

    def task2(k):
        copyF(k).wait_recv()
        f, _ = fs_of(k)
        w = lax.rem(k, WIN)

        def body(i, _):
            add_into(acc.at[w, f, i // NZ, lax.rem(i, NZ)], rF.at[lax.rem(k, WINF), i // NZ, lax.rem(i, NZ)])
            return 0

        lax.fori_loop(0, 2 * NZ, body, 0)
        copySA(k).start()
        zsub(k, 0, False)

    def taskSA(k):
        copySA(k).wait_recv()
        f, g = fs_of(k)
        w = lax.rem(k, WIN)
        add_into(acc.at[w, f, g, :, pl.ds(0, RA)], rSA.at[w])
        zsub(k, 0, True)

    def taskFinE(k):
        zfin(k, False)
        copySE(k).start()

    def taskSE(k):
        copySE(k).wait_recv()
        f, g = fs_of(k)
        w = lax.rem(k, WIN)
        add_into(acc.at[w, f, g, z, pl.ds(RA, RE)], rSE.at[w])
        src = acc.at[w, f, g, z]
        h, m = lax.rem(k, 2), k // 2
        half = pl.ds(pl.multiple_of(h * 128, 128), 128)
        for j in range(4):
            @pl.when(m == 2 * j)
            def _(j=j):
                local(src, outs[5].at[pl.ds(j * 128, 128), half], osem.at[k]).start()

            @pl.when(m == 2 * j + 1)
            def _(j=j):
                local(src, outs[4].at[:, pl.ds(pl.multiple_of(h * 512 + j * 128, 128), 128)], osem.at[k]).start()
        for mm, i in ((8, 6), (9, 3), (10, 2), (11, 1), (12, 0)):
            @pl.when(m == mm)
            def _(i=i):
                local(src, outs[i].at[:, half], osem.at[k]).start()

    def retire(k):
        copyF(k).wait_send()
        copySA(k).wait_send()
        copySE(k).wait_send()
        for late in (False, True):
            for q in range(NZ):
                @pl.when(q != z)
                def _(q=q, late=late):
                    rcopy(unit(k, q, late), zbuf(k, q, late), sZs.at[k, int(late), q], sZr.at[k, int(late), q], me.at(c=1 - c)).wait_send()
        local(acc.at[lax.rem(k, WIN), 0, 0, 0], outs[0].at[:, pl.ds(0, 128)], osem.at[k]).wait()

    stages = [
        (RETIRE, retire),
        (LAGS[7], lambda k: zfin(k, True)),
        (LAGS[8], taskSE),
        (LAGS[6], lambda k: zsub(k, 2, True)),
        (LAGS[5], lambda k: zsub(k, 1, True)),
        (LAGS[4], taskFinE),
        (LAGS[3], lambda k: zsub(k, 2, False)),
        (LAGS[2], lambda k: zsub(k, 1, False)),
        (LAGS[1], taskSA),
        (LAGS[0], task2),
        (1, task1),
        (0, taskP),
    ]

    def sm_copy(step):
        if step == 0:
            return rcopy(smb.at[0], smr.at[0], mss.at[0], msr.at[0], me.at(c=1 - c))
        if step == 1:
            return rcopy(smb.at[2], smr.at[1], mss.at[1], msr.at[1], me.at(y=1 - y))
        return rcopy(smb.at[1, 1 - x], smr.at[2, 0], mss.at[2], msr.at[2], me.at(x=1 - x))

    def sm_z(q, to_right):
        if to_right:
            return rcopy(smb.at[1, x, q], smr.at[3, 0, q], mss.at[3 + q], msr.at[3 + q], me.at(z=z + 1))
        return rcopy(smb.at[1, x, q], smr.at[3, 1, q], mss.at[3 + q], msr.at[3 + NZ + q], me.at(z=z - 1))

    vec = lax.broadcasted_iota(jnp.int32, (2, NZ, 16, 128), 2) < 11

    def sm1():
        sm_copy(0).wait_recv()
        smb[2] = smb[0] + jnp.where(vec, smr[0], 0.0)
        sm_copy(1).start()

    def sm2():
        sm_copy(1).wait_recv()
        smb[1] = smb[2] + jnp.where(vec, smr[1], 0.0)
        sm_copy(2).start()

    def sm3():
        sm_copy(2).wait_recv()
        smb[1, x] = smb[1, x] + smr[2, 0]

    def smz(tau):
        @pl.when(z <= tau)
        def _():
            q = NZ - 1 - tau + z

            @pl.when(z > 0)
            def _():
                sm_z(q, True).wait_recv()
                smb[1, x, q] = smb[1, x, q] + smr[3, 0, q]

            sm_z(q, True).start()

        @pl.when(NZ - 1 - z <= tau)
        def _():
            q = tau - (NZ - 1 - z)

            @pl.when(z < NZ - 1)
            def _():
                sm_z(q, False).wait_recv()
                smb[1, x, q] = smb[1, x, q] + smr[3, 1, q]

            sm_z(q, False).start()

    def sm_fin():
        @pl.when(z > 0)
        def _():
            sm_z(z, True).wait_recv()
            smb[1, x, z] = smb[1, x, z] + smr[3, 0, z]

        @pl.when(z < NZ - 1)
        def _():
            sm_z(z, False).wait_recv()
            smb[1, x, z] = smb[1, x, z] + smr[3, 1, z]

        local(smb.at[1, x, z], sm_out, msem).start()

    def tiles(n, rows, body):
        def step(i, _):
            body(i, pl.ds(pl.multiple_of(i * rows, rows), rows))
            return 0

        lax.fori_loop(0, n, step, 0)

    def widen(slot):
        def body(i, rows):
            for g in range(8):
                lanes[g, rows, :] = ob[slot, rows, g * 128:g * 128 + 128].astype(F32)

        tiles(T // 64, 64, body)

    def spread(i, count):
        return jnp.concatenate(
            [jnp.concatenate([lanes[g, pl.ds(i * count + a, 8, stride=SUB), :] for g in range(8)], axis=1) for a in range(count)], axis=0)

    def unspread(i, count, value):
        for a in range(count):
            for g in range(8):
                lanes2[g, pl.ds(i * count + a, 8, stride=SUB), :] = value[a * 8:a * 8 + 8, g * 128:g * 128 + 128]

    def narrow(slot, dst, sem):
        def body(i, rows):
            for g in range(8):
                ob[slot, rows, g * 128:g * 128 + 128] = lanes2[g, rows, :].astype(BF)

        tiles(T // 64, 64, body)
        local(ob.at[slot], dst, sem).start()

    def halves(body):
        tiles(2, 512, body)

    def gate_step():
        w_wait(0)

        def mm(i, cols):
            G[:, cols] = jnp.dot(ob[10], wbuf[0, :, cols], preferred_element_type=F32)

        halves(mm)
        w_start(3)

        def body(i, rows):
            gate = jax.nn.sigmoid(G[rows, :])
            G[rows, :] = gate
            ob[8, rows, :] = (spread(i, 4) * gate).astype(BF)

        tiles(T // 32, 32, body)

    def hid(j):
        w_wait(1 + 2 * j)
        slot = (1 + 2 * j) % 3

        def mm(i, cols):
            up = jnp.maximum(jnp.dot(ob[9], wbuf[slot, :, cols], preferred_element_type=F32), 0.0)
            X[pl.ds(0, T), cols] = up
            ob[j, :, cols] = (up * up).astype(BF)

        halves(mm)

    def gpre(j):
        w_wait(2 + 2 * j)
        slot = (2 + 2 * j) % 3

        def mm(i, cols):
            back = contract1(ob[8], wbuf[slot, cols, :])
            ob[4 + j, :, cols] = (back * 2.0 * X[pl.ds(0, T), cols]).astype(BF)

        halves(mm)

    def gk_step(j):
        slot = (1 + 2 * j) % 3

        def mm(i, cols):
            part = contract1(ob[4 + j], wbuf[slot, cols, :])
            K[pl.ds(0, T), cols] = part if j == 0 else K[pl.ds(0, T), cols] + part

        halves(mm)
        w_start(1 + 2 * j + 3)

    def ffv(j):
        slot = (2 + 2 * j) % 3

        def mm(i, cols):
            part = jnp.dot(ob[j], wbuf[slot, :, cols], preferred_element_type=F32)
            V[pl.ds(0, T), cols] = part if j == 0 else V[pl.ds(0, T), cols] + part

        halves(mm)
        w_start(2 + 2 * j + 3)

    def big_load(src, dst, i):
        return local(src, dst.at[pl.ds(0, T)], bigsem.at[i])

    def block_step():
        big_load(mid_h, X, 0).wait()

        def body(i, rows):
            gate, values = G[rows, :], V[rows, :]
            unspread(i, 4, X[rows, :] + gate * values)
            ob[0, rows, :] = (spread(i, 4) * values * gate * (1.0 - gate)).astype(BF)

        tiles(T // 32, 32, body)
        narrow(5, o_blk, outsem.at[0])

    row8 = lax.broadcasted_iota(jnp.int32, (8, D), 0)

    def tail(buf):
        buf[T:T + 8, :] = jnp.where(row8 == 7, 0.0, pltpu.roll(buf[0:8, :], 7, 0))

    def edge(src, dst, sem, dev):
        return rcopy(src, dst, sem.at[0], sem.at[1], dev)

    def recept_back():
        w_wait(9)

        def mm(i, cols):
            V[pl.ds(0, T), cols] = contract1(ob[0], wbuf[0, cols, :])

        halves(mm)
        w_start(12)
        tail(K)
        tail(V)
        es[...] = K[0:8, :] * (1.0 - fmk[...]) + V[0:8, :] * (1.0 - fmr[...])

        @pl.when(s > 0)
        def _():
            edge(es, er, esem, left).start()

    def fold(v):
        return v[0:8] + v[8:16] + v[16:24] + v[24:32]

    row32 = lax.broadcasted_iota(jnp.int32, (32, D), 0)

    def centre(v):
        mean = jnp.mean(v, axis=-1, keepdims=True)
        cen = v - mean
        inv = lax.rsqrt(jnp.mean(cen * cen, axis=-1, keepdims=True) + 1e-5)
        return cen * inv, inv

    def ln_back(grad, n, inv, gain):
        h = grad * gain[...]
        return inv * (h - jnp.mean(h, axis=-1, keepdims=True) - n * jnp.mean(h * n, axis=-1, keepdims=True))

    def ln_tile(i, rows, n, gain, bias, parts, arrived, sum_rows, ln_sums):
        later = pl.ds(pl.multiple_of(i * 32 + 8, 8), 32)
        normed = n * gain[...] + bias[...]
        grad = 0.0
        if arrived is not None:
            grad = jnp.where(jnp.logical_and(row32 == 31, i == T // 32 - 1), arrived, 0.0)
        for (buf, w), r in zip(parts, sum_rows):
            now, nxt = buf[rows, :], buf[later, :]
            grad = grad + now * w[...] + nxt * (1.0 - w[...])
            sums[r] = sums[r] + fold(normed * (now - nxt))
        sums[ln_sums[0]] = sums[ln_sums[0]] + fold(grad * n)
        sums[ln_sums[1]] = sums[ln_sums[1]] + fold(grad)
        return grad

    def wait_from_right(cp):
        @pl.when(s < NS - 1)
        def _():
            cp.wait_recv()

    def middle_back(lo, hi):
        arrived = jnp.where(s == NS - 1, 0.0, er[0:1, :]) if hi == T // 32 else None

        def body(i, _):
            rows = pl.ds(pl.multiple_of(i * 32, 32), 32)
            n, inv = centre(X[rows, :])
            grad = ln_tile(i, rows, n, g2, b2, ((K, fmk), (V, fmr)), arrived, (9, 10), (7, 8))
            gm = spread(i, 4) + ln_back(grad, n, inv, g2)
            G[rows, :] = gm
            ob[1, rows, :] = gm.astype(BF)
            return 0

        lax.fori_loop(lo, hi, body, 0)

    def middle_end():
        for r, buf in ((9, K), (10, V)):
            sums[r, 0:1, :] = sums[r, 0:1, :] - buf[0:1, :] * edges[8:9, :]
        sums[15, 0:1, :] = es[0:1, :]

    def gated_back():
        w_wait(10)

        def mm(i, cols):
            V[pl.ds(0, T), cols] = contract1(ob[1], wbuf[1, cols, :])

        halves(mm)
        w_start(13)
        big_load(r_h, X, 0).wait()
        big_load(mix_h, K, 1).wait()

        def body(i, rows):
            sg = jax.nn.sigmoid(X[rows, :])
            gg = V[rows, :]
            ob[2, rows, :] = (gg * K[rows, :] * sg * (1.0 - sg)).astype(BF)
            V[rows, :] = gg * sg

        tiles(T // 32, 32, body)

    streams = (k_h, m_h, d_h, n_h, v_h)

    def st_copies(blk, slot, count):
        rows = pl.ds(pl.multiple_of(blk * 64, 64), 64)
        return [local(src.at[rows, :], st.at[slot, i], stsem.at[slot, i]) for i, src in enumerate(streams[:count])]

    def st_start(blk, count):
        for cp in st_copies(blk, lax.rem(blk, 2), count):
            cp.start()

    def st_next(blk, count):
        for cp in st_copies(blk, lax.rem(blk, 2), count):
            cp.wait()

        @pl.when(blk > 0)
        def _():
            st_start(blk - 1, count)

    decay = -jnp.exp(td[...])

    def wide(v, cols):
        return jnp.broadcast_to(v[:, cols], (8, 512))

    def first_pass(lo):
        def block(i, _):
            blk = 7 - lo - i
            slot = lax.rem(blk, 2)
            st_next(blk, 3)
            for h in range(2):
                cols = slice(h * 512, h * 512 + 512)
                w, bonus = wide(decay, cols), wide(tf[...], cols)

                def step(jj, carry):
                    R, S = carry
                    j = 7 - jj
                    at = pl.ds(pl.multiple_of(j * 8, 8), 8)
                    rows = pl.ds(pl.multiple_of(blk * 64 + j * 8, 8), 8)
                    k, m, d = st[slot, 0, at, cols], st[slot, 1, at, cols], st[slot, 2, at, cols]
                    p, u = step_weights(m - (bonus + k))
                    q = V[rows, cols] / (p * d + u)
                    qp = p * q
                    V[rows, cols] = qp
                    X[rows, cols] = u * q
                    a, _ = step_weights(m + w - k)
                    return qp + a * R, qp * K[rows, cols] + a * S

                R, S = lax.fori_loop(0, 8, step, (RS[0, :, cols], RS[1, :, cols]), unroll=2)
                RS[0, :, cols] = R
                RS[1, :, cols] = S

                @pl.when(blk == 7)
                def _():
                    RS[2, :, cols] = jnp.maximum(st[slot, 1, 56:64, cols] + w, st[slot, 0, 56:64, cols])

                @pl.when(blk == 0)
                def _():
                    RS[3, :, cols] = st[slot, 1, 0:8, cols]
            return 0

        lax.fori_loop(0, 4, block, 0)

    def suffix(value, dist, fill):
        return jnp.where(row8 >= 8 - dist, fill, pltpu.roll(value, 8 - dist, 0))

    span = SUB * decay

    def state_copy(src, dst):
        return rcopy(ws, wr.at[src], wssem.at[dst], wrsem.at[src], (dst, me.b))

    def first_end():
        A = jnp.exp(jnp.minimum(RS[3] + span - RS[2], 0.0))
        R, S = RS[0], RS[1]
        for dist in (1, 2, 4):
            R = R + A * suffix(R, dist, 0.0)
            S = S + A * suffix(S, dist, 0.0)
            A = A * suffix(A, dist, 1.0)
        RS[0], RS[1], RS[4] = R, S, A
        ws[...] = jnp.where(row8 == 0, R[0:1], jnp.where(row8 == 1, S[0:1], RS[3, 0:1, :]))
        for i in range(NS - 1):
            @pl.when(i < s)
            def _(i=i):
                state_copy(s, i).start()

    def second_start():
        RS[5] = jnp.zeros((8, D), F32)
        RS[6] = jnp.zeros((8, D), F32)
        for i in range(1, NS):
            @pl.when(i > s)
            def _(i=i):
                state_copy(i, 0).wait_recv()
                far = jnp.exp(jnp.minimum(RS[2, 7:8, :] + (i - s - 1).astype(F32) * (8.0 * span) - wr[i, 2:3, :], 0.0))
                RS[5, 0:1, :] = RS[5, 0:1, :] + far * wr[i, 0:1, :]
                RS[6, 0:1, :] = RS[6, 0:1, :] + far * wr[i, 1:2, :]
        Rin, Sin = RS[5, 0:1, :], RS[6, 0:1, :]
        A = RS[4]
        R = RS[0] + A * Rin
        S = RS[1] + A * Sin
        RS[0] = jnp.where(row8 == 7, Rin, pltpu.roll(R, 7, 0))
        RS[1] = jnp.where(row8 == 7, Sin, pltpu.roll(S, 7, 0))

    def second_pass(lo, n):
        def block(i, _):
            blk = 7 - lo - i
            slot = lax.rem(blk, 2)
            st_next(blk, 5)
            for h in range(2):
                cols = slice(h * 512, h * 512 + 512)
                w = wide(decay, cols)

                def one(j, carry):
                    R, S, first, slow = carry
                    at = pl.ds(pl.multiple_of(j * 8, 8), 8)
                    rows = pl.ds(pl.multiple_of(blk * 64 + j * 8, 8), 8)
                    k, m, d, n_, v = (st[slot, q, at, cols] for q in range(5))
                    mixed, qp, uq = K[rows, cols], V[rows, cols], X[rows, cols]
                    a, b = step_weights(m + w - k)
                    own = uq * (v - mixed)
                    gv = uq + b * R
                    gk = own + b * (v * R - S)
                    first = first + own
                    slow = slow + a * (n_ * R - d * S)
                    return (qp + a * R, qp * mixed + a * S, first, slow), gk, gv

                def step(jj, carry):
                    j = 3 - jj
                    carry, gk1, gv1 = one(2 * j + 1, carry)
                    carry, gk0, gv0 = one(2 * j, carry)
                    pair = pl.ds(pl.multiple_of(blk * 64 + j * 16, 16), 16)
                    ob[6, pair, cols] = jnp.concatenate([gk0, gk1], axis=0).astype(BF)
                    ob[3, pair, cols] = jnp.concatenate([gv0, gv1], axis=0).astype(BF)
                    return carry

                R, S, first, slow = lax.fori_loop(0, 4, step, (RS[0, :, cols], RS[1, :, cols], sums[6, :, cols], sums[5, :, cols]))
                RS[0, :, cols] = R
                RS[1, :, cols] = S
                sums[6, :, cols] = first
                sums[5, :, cols] = slow
            return 0

        lax.fori_loop(0, n, block, 0)

    def second_end():
        gn, gd = RS[0, 0:1, :], -RS[1, 0:1, :]
        sums[11, 0:1, :] = gn
        sums[12, 0:1, :] = gd
        sums[13, 0:1, :] = sn[...] * gn + sd[...] * gd
        sums[5] = sums[5] * decay

    def input_mm(i, slot, buf):
        w_wait(i)

        def mm(_, cols):
            buf[pl.ds(0, T), cols] = contract1(ob[slot], wbuf[i % 3, cols, :])

        halves(mm)
        tail(buf)

    def input_edge():
        fs[...] = K[0:8, :] * (1.0 - mk[...]) + V[0:8, :] * (1.0 - mv[...]) + X[0:8, :] * (1.0 - mr[...])

        @pl.when(s > 0)
        def _():
            edge(fs, fr, fsem, left).start()

    def input_back(lo, hi):
        arrived = jnp.where(s == NS - 1, 0.0, fr[0:1, :]) if hi == T // 32 else None

        def body(i, _):
            rows = pl.ds(pl.multiple_of(i * 32, 32), 32)
            n, inv = centre(spread(i, 4))
            grad = ln_tile(i, rows, n, g1, b1, ((K, mk), (V, mv), (X, mr)), arrived, (2, 3, 4), (0, 1))
            unspread(i, 4, G[rows, :] + ln_back(grad, n, inv, g1))
            return 0

        lax.fori_loop(lo, hi, body, 0)

    def input_end():
        for r, buf in ((2, K), (3, V), (4, X)):
            sums[r, 0:1, :] = sums[r, 0:1, :] - buf[0:1, :] * edges[0:1, :]
        sums[14, 0:1, :] = fs[0:1, :]
        narrow(0, o_inp, outsem.at[1])
        alone = jnp.where(s == 0, 1.0, 0.0)
        rows = [jnp.sum(sums[r], axis=0, keepdims=True) for r in range(11)] + [jnp.where(s == 0, sums[r, 0:1, :], 0.0) for r in range(11, 16)]
        table = jnp.concatenate(rows, axis=0)
        for g in range(8):
            smb[0, g % 2, g // 2] = table[:, g * 128:g * 128 + 128]
        sm_copy(0).start()

    def start_all(*copies):
        for cp in copies:
            cp.start()

    compute = {
        0: [lambda: gpre(0)],
        1: [lambda: gk_step(0), lambda: hid(1)],
        2: [lambda: ffv(0), lambda: gpre(1)],
        3: [lambda: gk_step(1), lambda: hid(2)],
        4: [lambda: ffv(1), lambda: gpre(2)],
        5: [lambda: gk_step(2), lambda: hid(3), lambda: start_all(op_load(gat_h, 4))],
        6: [lambda: ffv(2), lambda: gpre(3), lambda: big_load(mid_h, X, 0).start()],
        7: [lambda: gk_step(3), lambda: ffv(3)],
        8: [block_step],
        9: [recept_back],
        10: [lambda: middle_back(0, 8)],
        11: [lambda: wait_from_right(edge(es, er, esem, left)), lambda: middle_back(8, 16), middle_end,
             lambda: start_all(big_load(r_h, X, 0), big_load(mix_h, K, 1)), lambda: st_start(7, 3),
             lambda: local(ob.at[5], o_blk, outsem.at[0]).wait(), lambda: start_all(op_load(rin_h, 5))],
        12: [gated_back],
        13: [lambda: first_pass(0)],
        14: [lambda: first_pass(4), first_end, lambda: st_start(7, 5)],
        15: [second_start, lambda: second_pass(0, 2), lambda: start_all(op_load(vin_h, 8))],
        16: [lambda: second_pass(2, 3)],
        17: [lambda: second_pass(5, 3), second_end, lambda: start_all(op_load(kin_h, 7), op_load(x_h, 9))],
        18: [lambda: input_mm(11, 2, X), lambda: input_mm(12, 3, V)],
        19: [lambda: input_mm(13, 6, K), input_edge, lambda: op_load(x_h, 9).wait(), lambda: widen(9)],
        20: [lambda: input_back(0, 8)],
        21: [lambda: wait_from_right(edge(fs, fr, fsem, left)), lambda: input_back(8, 16), input_end],
        23: [sm1],
        24: [sm2],
        25: [sm3, lambda: smz(0)],
        27: [lambda: smz(1)],
        29: [lambda: smz(2)],
        31: [sm_fin],
    }
    landed = {18: (gat_h, 4), 20: (rin_h, 5), 22: (vin_h, 8), 24: (kin_h, 7)}

    start_all(op_load(fr_h, 10), op_load(cot_h, 1), op_load(fk_h, 9))
    for i in range(3):
        w_start(i)
    sums[...] = jnp.zeros_like(sums)
    RS[...] = jnp.zeros_like(RS)
    op_load(cot_h, 1).wait()
    widen(1)
    op_load(fr_h, 10).wait()
    gate_step()
    op_load(fk_h, 9).wait()
    hid(0)
    pl.semaphore_wait(bar, NS + 1)

    def tick(t, _):
        for at, (src, slot) in landed.items():
            @pl.when(t == at)
            def _(src=src, slot=slot):
                op_load(src, slot).wait()

        for lag, task in stages:
            k = t - lag

            @pl.when(jnp.logical_and(k >= 0, k < NK))
            def _(k=k, task=task):
                task(k)

        for at, steps in compute.items():
            @pl.when(t == at)
            def _(steps=steps):
                for step in steps:
                    step()
        return 0

    lax.fori_loop(0, NK + RETIRE, tick, 0)

    copy0(NK - 2).wait_send()
    copy0(NK - 1).wait_send()
    for i in range(3):
        sm_copy(i).wait_send()
    for q in range(NZ):
        @pl.when(q != z)
        def _(q=q):
            sm_z(q, True).wait_send()

    @pl.when(s > 0)
    def _():
        edge(es, er, esem, left).wait_send()
        edge(fs, fr, fsem, left).wait_send()

    for i in range(NS - 1):
        @pl.when(i < s)
        def _(i=i):
            state_copy(s, i).wait_send()
    local(smb.at[1, x, z], sm_out, msem).wait()
    local(ob.at[0], o_inp, outsem.at[1]).wait()


def bwd_call(cot, x, mats, acts, edges, vectors, sn, sd):
    anyspec = pl.BlockSpec(memory_space=pl.ANY)
    vm = pl.BlockSpec(memory_space=pltpu.VMEM)
    S = jax.ShapeDtypeStruct
    sem = pltpu.SemaphoreType.DMA
    M = pltpu.VMEM
    return pl.pallas_call(
        bwd_kernel,
        out_shape=[S((T, D), BF)] * 2 + [S((128, 256), F32)] * 4 + [S((128, 1024), F32), S((512, 256), F32), S((128, 256), F32), S((16, 128), F32)],
        in_specs=[anyspec] * 23 + [vm] * 14,
        out_specs=[anyspec] * 10,
        scratch_shapes=[
            M((11, T, D), BF), M((3, D, D), BF), M((T, D), F32), M((T + 8, D), F32), M((T + 8, D), F32), M((T + 8, D), F32),
            M((8, T, 128), F32), M((8, T, 128), F32), M((2, 5, 64, D), F32), M((16, 8, D), F32), M((7, 8, D), F32),
            M((8, D), F32), M((8, D), F32), M((8, D), F32), M((8, D), F32), M((8, D), F32), M((NS, 8, D), F32),
            M((WIN, 2, 2, NZ, 128, 128), F32), M((2, 2, 2, NZ, 128, 128), F32), M((WINF, 2, NZ, 128, 128), F32),
            M((WIN, NZ, RA, 128), F32), M((WIN, RE, 128), F32), M((WIN, NZ + 1, RA, 128), F32), M((WIN, NZ + 1, 2, RE, 128), F32),
            M((3, 2, NZ, 16, 128), F32), M((4, 2, NZ, 16, 128), F32),
            sem((11,)), sem((3,)), sem((2, 5)), sem((2,)), sem((2,)), sem((2,)), sem((2,)), sem((NS,)), sem((NS,)),
            sem((NK,)), sem((NK,)), sem((NK,)), sem((NK,)), sem((NK, 2)), sem((NK, 2)),
            sem((NK, 2, NZ)), sem((NK, 2, NZ + 1)), sem((NK,)), sem, sem((3 + NZ,)), sem((3 + 2 * NZ,)),
        ],
        compiler_params=pltpu.CompilerParams(collective_id=0, has_side_effects=True, vmem_limit_bytes=67043328),
        name="backward",
    )(cot, x, *mats, *acts, edges, *vectors, sn, sd)

def fits(mesh):
    return (mesh.shape["seq"], mesh.shape["batch"]) == (2 * NZ, 4)


def local(
    inputs,
    w_key,
    w_value,
    w_recept,
    w_output,
    w_ffn_key,
    w_ffn_value,
    w_ffn_recept,
    ln1_gain,
    ln1_bias,
    mix_key,
    mix_value,
    mix_recept,
    time_decay,
    time_first,
    ln2_gain,
    ln2_bias,
    ffn_mix_key,
    ffn_mix_recept,
    state_num,
    state_den,
    state_max,
    prev_att,
    prev_ffn,
    cotangent,
):
    rows = inputs.reshape(T, D)
    vectors = [
        v.reshape(1, D)
        for v in (
            ln1_gain,
            ln1_bias,
            mix_key,
            mix_value,
            mix_recept,
            time_decay,
            time_first,
            ln2_gain,
            ln2_bias,
            ffn_mix_key,
            ffn_mix_recept,
        )
    ]
    states = [v.reshape(1, D) for v in (state_num, state_den, state_max, prev_att, prev_ffn)]
    *acts, edges = fwd_call(rows, w_key, w_value, w_recept, w_output, vectors, states)
    block_out, input_grad, *matrices, small = bwd_call(
        cotangent.reshape(T, D),
        rows,
        [w_ffn_key, w_ffn_value, w_ffn_recept, w_output, w_recept, w_value, w_key],
        acts,
        edges,
        vectors,
        states[0],
        states[1],
    )
    return (
        block_out.reshape(inputs.shape),
        input_grad.reshape(inputs.shape),
        *matrices,
        *[small[i] for i in range(11)],
        *[small[i][:, None] for i in range(11, 16)],
    )


BLOCK = 64


far_below = -1e30


def from_behind(block, axis, distance):
    devices = range(lax.axis_size(axis))
    route = [(i - distance, i) for i in devices if i - distance in devices]
    return lax.ppermute(block, axis, route)


def prefix(value, axis, join, neutral, backward):
    count, mine = (lax.axis_size(axis), lax.axis_index(axis))
    pieces = jax.tree.map(lambda part: lax.all_gather(part, axis), value)
    if backward:
        pieces = jax.tree.map(lambda part: part[::-1], pieces)
        mine = count - 1 - mine
    total = jax.tree.map(
        lambda part, zero: jnp.full_like(part, 0) + jnp.asarray(zero, part.dtype), value, neutral
    )

    def turn(position, total):
        longer = join(total, jax.tree.map(lambda part: part[position], pieces))
        return jax.tree.map(lambda new, old: jnp.where(position < mine, new, old), longer, total)

    return lax.fori_loop(0, count - 1, turn, total)


def layer_norm(values, ln_gain, ln_bias):
    centred = values - jnp.mean(values, axis=-1, keepdims=True)
    spread = jnp.mean(centred * centred, axis=-1, keepdims=True)
    return centred * lax.rsqrt(spread + 1e-05) * ln_gain + ln_bias


def matmul(operand, matrix):
    return lax.dot_general(
        operand, matrix, (((operand.ndim - 1,), (0,)), ((), ())), preferred_element_type=jnp.float32
    )


def matmul_back(gradient, matrix):
    return lax.dot_general(
        gradient,
        matrix,
        (((gradient.ndim - 1,), (1,)), ((), ())),
        preferred_element_type=jnp.float32,
    )


def outer_sum(operand, gradient):
    flat_operand = operand.reshape(-1, operand.shape[-1])
    flat_gradient = gradient.reshape(-1, gradient.shape[-1])
    return lax.dot_general(
        flat_operand, flat_gradient, (((0,), (0,)), ((), ())), preferred_element_type=jnp.float32
    )


def token_mix(normed, edge_row, mix_vectors):
    earlier = jnp.concatenate([edge_row[:, None, :], normed[:, :-1, :]], axis=1)
    return tuple((normed * member + earlier * (1.0 - member) for member in mix_vectors))


def gate_rows(recept_rows, mixed_rows):
    return jax.nn.sigmoid(recept_rows) * mixed_rows


def wkv_block(decay_rate, time_first, state_in, inputs_now):
    numerator, denominator, running_max = state_in
    key_rows, value_rows = inputs_now
    length = key_rows.shape[1]
    places = jnp.arange(length, dtype=jnp.float32)[None, :, None]
    own_terms = time_first + key_rows
    anchor = jnp.maximum(
        jnp.maximum(running_max, jnp.max(key_rows, axis=1)), jnp.max(own_terms, axis=1)
    )
    scaled = jnp.exp(key_rows - anchor[:, None, :] - (places + 1.0) * decay_rate)
    running_num = jnp.cumsum(scaled * value_rows, axis=1)
    running_den = jnp.cumsum(scaled, axis=1)
    past_num = jnp.concatenate([jnp.zeros_like(running_num[:, :1]), running_num[:, :-1]], axis=1)
    past_den = jnp.concatenate([jnp.zeros_like(running_den[:, :1]), running_den[:, :-1]], axis=1)
    fading = jnp.exp(places * decay_rate)
    carried = jnp.exp(running_max[:, None, :] + places * decay_rate - anchor[:, None, :])
    own_weight = jnp.exp(own_terms - anchor[:, None, :])
    top_num = past_num * fading + own_weight * value_rows + carried * numerator[:, None, :]
    top_den = past_den * fading + own_weight + carried * denominator[:, None, :]
    outputs = top_num / top_den
    final_terms = key_rows + (length - 1.0 - places) * decay_rate
    kept_max = running_max + length * decay_rate
    new_max = jnp.maximum(kept_max, jnp.max(final_terms, axis=1))
    final_weights = jnp.exp(final_terms - new_max[:, None, :])
    kept_weight = jnp.exp(kept_max - new_max)
    new_num = jnp.sum(final_weights * value_rows, axis=1) + kept_weight * numerator
    new_den = jnp.sum(final_weights, axis=1) + kept_weight * denominator
    return ((new_num, new_den, new_max), outputs)


def wkv_local(key_rows, value_rows, time_decay, time_first, in_num, in_den, in_max):
    decay_rate = -jnp.exp(time_decay)
    block_count = key_rows.shape[1] // BLOCK

    def arrange(values):
        return jnp.moveaxis(
            values.reshape(values.shape[0], block_count, BLOCK, values.shape[2]), 1, 0
        )

    block_step = jax.checkpoint(partial(wkv_block, decay_rate, time_first))
    state_out, outputs = lax.scan(
        block_step, (in_num, in_den, in_max), (arrange(key_rows), arrange(value_rows))
    )
    outputs = jnp.moveaxis(outputs, 0, 1).reshape(key_rows.shape)
    return (outputs, state_out)


def local_summary(key_rows, value_rows, decay_rate):
    length = key_rows.shape[1]
    places = jnp.arange(length, dtype=jnp.float32)[None, :, None]
    terms = key_rows + (length - 1.0 - places) * decay_rate
    top_term = jnp.max(terms, axis=1)
    weights_now = jnp.exp(terms - top_term[:, None, :])
    return (jnp.sum(weights_now * value_rows, axis=1), jnp.sum(weights_now, axis=1), top_term)


def combine_states(earlier_one, later_one):
    earlier_num, earlier_den, earlier_max, earlier_span = earlier_one
    later_num, later_den, later_max, later_span = later_one
    shifted_max = earlier_max + later_span
    top_both = jnp.maximum(shifted_max, later_max)
    weight_early = jnp.exp(shifted_max - top_both)
    weight_late = jnp.exp(later_max - top_both)
    return (
        earlier_num * weight_early + later_num * weight_late,
        earlier_den * weight_early + later_den * weight_late,
        top_both,
        earlier_span + later_span,
    )


def combine_grads(earlier_one, later_one):
    earlier_num, earlier_den, earlier_span = earlier_one
    later_num, later_den, later_span = later_one
    factor = jnp.exp(later_span)
    return (
        later_num + factor * earlier_num,
        later_den + factor * earlier_den,
        earlier_span + later_span,
    )


def local_plain(
    inputs,
    w_key,
    w_value,
    w_recept,
    w_output,
    w_ffn_key,
    w_ffn_value,
    w_ffn_recept,
    ln1_gain,
    ln1_bias,
    mix_key,
    mix_value,
    mix_recept,
    time_decay,
    time_first,
    ln2_gain,
    ln2_bias,
    ffn_mix_key,
    ffn_mix_recept,
    state_num,
    state_den,
    state_max,
    prev_att,
    prev_ffn,
    cotangent,
):
    position = lax.axis_index("seq")
    is_first = position == 0
    start_num = state_num.T
    start_den = state_den.T
    start_max = state_max.T
    before_att = prev_att.T
    before_ffn = prev_ffn.T
    input_rows = inputs.astype(jnp.float32)
    normed, norm_pull = jax.vjp(layer_norm, input_rows, ln1_gain, ln1_bias)
    from_left = from_behind(normed[:, -1, :], "seq", 1)
    edge_att = jnp.where(is_first, before_att, from_left)
    mixed_inputs, mix_pull = jax.vjp(token_mix, normed, edge_att, (mix_key, mix_value, mix_recept))
    key_in = mixed_inputs[0].astype(jnp.bfloat16)
    value_in = mixed_inputs[1].astype(jnp.bfloat16)
    recept_in = mixed_inputs[2].astype(jnp.bfloat16)
    key_rows = matmul(key_in, w_key)
    value_rows = matmul(value_in, w_value)
    recept_rows = matmul(recept_in, w_recept)
    decay_rate = -jnp.exp(time_decay)
    local_len = key_rows.shape[1]
    device_span = jnp.broadcast_to(local_len * decay_rate, start_num.shape)
    own_num, own_den, own_max = local_summary(key_rows, value_rows, decay_rate)
    first_element = combine_states(
        (start_num, start_den, start_max, jnp.zeros_like(device_span)),
        (own_num, own_den, own_max, device_span),
    )
    element_num = jnp.where(is_first, first_element[0], own_num)
    element_den = jnp.where(is_first, first_element[1], own_den)
    element_max = jnp.where(is_first, first_element[2], own_max)
    zero_rows = jnp.zeros_like(start_num)
    identity = (zero_rows, zero_rows, jnp.full_like(start_num, far_below), zero_rows)
    incoming = prefix(
        (element_num, element_den, element_max, device_span), "seq", combine_states, identity, False
    )
    prior_num, prior_den, prior_max = (incoming[0], incoming[1], incoming[2])
    in_num = jnp.where(is_first, start_num, prior_num)
    in_den = jnp.where(is_first, start_den, prior_den)
    in_max = jnp.where(is_first, start_max, prior_max)
    (mixed_rows, state_out), wkv_pull = jax.vjp(
        wkv_local, key_rows, value_rows, time_decay, time_first, in_num, in_den, in_max
    )
    gated, gate_pull = jax.vjp(gate_rows, recept_rows, mixed_rows)
    gated_low = gated.astype(jnp.bfloat16)
    attended = matmul(gated_low, w_output)
    middle = input_rows + attended
    normed_ffn, norm_ffn_pull = jax.vjp(layer_norm, middle, ln2_gain, ln2_bias)
    from_left_ffn = from_behind(normed_ffn[:, -1, :], "seq", 1)
    edge_ffn = jnp.where(is_first, before_ffn, from_left_ffn)
    ffn_inputs, ffn_mix_pull = jax.vjp(
        token_mix, normed_ffn, edge_ffn, (ffn_mix_key, ffn_mix_recept)
    )
    ffn_key_in = ffn_inputs[0].astype(jnp.bfloat16)
    ffn_recept_in = ffn_inputs[1].astype(jnp.bfloat16)
    hidden_pre = matmul(ffn_key_in, w_ffn_key)
    hidden = jnp.square(jax.nn.relu(hidden_pre)).astype(jnp.bfloat16)
    ffn_values = matmul(hidden, w_ffn_value)
    gate_now = jax.nn.sigmoid(matmul(ffn_recept_in, w_ffn_recept))
    block_out = (middle + gate_now * ffn_values).astype(jnp.bfloat16)
    grad_out = cotangent.astype(jnp.float32)
    grad_values = (grad_out * gate_now).astype(jnp.bfloat16)
    grad_gate = (grad_out * ffn_values * gate_now * (1.0 - gate_now)).astype(jnp.bfloat16)
    grad_hidden = matmul_back(grad_values, w_ffn_value)
    grad_pre = (grad_hidden * 2.0 * jax.nn.relu(hidden_pre)).astype(jnp.bfloat16)
    grad_w_ffn_value = outer_sum(hidden, grad_values)
    grad_w_ffn_key = outer_sum(ffn_key_in, grad_pre)
    grad_w_ffn_recept = outer_sum(ffn_recept_in, grad_gate)
    grad_normed_ffn, grad_edge_ffn, ffn_mix_grads = ffn_mix_pull(
        (matmul_back(grad_pre, w_ffn_key), matmul_back(grad_gate, w_ffn_recept))
    )
    from_right_ffn = from_behind(grad_edge_ffn, "seq", -1)
    grad_normed_ffn = grad_normed_ffn.at[:, -1, :].add(from_right_ffn)
    grad_middle, grad_ln2_gain, grad_ln2_bias = norm_ffn_pull(grad_normed_ffn)
    grad_middle = grad_middle + grad_out
    grad_attended = grad_middle.astype(jnp.bfloat16)
    grad_w_output = outer_sum(gated_low, grad_attended)
    grad_recept_full, grad_mixed = gate_pull(matmul_back(grad_attended, w_output))
    grad_recept = grad_recept_full.astype(jnp.bfloat16)
    zero_state = (zero_rows, zero_rows, zero_rows)
    first_pass = wkv_pull((grad_mixed, zero_state))
    unscale = jnp.exp(-in_max)
    local_grad_num = first_pass[4] * unscale
    local_grad_den = first_pass[5] * unscale
    later_grads = prefix(
        (local_grad_num, local_grad_den, device_span),
        "seq",
        combine_grads,
        (zero_rows, zero_rows, zero_rows),
        True,
    )
    exit_num, exit_den = (later_grads[0], later_grads[1])
    out_num, out_den, out_max = state_out
    lifting = jnp.exp(out_max)
    exit_cotangent = (
        exit_num * lifting,
        exit_den * lifting,
        (exit_num * out_num + exit_den * out_den) * lifting,
    )
    second_pass = wkv_pull((jnp.zeros_like(grad_mixed), exit_cotangent))
    grad_key_rows = (first_pass[0] + second_pass[0]).astype(jnp.bfloat16)
    grad_value_rows = (first_pass[1] + second_pass[1]).astype(jnp.bfloat16)
    grad_time_decay = first_pass[2] + second_pass[2]
    grad_time_first = first_pass[3] + second_pass[3]
    grad_start_num = first_pass[4] + second_pass[4]
    grad_start_den = first_pass[5] + second_pass[5]
    grad_start_max = first_pass[6] + second_pass[6]
    grad_w_key = outer_sum(key_in, grad_key_rows)
    grad_w_value = outer_sum(value_in, grad_value_rows)
    grad_w_recept = outer_sum(recept_in, grad_recept)
    grad_normed, grad_edge_att, mix_grads = mix_pull(
        (
            matmul_back(grad_key_rows, w_key),
            matmul_back(grad_value_rows, w_value),
            matmul_back(grad_recept, w_recept),
        )
    )
    from_right = from_behind(grad_edge_att, "seq", -1)
    grad_normed = grad_normed.at[:, -1, :].add(from_right)
    grad_input_ln, grad_ln1_gain, grad_ln1_bias = norm_pull(grad_normed)
    input_grad = (grad_input_ln + grad_middle).astype(jnp.bfloat16)
    start_num_grad = jnp.where(is_first, grad_start_num, 0.0).T
    start_den_grad = jnp.where(is_first, grad_start_den, 0.0).T
    start_max_grad = jnp.where(is_first, grad_start_max, 0.0).T
    edge_att_grad = jnp.where(is_first, grad_edge_att, 0.0).T
    edge_ffn_grad = jnp.where(is_first, grad_edge_ffn, 0.0).T
    row_parts = (
        lax.psum_scatter(grad_w_key, "seq", scatter_dimension=0, tiled=True),
        lax.psum_scatter(grad_w_value, "seq", scatter_dimension=0, tiled=True),
        lax.psum_scatter(grad_w_recept, "seq", scatter_dimension=0, tiled=True),
        lax.psum_scatter(grad_w_output, "seq", scatter_dimension=0, tiled=True),
        lax.psum_scatter(grad_w_ffn_key, "seq", scatter_dimension=0, tiled=True),
        lax.psum_scatter(grad_w_ffn_value, "seq", scatter_dimension=0, tiled=True),
        lax.psum_scatter(grad_w_ffn_recept, "seq", scatter_dimension=0, tiled=True),
        lax.psum_scatter(grad_ln1_gain, "seq", scatter_dimension=0, tiled=True),
        lax.psum_scatter(grad_ln1_bias, "seq", scatter_dimension=0, tiled=True),
        lax.psum_scatter(mix_grads[0], "seq", scatter_dimension=0, tiled=True),
        lax.psum_scatter(mix_grads[1], "seq", scatter_dimension=0, tiled=True),
        lax.psum_scatter(mix_grads[2], "seq", scatter_dimension=0, tiled=True),
        lax.psum_scatter(grad_time_decay, "seq", scatter_dimension=0, tiled=True),
        lax.psum_scatter(grad_time_first, "seq", scatter_dimension=0, tiled=True),
        lax.psum_scatter(grad_ln2_gain, "seq", scatter_dimension=0, tiled=True),
        lax.psum_scatter(grad_ln2_bias, "seq", scatter_dimension=0, tiled=True),
        lax.psum_scatter(ffn_mix_grads[0], "seq", scatter_dimension=0, tiled=True),
        lax.psum_scatter(ffn_mix_grads[1], "seq", scatter_dimension=0, tiled=True),
        lax.psum_scatter(start_num_grad, "seq", scatter_dimension=0, tiled=True),
        lax.psum_scatter(start_den_grad, "seq", scatter_dimension=0, tiled=True),
        lax.psum_scatter(start_max_grad, "seq", scatter_dimension=0, tiled=True),
        lax.psum_scatter(edge_att_grad, "seq", scatter_dimension=0, tiled=True),
        lax.psum_scatter(edge_ffn_grad, "seq", scatter_dimension=0, tiled=True),
    )
    matrix_parts = (
        lax.psum_scatter(row_parts[0], "batch", scatter_dimension=1, tiled=True),
        lax.psum_scatter(row_parts[1], "batch", scatter_dimension=1, tiled=True),
        lax.psum_scatter(row_parts[2], "batch", scatter_dimension=1, tiled=True),
        lax.psum_scatter(row_parts[3], "batch", scatter_dimension=1, tiled=True),
        lax.psum_scatter(row_parts[4], "batch", scatter_dimension=1, tiled=True),
        lax.psum_scatter(row_parts[5], "batch", scatter_dimension=1, tiled=True),
        lax.psum_scatter(row_parts[6], "batch", scatter_dimension=1, tiled=True),
    )
    vector_parts = lax.psum(
        (
            row_parts[7],
            row_parts[8],
            row_parts[9],
            row_parts[10],
            row_parts[11],
            row_parts[12],
            row_parts[13],
            row_parts[14],
            row_parts[15],
            row_parts[16],
            row_parts[17],
        ),
        "batch",
    )
    start_parts = (row_parts[18], row_parts[19], row_parts[20], row_parts[21], row_parts[22])
    return (
        block_out,
        input_grad,
        matrix_parts[0],
        matrix_parts[1],
        matrix_parts[2],
        matrix_parts[3],
        matrix_parts[4],
        matrix_parts[5],
        matrix_parts[6],
        vector_parts[0],
        vector_parts[1],
        vector_parts[2],
        vector_parts[3],
        vector_parts[4],
        vector_parts[5],
        vector_parts[6],
        vector_parts[7],
        vector_parts[8],
        vector_parts[9],
        vector_parts[10],
        start_parts[0],
        start_parts[1],
        start_parts[2],
        start_parts[3],
        start_parts[4],
    )


def solution(mesh):
    placed = (
        P("batch", "seq", None),
        P(),
        P(),
        P(),
        P(),
        P(),
        P(),
        P(),
        P(),
        P(),
        P(),
        P(),
        P(),
        P(),
        P(),
        P(),
        P(),
        P(),
        P(),
        P(None, "batch"),
        P(None, "batch"),
        P(None, "batch"),
        P(None, "batch"),
        P(None, "batch"),
        P("batch", "seq", None),
    )
    return jax.shard_map(
        local if fits(mesh) else local_plain,
        mesh=mesh,
        in_specs=placed,
        out_specs=(
            P("batch", "seq", None),
            P("batch", "seq", None),
            P("seq", "batch"),
            P("seq", "batch"),
            P("seq", "batch"),
            P("seq", "batch"),
            P("seq", "batch"),
            P("seq", "batch"),
            P("seq", "batch"),
            P("seq"),
            P("seq"),
            P("seq"),
            P("seq"),
            P("seq"),
            P("seq"),
            P("seq"),
            P("seq"),
            P("seq"),
            P("seq"),
            P("seq"),
            P("seq", "batch"),
            P("seq", "batch"),
            P("seq", "batch"),
            P("seq", "batch"),
            P("seq", "batch"),
        ),
        check_vma=False,
    )
```

```python
import functools
from functools import partial

import jax
import jax.numpy as jnp
from jax import lax
from jax.experimental import pallas as pl
from jax.experimental.pallas import tpu as pltpu
from jax.sharding import PartitionSpec as P

MESH = pl.DeviceIdType.MESH
F32 = jnp.float32
BF = jnp.bfloat16
NS = 8
T = 512
D = 1024
SUB = T // 8

NZ = 4
NM = 13
NK = 2 * NM
WIN = 12
WINF = 4
RA = 48
RE = 128 - RA
LAGS = [3, 5, 4, 5, 6, 6, 7, 8, 8]
RETIRE = 9


def normalize(v, gain, bias):
    mean = jnp.mean(v, axis=-1, keepdims=True)
    cen = v - mean
    var = jnp.mean(cen * cen, axis=-1, keepdims=True)
    return cen * lax.rsqrt(var + 1e-5) * gain + bias


def step_weights(delta):
    e = jnp.exp(-jnp.abs(delta))
    up = delta >= 0
    return jnp.where(up, 1.0, e), jnp.where(up, e, 1.0)


def join(early, late, span):
    em, en, ed = early
    lm, ln, ld = late
    a, b = step_weights(em + span - lm)
    return jnp.maximum(em + span, lm), a * en + b * ln, a * ed + b * ld


def contract0(a, b):
    return lax.dot_general(a, b, (((0,), (0,)), ((), ())), preferred_element_type=F32)


def contract1(a, b):
    return lax.dot_general(a, b, (((1,), (1,)), ((), ())), preferred_element_type=F32)


def pick(m, table):
    out = jnp.int32(table[0])
    for i, v in enumerate(table[1:], 1):
        out = jnp.where(m == i, v, out)
    return out


LEFT = (0, 9, 1, 9, 2, 9, 3, 9, 10, 4, 5, 8, 7)
RIGHT = (8, 4, 8, 5, 8, 6, 8, 7, 0, 1, 2, 3, 6)


class Place:
    def __init__(self):
        self.s, self.b = lax.axis_index("seq"), lax.axis_index("batch")
        self.z, self.x = self.s // 2, self.s % 2
        self.y, self.c = self.b // 2, self.b % 2

    def at(self, z=None, x=None, y=None, c=None):
        z = self.z if z is None else z
        x = self.x if x is None else x
        y = self.y if y is None else y
        c = self.c if c is None else c
        return (z * 2 + x, y * 2 + c)


def rcopy(src, dst, ss, rs, dev):
    return pltpu.make_async_remote_copy(src_ref=src, dst_ref=dst, send_sem=ss, recv_sem=rs, device_id=dev, device_id_type=MESH)


def block_kernel(*refs):
    x_h, cot_h, wk_h, wv_h, wr_h, wo_h, wfk_h, wfv_h, wfr_h = refs[:9]
    (g1, b1, mk, mv, mr, td, tf, g2, b2, fmk, fmr, sn, sd, sm, pa, pf) = refs[9:25]
    o_blk, o_inp = refs[25:27]
    outs = refs[27:34]
    sm_out = refs[34]
    kin_h, vin_h, rin_h, gat_h, k_h, v_h, r_h, mix_h, m_h, n_h, d_h = refs[35:46]
    (ob, wbuf, Y, G, V, K, X, lanes, lanes2, st, sums, RS, es, er, fs, fr, ws, wr, edges, as_, ar, bs_, br_, us, ur,
     acc, sbuf, rF, rSA, rSE, rZA, rZE, smb, smr,
     obsem, wsem, stsem, bigsem, outsem, spsem, esem, fsem, asem, bsem, wssem, wrsem, ussem, ursem,
     s0s, s0r, sFs, sFr, sSs, sSr, sZs, sZr, osem, msem, mss, msr) = refs[46:]
    me = Place()
    z, x, y, c, s = me.z, me.x, me.y, me.c, me.s
    left, right = (jnp.maximum(s - 1, 0), me.b), (jnp.minimum(s + 1, NS - 1), me.b)

    bar = pltpu.get_barrier_semaphore()

    def sig(dev):
        pl.semaphore_signal(bar, inc=1, device_id=dev, device_id_type=MESH)

    sig(me.at(c=1 - c))
    sig(me.at(y=1 - y))
    for i in range(1, NS):
        sig((lax.rem(s + i, NS), me.b))

    def local(src, dst, sem):
        return pltpu.make_async_copy(src, dst, sem)

    def op_load(src, slot):
        return local(src, ob.at[slot], obsem.at[slot])

    def slab_columns(src, j, dst, sem):
        return [local(src.at[:, pl.ds(i * 512 + j * 128, 128)], dst.at[:, pl.ds(i * 128, 128)], sem) for i in range(8)]

    def slab_rows(src, j, dst, sem):
        return [local(src.at[pl.ds(i * 512 + j * 128, 128), :], dst.at[pl.ds(i * 128, 128), :], sem) for i in range(8)]

    weights = [("p", wk_h), ("p", wv_h), ("p", wr_h), ("p", wo_h), ("p", wfr_h)]
    for j in range(4):
        weights += [("c", wfk_h, j), ("r", wfv_h, j)]
    weights += [("p", wfr_h), ("p", wo_h), ("p", wr_h), ("p", wv_h), ("p", wk_h)]

    def w_start(i):
        if i >= len(weights):
            return
        kind, src, *j = weights[i]
        dst, sem = wbuf.at[i % 3], wsem.at[i % 3]
        if kind == "p":
            local(src, dst, sem).start()
        else:
            for cp in (slab_columns if kind == "c" else slab_rows)(src, j[0], dst, sem):
                cp.start()

    def w_wait(i):
        local(wo_h, wbuf.at[i % 3], wsem.at[i % 3]).wait()

    def fs_of(k):
        h = lax.rem(k, 2)
        return jnp.where(h == 0, x, y), jnp.where(h == 0, y, x)

    def partner(h):
        a, b = me.at(x=1 - x), me.at(y=1 - y)
        return (jnp.where(h == 0, a[0], b[0]), jnp.where(h == 0, a[1], b[1]))

    def copy0(k):
        return rcopy(sbuf.at[lax.rem(k, 2)], acc.at[lax.rem(k, WIN)], s0s.at[k], s0r.at[k], me.at(c=1 - c))

    def copyF(k):
        f, _ = fs_of(k)
        return rcopy(acc.at[lax.rem(k, WIN), 1 - f], rF.at[lax.rem(k, WINF)], sFs.at[k], sFr.at[k], partner(lax.rem(k, 2)))

    def copySA(k):
        f, g = fs_of(k)
        w = lax.rem(k, WIN)
        return rcopy(acc.at[w, f, 1 - g, :, pl.ds(0, RA)], rSA.at[w], sSs.at[k, 0], sSr.at[k, 0], partner(1 - lax.rem(k, 2)))

    def copySE(k):
        f, g = fs_of(k)
        w = lax.rem(k, WIN)
        return rcopy(acc.at[w, f, 1 - g, z, pl.ds(RA, RE)], rSE.at[w], sSs.at[k, 1], sSr.at[k, 1], partner(1 - lax.rem(k, 2)))

    def unit(k, q, late):
        f, g = fs_of(k)
        w = lax.rem(k, WIN)
        return acc.at[w, f, g, q, pl.ds(0, RA)] if late else acc.at[w, f, :, q, pl.ds(RA, RE)]

    def zbuf(k, slot, late):
        return (rZA if late else rZE).at[lax.rem(k, WIN), slot]

    def copyR(k, q, late):
        i = int(late)
        return rcopy(unit(k, q, late), zbuf(k, q + 1, late), sZs.at[k, i, q], sZr.at[k, i, q + 1], me.at(z=z + 1))

    def copyL(k, q, late):
        i = int(late)
        return rcopy(unit(k, q, late), zbuf(k, q, late), sZs.at[k, i, q], sZr.at[k, i, q], me.at(z=z - 1))

    def add_into(dst, src):
        dst[...] = dst[...] + src[...]

    def zsub(k, tau, late):
        @pl.when(z <= tau)
        def _():
            q = NZ - 1 - tau + z

            @pl.when(z > 0)
            def _():
                copyR(k, q, late).wait_recv()
                add_into(unit(k, q, late), zbuf(k, q + 1, late))

            copyR(k, q, late).start()

        @pl.when(NZ - 1 - z <= tau)
        def _():
            q = tau - (NZ - 1 - z)

            @pl.when(z < NZ - 1)
            def _():
                copyL(k, q, late).wait_recv()
                add_into(unit(k, q, late), zbuf(k, q, late))

            copyL(k, q, late).start()

    def zfin(k, late):
        @pl.when(z > 0)
        def _():
            copyR(k, z, late).wait_recv()
            add_into(unit(k, z, late), zbuf(k, z + 1, late))

        @pl.when(z < NZ - 1)
        def _():
            copyL(k, z, late).wait_recv()
            add_into(unit(k, z, late), zbuf(k, z, late))

    def gradient(k, core, write):
        h, m = lax.rem(k, 2), k // 2
        ls, rs = pick(m, LEFT), pick(m, RIGHT)
        cols = jnp.concatenate(
            [ob[rs, :, pl.ds(pl.multiple_of((2 * yy + core) * 256 + h * 128, 128), 128)] for yy in range(2)], axis=1)

        def group(g, _):
            res = contract0(ob[ls, :, pl.ds(pl.multiple_of(g * 512, 512), 512)], cols)
            for i in range(4):
                zz, xx = g * 2 + i // 2, i % 2
                for yy in range(2):
                    f = jnp.where(h == 0, xx, yy)
                    g2_ = jnp.where(h == 0, yy, xx)
                    write(f, g2_, zz, res[i * 128:(i + 1) * 128, yy * 128:(yy + 1) * 128])
            return 0

        lax.fori_loop(0, 2, group, 0)

    def taskP(k):
        @pl.when(k >= 2)
        def _():
            copy0(k - 2).wait_send()

        slot = lax.rem(k, 2)

        def write(f, g, zz, v):
            sbuf[slot, f, g, zz] = v

        gradient(k, 1 - c, write)
        copy0(k).start()

    def task1(k):
        copy0(k).wait_recv()
        w = lax.rem(k, WIN)

        def write(f, g, zz, v):
            acc[w, f, g, zz] = acc[w, f, g, zz] + v

        gradient(k, c, write)
        copyF(k).start()

    def task2(k):
        copyF(k).wait_recv()
        f, _ = fs_of(k)
        w = lax.rem(k, WIN)

        def body(i, _):
            add_into(acc.at[w, f, i // NZ, lax.rem(i, NZ)], rF.at[lax.rem(k, WINF), i // NZ, lax.rem(i, NZ)])
            return 0

        lax.fori_loop(0, 2 * NZ, body, 0)
        copySA(k).start()
        zsub(k, 0, False)

    def taskSA(k):
        copySA(k).wait_recv()
        f, g = fs_of(k)
        w = lax.rem(k, WIN)
        add_into(acc.at[w, f, g, :, pl.ds(0, RA)], rSA.at[w])
        zsub(k, 0, True)

    def taskFinE(k):
        zfin(k, False)
        copySE(k).start()

    def taskSE(k):
        copySE(k).wait_recv()
        f, g = fs_of(k)
        w = lax.rem(k, WIN)
        add_into(acc.at[w, f, g, z, pl.ds(RA, RE)], rSE.at[w])
        src = acc.at[w, f, g, z]
        h, m = lax.rem(k, 2), k // 2
        half = pl.ds(pl.multiple_of(h * 128, 128), 128)
        for j in range(4):
            @pl.when(m == 2 * j)
            def _(j=j):
                local(src, outs[5].at[pl.ds(j * 128, 128), half], osem.at[k]).start()

            @pl.when(m == 2 * j + 1)
            def _(j=j):
                local(src, outs[4].at[:, pl.ds(pl.multiple_of(h * 512 + j * 128, 128), 128)], osem.at[k]).start()
        for mm, i in ((8, 6), (9, 3), (10, 2), (11, 1), (12, 0)):
            @pl.when(m == mm)
            def _(i=i):
                local(src, outs[i].at[:, half], osem.at[k]).start()

    def retire(k):
        copyF(k).wait_send()
        copySA(k).wait_send()
        copySE(k).wait_send()
        for late in (False, True):
            for q in range(NZ):
                @pl.when(q != z)
                def _(q=q, late=late):
                    rcopy(unit(k, q, late), zbuf(k, q, late), sZs.at[k, int(late), q], sZr.at[k, int(late), q], me.at(c=1 - c)).wait_send()
        local(acc.at[lax.rem(k, WIN), 0, 0, 0], outs[0].at[:, pl.ds(0, 128)], osem.at[k]).wait()

    stages = [
        (RETIRE, retire),
        (LAGS[7], lambda k: zfin(k, True)),
        (LAGS[8], taskSE),
        (LAGS[6], lambda k: zsub(k, 2, True)),
        (LAGS[5], lambda k: zsub(k, 1, True)),
        (LAGS[4], taskFinE),
        (LAGS[3], lambda k: zsub(k, 2, False)),
        (LAGS[2], lambda k: zsub(k, 1, False)),
        (LAGS[1], taskSA),
        (LAGS[0], task2),
        (1, task1),
        (0, taskP),
    ]

    def sm_copy(step):
        if step == 0:
            return rcopy(smb.at[0], smr.at[0], mss.at[0], msr.at[0], me.at(c=1 - c))
        if step == 1:
            return rcopy(smb.at[2], smr.at[1], mss.at[1], msr.at[1], me.at(y=1 - y))
        return rcopy(smb.at[1, 1 - x], smr.at[2, 0], mss.at[2], msr.at[2], me.at(x=1 - x))

    def sm_z(q, to_right):
        if to_right:
            return rcopy(smb.at[1, x, q], smr.at[3, 0, q], mss.at[3 + q], msr.at[3 + q], me.at(z=z + 1))
        return rcopy(smb.at[1, x, q], smr.at[3, 1, q], mss.at[3 + q], msr.at[3 + NZ + q], me.at(z=z - 1))

    vec = lax.broadcasted_iota(jnp.int32, (2, NZ, 16, 128), 2) < 11

    def sm1():
        sm_copy(0).wait_recv()
        smb[2] = smb[0] + jnp.where(vec, smr[0], 0.0)
        sm_copy(1).start()

    def sm2():
        sm_copy(1).wait_recv()
        smb[1] = smb[2] + jnp.where(vec, smr[1], 0.0)
        sm_copy(2).start()

    def sm3():
        sm_copy(2).wait_recv()
        smb[1, x] = smb[1, x] + smr[2, 0]

    def smz(tau):
        @pl.when(z <= tau)
        def _():
            q = NZ - 1 - tau + z

            @pl.when(z > 0)
            def _():
                sm_z(q, True).wait_recv()
                smb[1, x, q] = smb[1, x, q] + smr[3, 0, q]

            sm_z(q, True).start()

        @pl.when(NZ - 1 - z <= tau)
        def _():
            q = tau - (NZ - 1 - z)

            @pl.when(z < NZ - 1)
            def _():
                sm_z(q, False).wait_recv()
                smb[1, x, q] = smb[1, x, q] + smr[3, 1, q]

            sm_z(q, False).start()

    def sm_fin():
        @pl.when(z > 0)
        def _():
            sm_z(z, True).wait_recv()
            smb[1, x, z] = smb[1, x, z] + smr[3, 0, z]

        @pl.when(z < NZ - 1)
        def _():
            sm_z(z, False).wait_recv()
            smb[1, x, z] = smb[1, x, z] + smr[3, 1, z]

        local(smb.at[1, x, z], sm_out, msem).start()

    def tiles(n, rows, body):
        def step(i, _):
            body(i, pl.ds(pl.multiple_of(i * rows, rows), rows))
            return 0

        lax.fori_loop(0, n, step, 0)

    def widen(slot):
        def body(i, rows):
            for g in range(8):
                lanes[g, rows, :] = ob[slot, rows, g * 128:g * 128 + 128].astype(F32)

        tiles(T // 64, 64, body)

    def spread(i, count):
        return jnp.concatenate(
            [jnp.concatenate([lanes[g, pl.ds(i * count + a, 8, stride=SUB), :] for g in range(8)], axis=1) for a in range(count)], axis=0)

    def unspread(i, count, value):
        for a in range(count):
            for g in range(8):
                lanes2[g, pl.ds(i * count + a, 8, stride=SUB), :] = value[a * 8:a * 8 + 8, g * 128:g * 128 + 128]

    def narrow(slot, dst, sem):
        def body(i, rows):
            for g in range(8):
                ob[slot, rows, g * 128:g * 128 + 128] = lanes2[g, rows, :].astype(BF)

        tiles(T // 64, 64, body)
        local(ob.at[slot], dst, sem).start()

    def halves(body):
        tiles(2, 512, body)

    def gate_step():
        w_wait(4)

        def mm(i, cols):
            G[:, cols] = jnp.dot(ob[10], wbuf[4 % 3, :, cols], preferred_element_type=F32)

        halves(mm)
        w_start(7)

        def body(i, rows):
            gate = jax.nn.sigmoid(G[rows, :])
            G[rows, :] = gate
            ob[8, rows, :] = (spread(i, 4) * gate).astype(BF)

        tiles(T // 32, 32, body)

    def hid(j):
        w_wait(5 + 2 * j)
        slot = (5 + 2 * j) % 3

        def mm(i, cols):
            up = jnp.maximum(jnp.dot(ob[9], wbuf[slot, :, cols], preferred_element_type=F32), 0.0)
            X[pl.ds(0, T), cols] = up
            ob[j, :, cols] = (up * up).astype(BF)

        halves(mm)

    def gpre(j):
        w_wait(6 + 2 * j)
        slot = (6 + 2 * j) % 3

        def mm(i, cols):
            back = contract1(ob[8], wbuf[slot, cols, :])
            ob[4 + j, :, cols] = (back * 2.0 * X[pl.ds(0, T), cols]).astype(BF)

        halves(mm)

    def gk_step(j):
        slot = (5 + 2 * j) % 3

        def mm(i, cols):
            part = contract1(ob[4 + j], wbuf[slot, cols, :])
            K[pl.ds(0, T), cols] = part if j == 0 else K[pl.ds(0, T), cols] + part

        halves(mm)
        w_start(5 + 2 * j + 3)

    def ffv(j):
        slot = (6 + 2 * j) % 3

        def mm(i, cols):
            part = jnp.dot(ob[j], wbuf[slot, :, cols], preferred_element_type=F32)
            V[pl.ds(0, T), cols] = part if j == 0 else V[pl.ds(0, T), cols] + part

        halves(mm)
        w_start(6 + 2 * j + 3)

    def big_load(src, dst, i):
        return local(src, dst.at[pl.ds(0, T)], bigsem.at[i])

    def block_step():
        def body(i, rows):
            gate, values = G[rows, :], V[rows, :]
            unspread(i, 4, Y[rows, :] + gate * values)
            ob[0, rows, :] = (spread(i, 4) * values * gate * (1.0 - gate)).astype(BF)

        tiles(T // 32, 32, body)
        narrow(5, o_blk, outsem.at[0])

    row8 = lax.broadcasted_iota(jnp.int32, (8, D), 0)

    def tail(buf):
        buf[T:T + 8, :] = jnp.where(row8 == 7, 0.0, pltpu.roll(buf[0:8, :], 7, 0))

    def edge(src, dst, sem, dev):
        return rcopy(src, dst, sem.at[0], sem.at[1], dev)

    def recept_back():
        w_wait(13)

        def mm(i, cols):
            V[pl.ds(0, T), cols] = contract1(ob[0], wbuf[13 % 3, cols, :])

        halves(mm)
        w_start(16)
        tail(K)
        tail(V)
        es[...] = K[0:8, :] * (1.0 - fmk[...]) + V[0:8, :] * (1.0 - fmr[...])

        @pl.when(s > 0)
        def _():
            edge(es, er, esem, left).start()

    def fold(v):
        return v[0:8] + v[8:16] + v[16:24] + v[24:32]

    row32 = lax.broadcasted_iota(jnp.int32, (32, D), 0)

    def centre(v):
        mean = jnp.mean(v, axis=-1, keepdims=True)
        cen = v - mean
        inv = lax.rsqrt(jnp.mean(cen * cen, axis=-1, keepdims=True) + 1e-5)
        return cen * inv, inv

    def ln_back(grad, n, inv, gain):
        h = grad * gain[...]
        return inv * (h - jnp.mean(h, axis=-1, keepdims=True) - n * jnp.mean(h * n, axis=-1, keepdims=True))

    def ln_tile(i, rows, n, gain, bias, parts, arrived, sum_rows, ln_sums):
        later = pl.ds(pl.multiple_of(i * 32 + 8, 8), 32)
        normed = n * gain[...] + bias[...]
        grad = 0.0
        if arrived is not None:
            grad = jnp.where(jnp.logical_and(row32 == 31, i == T // 32 - 1), arrived, 0.0)
        for (buf, w), r in zip(parts, sum_rows):
            now, nxt = buf[rows, :], buf[later, :]
            grad = grad + now * w[...] + nxt * (1.0 - w[...])
            sums[r] = sums[r] + fold(normed * (now - nxt))
        sums[ln_sums[0]] = sums[ln_sums[0]] + fold(grad * n)
        sums[ln_sums[1]] = sums[ln_sums[1]] + fold(grad)
        return grad

    def wait_from_right(cp):
        @pl.when(s < NS - 1)
        def _():
            cp.wait_recv()

    def middle_back(lo, hi):
        arrived = jnp.where(s == NS - 1, 0.0, er[0:1, :]) if hi == T // 32 else None

        def body(i, _):
            rows = pl.ds(pl.multiple_of(i * 32, 32), 32)
            n, inv = centre(Y[rows, :])
            grad = ln_tile(i, rows, n, g2, b2, ((K, fmk), (V, fmr)), arrived, (9, 10), (7, 8))
            gm = spread(i, 4) + ln_back(grad, n, inv, g2)
            G[rows, :] = gm
            ob[1, rows, :] = gm.astype(BF)
            return 0

        lax.fori_loop(lo, hi, body, 0)

    def middle_end():
        for r, buf in ((9, K), (10, V)):
            sums[r, 0:1, :] = sums[r, 0:1, :] - buf[0:1, :] * edges[8:9, :]
        sums[15, 0:1, :] = es[0:1, :]

    def gated_back():
        w_wait(14)

        def mm(i, cols):
            V[pl.ds(0, T), cols] = contract1(ob[1], wbuf[14 % 3, cols, :])

        halves(mm)
        w_start(17)
        big_load(r_h, X, 0).wait()
        big_load(mix_h, K, 1).wait()

        def body(i, rows):
            sg = jax.nn.sigmoid(X[rows, :])
            gg = V[rows, :]
            ob[2, rows, :] = (gg * K[rows, :] * sg * (1.0 - sg)).astype(BF)
            V[rows, :] = gg * sg

        tiles(T // 32, 32, body)

    streams = (k_h, m_h, d_h, n_h, v_h)

    def st_copies(blk, slot, count):
        rows = pl.ds(pl.multiple_of(blk * 64, 64), 64)
        return [local(src.at[rows, :], st.at[slot, i], stsem.at[slot, i]) for i, src in enumerate(streams[:count])]

    def st_start(blk, count):
        for cp in st_copies(blk, lax.rem(blk, 2), count):
            cp.start()

    def st_next(blk, count):
        for cp in st_copies(blk, lax.rem(blk, 2), count):
            cp.wait()

        @pl.when(blk > 0)
        def _():
            st_start(blk - 1, count)

    decay = -jnp.exp(td[...])

    def wide(v, cols):
        return jnp.broadcast_to(v[:, cols], (8, 512))

    def first_pass(lo):
        def block(i, _):
            blk = 7 - lo - i
            slot = lax.rem(blk, 2)
            st_next(blk, 3)
            for h in range(2):
                cols = slice(h * 512, h * 512 + 512)
                w, bonus = wide(decay, cols), wide(tf[...], cols)

                def step(jj, carry):
                    R, S = carry
                    j = 7 - jj
                    at = pl.ds(pl.multiple_of(j * 8, 8), 8)
                    rows = pl.ds(pl.multiple_of(blk * 64 + j * 8, 8), 8)
                    k, m, d = st[slot, 0, at, cols], st[slot, 1, at, cols], st[slot, 2, at, cols]
                    p, u = step_weights(m - (bonus + k))
                    q = V[rows, cols] / (p * d + u)
                    qp = p * q
                    V[rows, cols] = qp
                    X[rows, cols] = u * q
                    a, _ = step_weights(m + w - k)
                    return qp + a * R, qp * K[rows, cols] + a * S

                R, S = lax.fori_loop(0, 8, step, (RS[0, :, cols], RS[1, :, cols]), unroll=2)
                RS[0, :, cols] = R
                RS[1, :, cols] = S

                @pl.when(blk == 7)
                def _():
                    RS[2, :, cols] = jnp.maximum(st[slot, 1, 56:64, cols] + w, st[slot, 0, 56:64, cols])

                @pl.when(blk == 0)
                def _():
                    RS[3, :, cols] = st[slot, 1, 0:8, cols]
            return 0

        lax.fori_loop(0, 4, block, 0)

    def suffix(value, dist, fill):
        return jnp.where(row8 >= 8 - dist, fill, pltpu.roll(value, 8 - dist, 0))

    span = SUB * decay

    def state_copy(src, dst):
        return rcopy(ws, wr.at[src], wssem.at[dst], wrsem.at[src], (dst, me.b))

    def first_end():
        A = jnp.exp(jnp.minimum(RS[3] + span - RS[2], 0.0))
        R, S = RS[0], RS[1]
        for dist in (1, 2, 4):
            R = R + A * suffix(R, dist, 0.0)
            S = S + A * suffix(S, dist, 0.0)
            A = A * suffix(A, dist, 1.0)
        RS[0], RS[1], RS[4] = R, S, A
        ws[...] = jnp.where(row8 == 0, R[0:1], jnp.where(row8 == 1, S[0:1], RS[3, 0:1, :]))
        for i in range(NS - 1):
            @pl.when(i < s)
            def _(i=i):
                state_copy(s, i).start()

    def second_start():
        RS[5] = jnp.zeros((8, D), F32)
        RS[6] = jnp.zeros((8, D), F32)
        for i in range(1, NS):
            @pl.when(i > s)
            def _(i=i):
                state_copy(i, 0).wait_recv()
                far = jnp.exp(jnp.minimum(RS[2, 7:8, :] + (i - s - 1).astype(F32) * (8.0 * span) - wr[i, 2:3, :], 0.0))
                RS[5, 0:1, :] = RS[5, 0:1, :] + far * wr[i, 0:1, :]
                RS[6, 0:1, :] = RS[6, 0:1, :] + far * wr[i, 1:2, :]
        Rin, Sin = RS[5, 0:1, :], RS[6, 0:1, :]
        A = RS[4]
        R = RS[0] + A * Rin
        S = RS[1] + A * Sin
        RS[0] = jnp.where(row8 == 7, Rin, pltpu.roll(R, 7, 0))
        RS[1] = jnp.where(row8 == 7, Sin, pltpu.roll(S, 7, 0))

    def second_pass(lo, n):
        def block(i, _):
            blk = 7 - lo - i
            slot = lax.rem(blk, 2)
            st_next(blk, 5)
            for h in range(2):
                cols = slice(h * 512, h * 512 + 512)
                w = wide(decay, cols)

                def one(j, carry):
                    R, S, first, slow = carry
                    at = pl.ds(pl.multiple_of(j * 8, 8), 8)
                    rows = pl.ds(pl.multiple_of(blk * 64 + j * 8, 8), 8)
                    k, m, d, n_, v = (st[slot, q, at, cols] for q in range(5))
                    mixed, qp, uq = K[rows, cols], V[rows, cols], X[rows, cols]
                    a, b = step_weights(m + w - k)
                    own = uq * (v - mixed)
                    gv = uq + b * R
                    gk = own + b * (v * R - S)
                    first = first + own
                    slow = slow + a * (n_ * R - d * S)
                    return (qp + a * R, qp * mixed + a * S, first, slow), gk, gv

                def step(jj, carry):
                    j = 3 - jj
                    carry, gk1, gv1 = one(2 * j + 1, carry)
                    carry, gk0, gv0 = one(2 * j, carry)
                    pair = pl.ds(pl.multiple_of(blk * 64 + j * 16, 16), 16)
                    ob[6, pair, cols] = jnp.concatenate([gk0, gk1], axis=0).astype(BF)
                    ob[3, pair, cols] = jnp.concatenate([gv0, gv1], axis=0).astype(BF)
                    return carry

                R, S, first, slow = lax.fori_loop(0, 4, step, (RS[0, :, cols], RS[1, :, cols], sums[6, :, cols], sums[5, :, cols]))
                RS[0, :, cols] = R
                RS[1, :, cols] = S
                sums[6, :, cols] = first
                sums[5, :, cols] = slow
            return 0

        lax.fori_loop(0, n, block, 0)

    def second_end():
        gn, gd = RS[0, 0:1, :], -RS[1, 0:1, :]
        sums[11, 0:1, :] = gn
        sums[12, 0:1, :] = gd
        sums[13, 0:1, :] = sn[...] * gn + sd[...] * gd
        sums[5] = sums[5] * decay

    def input_mm(i, slot, buf):
        w_wait(i)

        def mm(_, cols):
            buf[pl.ds(0, T), cols] = contract1(ob[slot], wbuf[i % 3, cols, :])

        halves(mm)
        tail(buf)

    def input_edge():
        fs[...] = K[0:8, :] * (1.0 - mk[...]) + V[0:8, :] * (1.0 - mv[...]) + X[0:8, :] * (1.0 - mr[...])

        @pl.when(s > 0)
        def _():
            edge(fs, fr, fsem, left).start()

    def input_back(lo, hi):
        arrived = jnp.where(s == NS - 1, 0.0, fr[0:1, :]) if hi == T // 32 else None

        def body(i, _):
            rows = pl.ds(pl.multiple_of(i * 32, 32), 32)
            n, inv = centre(spread(i, 4))
            grad = ln_tile(i, rows, n, g1, b1, ((K, mk), (V, mv), (X, mr)), arrived, (2, 3, 4), (0, 1))
            unspread(i, 4, G[rows, :] + ln_back(grad, n, inv, g1))
            return 0

        lax.fori_loop(lo, hi, body, 0)

    def input_end():
        for r, buf in ((2, K), (3, V), (4, X)):
            sums[r, 0:1, :] = sums[r, 0:1, :] - buf[0:1, :] * edges[0:1, :]
        sums[14, 0:1, :] = fs[0:1, :]
        narrow(0, o_inp, outsem.at[1])
        alone = jnp.where(s == 0, 1.0, 0.0)
        rows = [jnp.sum(sums[r], axis=0, keepdims=True) for r in range(11)] + [jnp.where(s == 0, sums[r, 0:1, :], 0.0) for r in range(11, 16)]
        table = jnp.concatenate(rows, axis=0)
        for g in range(8):
            smb[0, g % 2, g // 2] = table[:, g * 128:g * 128 + 128]
        sm_copy(0).start()

    def start_all(*copies):
        for cp in copies:
            cp.start()

    compute = {
        0: [lambda: gpre(0)],
        1: [lambda: gk_step(0), lambda: hid(1)],
        2: [lambda: ffv(0), lambda: gpre(1)],
        3: [lambda: gk_step(1), lambda: hid(2)],
        4: [lambda: ffv(1), lambda: gpre(2)],
        5: [lambda: gk_step(2), lambda: hid(3), lambda: start_all(op_load(gat_h, 4))],
        6: [lambda: ffv(2), lambda: gpre(3)],
        7: [lambda: gk_step(3), lambda: ffv(3)],
        8: [block_step],
        9: [recept_back],
        10: [lambda: middle_back(0, 8)],
        11: [lambda: start_all(big_load(r_h, X, 0)), lambda: wait_from_right(edge(es, er, esem, left)), lambda: middle_back(8, 16), middle_end,
             lambda: start_all(big_load(mix_h, K, 1)), lambda: st_start(7, 3),
             lambda: local(ob.at[5], o_blk, outsem.at[0]).wait(), lambda: start_all(op_load(rin_h, 5))],
        12: [gated_back],
        13: [lambda: first_pass(0)],
        14: [lambda: first_pass(4), first_end, lambda: st_start(7, 5)],
        15: [second_start, lambda: second_pass(0, 2), lambda: start_all(op_load(vin_h, 8))],
        16: [lambda: second_pass(2, 3)],
        17: [lambda: second_pass(5, 3), second_end, lambda: start_all(op_load(kin_h, 7), op_load(x_h, 9))],
        18: [lambda: input_mm(15, 2, X), lambda: input_mm(16, 3, V)],
        19: [lambda: input_mm(17, 6, K), input_edge, lambda: op_load(x_h, 9).wait(), lambda: widen(9)],
        20: [lambda: input_back(0, 8)],
        21: [lambda: wait_from_right(edge(fs, fr, fsem, left)), lambda: input_back(8, 16), input_end],
        23: [sm1],
        24: [sm2],
        25: [sm3, lambda: smz(0)],
        27: [lambda: smz(1)],
        29: [lambda: smz(2)],
        31: [sm_fin],
    }
    landed = {18: (gat_h, 4), 20: (rin_h, 5), 22: (vin_h, 8), 24: (kin_h, 7)}

    def spill(src, dst, i):
        return local(src, dst, spsem.at[i])

    kb, vb, rb, nb = G, V, X, K
    to_next = rcopy(as_, ar, asem.at[0], asem.at[1], right)
    to_next2 = rcopy(bs_, br_, bsem.at[0], bsem.at[1], right)

    def wait_from_left(cp):
        @pl.when(s > 0)
        def _():
            cp.wait_recv()

    def send_right(cp):
        @pl.when(s < NS - 1)
        def _():
            cp.start()

    def norm1(j, _):
        rows = pl.ds(pl.multiple_of(j * 8, 8), 8)
        v = spread(j, 1)
        Y[rows, :] = v
        nb[pl.ds(pl.multiple_of(j * 8 + 8, 8), 8), :] = normalize(v, g1[...], b1[...])
        return 0

    def header(start_row):
        nb[0:8, :] = jnp.where(row8 == 0, start_row, pltpu.roll(nb[T:T + 8, :], 1, 0))

    def mix(pairs, i):
        rows = pl.ds(pl.multiple_of(i * 32, 32), 32)
        before = nb[rows, :]
        now = nb[pl.ds(pl.multiple_of(i * 32 + 8, 8), 32), :]
        for slot, w in pairs:
            ob[slot, rows, :] = (now * w[...] + before * (1.0 - w[...])).astype(BF)

    def project(i, slot, dst):
        w_wait(i)
        dst[pl.ds(0, T), :] = jnp.dot(ob[slot], wbuf[i % 3], preferred_element_type=F32)
        w_start(i + 3)

    start_all(op_load(x_h, 4), op_load(cot_h, 5))
    for i in range(3):
        w_start(i)
    op_load(x_h, 4).wait()
    as_[...] = normalize(ob[4, T - 16:T, :].astype(F32), g1[...], b1[...])[8:16, :]
    pl.semaphore_wait(bar, NS + 1)
    send_right(to_next)
    widen(4)
    lax.fori_loop(0, SUB, norm1, 0, unroll=4)
    wait_from_left(to_next)
    header(jnp.where(s == 0, pa[...], ar[7:8, :]))
    edges[0:8, :] = nb[0:8, :]
    tiles(T // 32, 32, lambda i, rows: mix(((0, mk), (1, mv), (2, mr)), i))
    start_all(spill(ob.at[0], kin_h, 0), spill(ob.at[1], vin_h, 1), spill(ob.at[2], rin_h, 2))
    project(0, 0, kb)
    project(1, 1, vb)
    start_all(spill(kb, k_h, 3), spill(vb.at[pl.ds(0, T)], v_h, 4))

    def own_state(h):
        cols = slice(h * 512, h * 512 + 512)
        w = wide(decay, cols)

        def step(j, state):
            rows = pl.ds(pl.multiple_of(j * 8, 8), 8)
            m, n, d = state
            k, v = kb[rows, cols], vb[rows, cols]
            low = m + w
            a, b = step_weights(low - k)
            return jnp.maximum(low, k), a * n + b * v, a * d + b

        return lax.fori_loop(1, SUB, step, (kb[0:8, cols], vb[0:8, cols], jnp.ones((8, 512), F32)), unroll=3)

    parts = [own_state(h) for h in range(2)]
    total = tuple(jnp.concatenate([parts[0][i], parts[1][i]], axis=1) for i in range(3))

    def earlier(state, dist):
        m, n, d = (pltpu.roll(p, dist, 0) for p in state)
        out = row8 < dist
        return jnp.where(out, -1e30, m), jnp.where(out, 0.0, n), jnp.where(out, 0.0, d)

    for dist in (1, 2, 4):
        total = join(earlier(total, dist), total, dist * span)
    before_own = earlier(total, 1)
    us[...] = jnp.where(row8 == 0, total[0][7:8], jnp.where(row8 == 1, total[1][7:8], total[2][7:8]))

    def reach_copy(src, dst):
        return rcopy(us, ur.at[src], ussem.at[dst], ursem.at[src], (dst, me.b))

    for i in range(1, NS):
        @pl.when(s < i)
        def _(i=i):
            reach_copy(s, i).start()

    project(2, 2, rb)
    start_all(spill(rb.at[pl.ds(0, T)], r_h, 5))
    op_load(cot_h, 5).wait()
    widen(5)
    RS[0, 0:1, :] = sm[...]
    RS[1, 0:1, :] = sn[...]
    RS[2, 0:1, :] = sd[...]
    for i in range(NS - 1):
        @pl.when(i < s)
        def _(i=i):
            reach_copy(i, NS - 1).wait_recv()
            now = join(tuple(RS[r, 0:1, :] for r in range(3)), tuple(ur[i, r:r + 1, :] for r in range(3)), 8.0 * span)
            for r in range(3):
                RS[r, 0:1, :] = now[r]

    base = tuple(RS[r, 0:1, :] for r in range(3))
    lifted = (base[0] + row8.astype(F32) * span, jnp.broadcast_to(base[1], (8, D)), jnp.broadcast_to(base[2], (8, D)))
    for r, v in enumerate(join(lifted, before_own, 0.0)):
        RS[r] = v

    def state_spills(blk, slot):
        rows = pl.ds(pl.multiple_of(blk * 64, 64), 64)
        return [local(st.at[slot, q], dst.at[rows, :], stsem.at[slot, q]) for q, dst in enumerate((mix_h, m_h, n_h, d_h))]

    def outputs(blk, _):
        slot = lax.rem(blk, 2)

        @pl.when(blk >= 2)
        def _():
            for cp in state_spills(blk - 2, slot):
                cp.wait()

        for h in range(2):
            cols = slice(h * 512, h * 512 + 512)
            w, bonus = wide(decay, cols), wide(tf[...], cols)

            def one(j, state):
                at = pl.ds(pl.multiple_of(j * 8, 8), 8)
                rows = pl.ds(pl.multiple_of(blk * 64 + j * 8, 8), 8)
                m, n, d = state
                k, v = kb[rows, cols], vb[rows, cols]
                p, u = step_weights(m - (bonus + k))
                mixed = (p * n + u * v) / (p * d + u)
                for q, val in enumerate((mixed, m, n, d)):
                    st[slot, q, at, cols] = val
                low = m + w
                a, b = step_weights(low - k)
                return (jnp.maximum(low, k), a * n + b * v, a * d + b), jax.nn.sigmoid(rb[rows, cols]) * mixed

            def two(i, state):
                state, ga = one(2 * i, state)
                state, gb = one(2 * i + 1, state)
                ob[3, pl.ds(pl.multiple_of(blk * 64 + i * 16, 16), 16), cols] = jnp.concatenate([ga, gb], axis=0).astype(BF)
                return state

            for r, v in enumerate(lax.fori_loop(0, 4, two, tuple(RS[r, :, cols] for r in range(3)))):
                RS[r, :, cols] = v
        start_all(*state_spills(blk, slot))
        return 0

    lax.fori_loop(0, 8, outputs, 0)
    start_all(spill(ob.at[3], gat_h, 6))
    spill(kb, k_h, 3).wait()
    project(3, 3, G)

    def norm2(i, rows):
        v = Y[rows, :] + G[rows, :]
        Y[rows, :] = v
        nb[pl.ds(pl.multiple_of(i * 32 + 8, 8), 32), :] = normalize(v, g2[...], b2[...])

    norm2(T // 32 - 1, pl.ds(T - 32, 32))
    bs_[...] = nb[T:T + 8, :]
    send_right(to_next2)
    tiles(T // 32 - 1, 32, norm2)

    def mix2(i, _):
        mix(((9, fmk), (10, fmr)), i)
        return 0

    lax.fori_loop(1, T // 32, mix2, 0)
    wait_from_left(to_next2)
    header(jnp.where(s == 0, pf[...], br_[7:8, :]))
    edges[8:16, :] = nb[0:8, :]
    mix2(0, 0)

    sums[...] = jnp.zeros_like(sums)
    gate_step()
    spill(ob.at[0], kin_h, 0).wait()
    spill(rb.at[pl.ds(0, T)], r_h, 5).wait()
    hid(0)
    RS[...] = jnp.zeros_like(RS)
    for i, (src, dst) in enumerate(((ob.at[1], vin_h), (ob.at[2], rin_h))):
        spill(src, dst, 1 + i).wait()
    spill(vb.at[pl.ds(0, T)], v_h, 4).wait()
    spill(ob.at[3], gat_h, 6).wait()
    for blk in (6, 7):
        for cp in state_spills(blk, blk % 2):
            cp.wait()

    def tick(t, _):
        for at, (src, slot) in landed.items():
            @pl.when(t == at)
            def _(src=src, slot=slot):
                op_load(src, slot).wait()

        for lag, task in stages:
            k = t - lag

            @pl.when(jnp.logical_and(k >= 0, k < NK))
            def _(k=k, task=task):
                task(k)

        for at, steps in compute.items():
            @pl.when(t == at)
            def _(steps=steps):
                for step in steps:
                    step()
        return 0

    lax.fori_loop(0, NK + RETIRE, tick, 0)

    copy0(NK - 2).wait_send()
    copy0(NK - 1).wait_send()
    for i in range(3):
        sm_copy(i).wait_send()
    for q in range(NZ):
        @pl.when(q != z)
        def _(q=q):
            sm_z(q, True).wait_send()

    @pl.when(s > 0)
    def _():
        edge(es, er, esem, left).wait_send()
        edge(fs, fr, fsem, left).wait_send()

    @pl.when(s < NS - 1)
    def _():
        to_next.wait_send()
        to_next2.wait_send()

    for i in range(NS):
        @pl.when(i < s)
        def _(i=i):
            state_copy(s, i).wait_send()

        @pl.when(i > s)
        def _(i=i):
            reach_copy(s, i).wait_send()
    local(smb.at[1, x, z], sm_out, msem).wait()
    local(ob.at[0], o_inp, outsem.at[1]).wait()


def block_call(x, cot, mats, vectors, states):
    anyspec = pl.BlockSpec(memory_space=pl.ANY)
    vm = pl.BlockSpec(memory_space=pltpu.VMEM)
    S = jax.ShapeDtypeStruct
    sem = pltpu.SemaphoreType.DMA
    M = pltpu.VMEM
    row = M((8, D), F32)
    return pl.pallas_call(
        block_kernel,
        out_shape=[S((T, D), BF)] * 2 + [S((128, 256), F32)] * 4 + [S((128, 1024), F32), S((512, 256), F32), S((128, 256), F32), S((16, 128), F32)]
        + [S((T, D), BF)] * 4 + [S((T, D), F32)] * 7,
        in_specs=[anyspec] * 9 + [vm] * 16,
        out_specs=[anyspec] * 21,
        scratch_shapes=[
            M((11, T, D), BF), M((3, D, D), BF), M((T, D), F32), M((T, D), F32), M((T + 8, D), F32), M((T + 8, D), F32), M((T + 8, D), F32),
            M((8, T, 128), F32), M((8, T, 128), F32), M((2, 5, 64, D), F32), M((16, 8, D), F32), M((7, 8, D), F32),
            row, row, row, row, row, M((NS, 8, D), F32), M((16, D), F32), row, row, row, row, row, M((NS, 8, D), F32),
            M((WIN, 2, 2, NZ, 128, 128), F32), M((2, 2, 2, NZ, 128, 128), F32), M((WINF, 2, NZ, 128, 128), F32),
            M((WIN, NZ, RA, 128), F32), M((WIN, RE, 128), F32), M((WIN, NZ + 1, RA, 128), F32), M((WIN, NZ + 1, 2, RE, 128), F32),
            M((3, 2, NZ, 16, 128), F32), M((4, 2, NZ, 16, 128), F32),
            sem((11,)), sem((3,)), sem((2, 5)), sem((2,)), sem((2,)), sem((7,)), sem((2,)), sem((2,)), sem((2,)), sem((2,)), sem((NS,)), sem((NS,)), sem((NS,)), sem((NS,)),
            sem((NK,)), sem((NK,)), sem((NK,)), sem((NK,)), sem((NK, 2)), sem((NK, 2)),
            sem((NK, 2, NZ)), sem((NK, 2, NZ + 1)), sem((NK,)), sem, sem((3 + NZ,)), sem((3 + 2 * NZ,)),
        ],
        compiler_params=pltpu.CompilerParams(collective_id=0, has_side_effects=True, vmem_limit_bytes=67043328),
        name="block",
    )(x, cot, *mats, *vectors, *states)[:10]

def finish_kernel(*refs):
    ins, outs, (scratch, sems) = refs[:10], refs[10:35], (refs[35:-2], refs[-2:])
    into, out = sems
    loads = [pltpu.make_async_copy(src, buf, into.at[i]) for i, (src, buf) in enumerate(zip(ins, scratch))]
    for cp in loads:
        cp.start()
    stores = []
    for i in (9, 2, 3, 4, 5, 8, 6, 7, 0, 1):
        loads[i].wait()
        if i < 9:
            stores.append(pltpu.make_async_copy(scratch[i], outs[i], out.at[i]))
            stores[-1].start()
        else:
            for r in range(16):
                stores.append(pltpu.make_async_copy(scratch[i].at[pl.ds(r, 1)], outs[9 + r], out.at[9 + r]))
                stores[-1].start()
    for cp in stores:
        cp.wait()


def finish_call(parts):
    anyspec = pl.BlockSpec(memory_space=pl.ANY)
    return pl.pallas_call(
        finish_kernel,
        out_shape=[jax.ShapeDtypeStruct(p.shape, p.dtype) for p in parts[:9]] + [jax.ShapeDtypeStruct((1, 128), F32)] * 16,
        in_specs=[anyspec] * 10,
        out_specs=[anyspec] * 25,
        scratch_shapes=[pltpu.VMEM(p.shape, p.dtype) for p in parts] + [pltpu.SemaphoreType.DMA((10,)), pltpu.SemaphoreType.DMA((25,))],
        name="finish",
    )(*parts)


def fits(mesh):
    return (mesh.shape["seq"], mesh.shape["batch"]) == (2 * NZ, 4)


def local(
    inputs,
    w_key,
    w_value,
    w_recept,
    w_output,
    w_ffn_key,
    w_ffn_value,
    w_ffn_recept,
    ln1_gain,
    ln1_bias,
    mix_key,
    mix_value,
    mix_recept,
    time_decay,
    time_first,
    ln2_gain,
    ln2_bias,
    ffn_mix_key,
    ffn_mix_recept,
    state_num,
    state_den,
    state_max,
    prev_att,
    prev_ffn,
    cotangent,
):
    rows = inputs.reshape(T, D)
    vectors = [
        v.reshape(1, D)
        for v in (
            ln1_gain,
            ln1_bias,
            mix_key,
            mix_value,
            mix_recept,
            time_decay,
            time_first,
            ln2_gain,
            ln2_bias,
            ffn_mix_key,
            ffn_mix_recept,
        )
    ]
    states = [v.reshape(1, D) for v in (state_num, state_den, state_max, prev_att, prev_ffn)]
    parts = block_call(
        rows,
        cotangent.reshape(T, D),
        [w_key, w_value, w_recept, w_output, w_ffn_key, w_ffn_value, w_ffn_recept],
        vectors,
        states,
    )
    block_out, input_grad, *rest = finish_call(parts)
    return (
        block_out.reshape(inputs.shape),
        input_grad.reshape(inputs.shape),
        *rest[:7],
        *[v.reshape(128) for v in rest[7:18]],
        *[v.reshape(128, 1) for v in rest[18:]],
    )


BLOCK = 64


far_below = -1e30


def from_behind(block, axis, distance):
    devices = range(lax.axis_size(axis))
    route = [(i - distance, i) for i in devices if i - distance in devices]
    return lax.ppermute(block, axis, route)


def prefix(value, axis, join, neutral, backward):
    count, mine = (lax.axis_size(axis), lax.axis_index(axis))
    pieces = jax.tree.map(lambda part: lax.all_gather(part, axis), value)
    if backward:
        pieces = jax.tree.map(lambda part: part[::-1], pieces)
        mine = count - 1 - mine
    total = jax.tree.map(
        lambda part, zero: jnp.full_like(part, 0) + jnp.asarray(zero, part.dtype), value, neutral
    )

    def turn(position, total):
        longer = join(total, jax.tree.map(lambda part: part[position], pieces))
        return jax.tree.map(lambda new, old: jnp.where(position < mine, new, old), longer, total)

    return lax.fori_loop(0, count - 1, turn, total)


def layer_norm(values, ln_gain, ln_bias):
    centred = values - jnp.mean(values, axis=-1, keepdims=True)
    spread = jnp.mean(centred * centred, axis=-1, keepdims=True)
    return centred * lax.rsqrt(spread + 1e-05) * ln_gain + ln_bias


def matmul(operand, matrix):
    return lax.dot_general(
        operand, matrix, (((operand.ndim - 1,), (0,)), ((), ())), preferred_element_type=jnp.float32
    )


def matmul_back(gradient, matrix):
    return lax.dot_general(
        gradient,
        matrix,
        (((gradient.ndim - 1,), (1,)), ((), ())),
        preferred_element_type=jnp.float32,
    )


def outer_sum(operand, gradient):
    flat_operand = operand.reshape(-1, operand.shape[-1])
    flat_gradient = gradient.reshape(-1, gradient.shape[-1])
    return lax.dot_general(
        flat_operand, flat_gradient, (((0,), (0,)), ((), ())), preferred_element_type=jnp.float32
    )


def token_mix(normed, edge_row, mix_vectors):
    earlier = jnp.concatenate([edge_row[:, None, :], normed[:, :-1, :]], axis=1)
    return tuple((normed * member + earlier * (1.0 - member) for member in mix_vectors))


def gate_rows(recept_rows, mixed_rows):
    return jax.nn.sigmoid(recept_rows) * mixed_rows


def wkv_block(decay_rate, time_first, state_in, inputs_now):
    numerator, denominator, running_max = state_in
    key_rows, value_rows = inputs_now
    length = key_rows.shape[1]
    places = jnp.arange(length, dtype=jnp.float32)[None, :, None]
    own_terms = time_first + key_rows
    anchor = jnp.maximum(
        jnp.maximum(running_max, jnp.max(key_rows, axis=1)), jnp.max(own_terms, axis=1)
    )
    scaled = jnp.exp(key_rows - anchor[:, None, :] - (places + 1.0) * decay_rate)
    running_num = jnp.cumsum(scaled * value_rows, axis=1)
    running_den = jnp.cumsum(scaled, axis=1)
    past_num = jnp.concatenate([jnp.zeros_like(running_num[:, :1]), running_num[:, :-1]], axis=1)
    past_den = jnp.concatenate([jnp.zeros_like(running_den[:, :1]), running_den[:, :-1]], axis=1)
    fading = jnp.exp(places * decay_rate)
    carried = jnp.exp(running_max[:, None, :] + places * decay_rate - anchor[:, None, :])
    own_weight = jnp.exp(own_terms - anchor[:, None, :])
    top_num = past_num * fading + own_weight * value_rows + carried * numerator[:, None, :]
    top_den = past_den * fading + own_weight + carried * denominator[:, None, :]
    outputs = top_num / top_den
    final_terms = key_rows + (length - 1.0 - places) * decay_rate
    kept_max = running_max + length * decay_rate
    new_max = jnp.maximum(kept_max, jnp.max(final_terms, axis=1))
    final_weights = jnp.exp(final_terms - new_max[:, None, :])
    kept_weight = jnp.exp(kept_max - new_max)
    new_num = jnp.sum(final_weights * value_rows, axis=1) + kept_weight * numerator
    new_den = jnp.sum(final_weights, axis=1) + kept_weight * denominator
    return ((new_num, new_den, new_max), outputs)


def wkv_local(key_rows, value_rows, time_decay, time_first, in_num, in_den, in_max):
    decay_rate = -jnp.exp(time_decay)
    block_count = key_rows.shape[1] // BLOCK

    def arrange(values):
        return jnp.moveaxis(
            values.reshape(values.shape[0], block_count, BLOCK, values.shape[2]), 1, 0
        )

    block_step = jax.checkpoint(partial(wkv_block, decay_rate, time_first))
    state_out, outputs = lax.scan(
        block_step, (in_num, in_den, in_max), (arrange(key_rows), arrange(value_rows))
    )
    outputs = jnp.moveaxis(outputs, 0, 1).reshape(key_rows.shape)
    return (outputs, state_out)


def local_summary(key_rows, value_rows, decay_rate):
    length = key_rows.shape[1]
    places = jnp.arange(length, dtype=jnp.float32)[None, :, None]
    terms = key_rows + (length - 1.0 - places) * decay_rate
    top_term = jnp.max(terms, axis=1)
    weights_now = jnp.exp(terms - top_term[:, None, :])
    return (jnp.sum(weights_now * value_rows, axis=1), jnp.sum(weights_now, axis=1), top_term)


def combine_states(earlier_one, later_one):
    earlier_num, earlier_den, earlier_max, earlier_span = earlier_one
    later_num, later_den, later_max, later_span = later_one
    shifted_max = earlier_max + later_span
    top_both = jnp.maximum(shifted_max, later_max)
    weight_early = jnp.exp(shifted_max - top_both)
    weight_late = jnp.exp(later_max - top_both)
    return (
        earlier_num * weight_early + later_num * weight_late,
        earlier_den * weight_early + later_den * weight_late,
        top_both,
        earlier_span + later_span,
    )


def combine_grads(earlier_one, later_one):
    earlier_num, earlier_den, earlier_span = earlier_one
    later_num, later_den, later_span = later_one
    factor = jnp.exp(later_span)
    return (
        later_num + factor * earlier_num,
        later_den + factor * earlier_den,
        earlier_span + later_span,
    )


def local_plain(
    inputs,
    w_key,
    w_value,
    w_recept,
    w_output,
    w_ffn_key,
    w_ffn_value,
    w_ffn_recept,
    ln1_gain,
    ln1_bias,
    mix_key,
    mix_value,
    mix_recept,
    time_decay,
    time_first,
    ln2_gain,
    ln2_bias,
    ffn_mix_key,
    ffn_mix_recept,
    state_num,
    state_den,
    state_max,
    prev_att,
    prev_ffn,
    cotangent,
):
    position = lax.axis_index("seq")
    is_first = position == 0
    start_num = state_num.T
    start_den = state_den.T
    start_max = state_max.T
    before_att = prev_att.T
    before_ffn = prev_ffn.T
    input_rows = inputs.astype(jnp.float32)
    normed, norm_pull = jax.vjp(layer_norm, input_rows, ln1_gain, ln1_bias)
    from_left = from_behind(normed[:, -1, :], "seq", 1)
    edge_att = jnp.where(is_first, before_att, from_left)
    mixed_inputs, mix_pull = jax.vjp(token_mix, normed, edge_att, (mix_key, mix_value, mix_recept))
    key_in = mixed_inputs[0].astype(jnp.bfloat16)
    value_in = mixed_inputs[1].astype(jnp.bfloat16)
    recept_in = mixed_inputs[2].astype(jnp.bfloat16)
    key_rows = matmul(key_in, w_key)
    value_rows = matmul(value_in, w_value)
    recept_rows = matmul(recept_in, w_recept)
    decay_rate = -jnp.exp(time_decay)
    local_len = key_rows.shape[1]
    device_span = jnp.broadcast_to(local_len * decay_rate, start_num.shape)
    own_num, own_den, own_max = local_summary(key_rows, value_rows, decay_rate)
    first_element = combine_states(
        (start_num, start_den, start_max, jnp.zeros_like(device_span)),
        (own_num, own_den, own_max, device_span),
    )
    element_num = jnp.where(is_first, first_element[0], own_num)
    element_den = jnp.where(is_first, first_element[1], own_den)
    element_max = jnp.where(is_first, first_element[2], own_max)
    zero_rows = jnp.zeros_like(start_num)
    identity = (zero_rows, zero_rows, jnp.full_like(start_num, far_below), zero_rows)
    incoming = prefix(
        (element_num, element_den, element_max, device_span), "seq", combine_states, identity, False
    )
    prior_num, prior_den, prior_max = (incoming[0], incoming[1], incoming[2])
    in_num = jnp.where(is_first, start_num, prior_num)
    in_den = jnp.where(is_first, start_den, prior_den)
    in_max = jnp.where(is_first, start_max, prior_max)
    (mixed_rows, state_out), wkv_pull = jax.vjp(
        wkv_local, key_rows, value_rows, time_decay, time_first, in_num, in_den, in_max
    )
    gated, gate_pull = jax.vjp(gate_rows, recept_rows, mixed_rows)
    gated_low = gated.astype(jnp.bfloat16)
    attended = matmul(gated_low, w_output)
    middle = input_rows + attended
    normed_ffn, norm_ffn_pull = jax.vjp(layer_norm, middle, ln2_gain, ln2_bias)
    from_left_ffn = from_behind(normed_ffn[:, -1, :], "seq", 1)
    edge_ffn = jnp.where(is_first, before_ffn, from_left_ffn)
    ffn_inputs, ffn_mix_pull = jax.vjp(
        token_mix, normed_ffn, edge_ffn, (ffn_mix_key, ffn_mix_recept)
    )
    ffn_key_in = ffn_inputs[0].astype(jnp.bfloat16)
    ffn_recept_in = ffn_inputs[1].astype(jnp.bfloat16)
    hidden_pre = matmul(ffn_key_in, w_ffn_key)
    hidden = jnp.square(jax.nn.relu(hidden_pre)).astype(jnp.bfloat16)
    ffn_values = matmul(hidden, w_ffn_value)
    gate_now = jax.nn.sigmoid(matmul(ffn_recept_in, w_ffn_recept))
    block_out = (middle + gate_now * ffn_values).astype(jnp.bfloat16)
    grad_out = cotangent.astype(jnp.float32)
    grad_values = (grad_out * gate_now).astype(jnp.bfloat16)
    grad_gate = (grad_out * ffn_values * gate_now * (1.0 - gate_now)).astype(jnp.bfloat16)
    grad_hidden = matmul_back(grad_values, w_ffn_value)
    grad_pre = (grad_hidden * 2.0 * jax.nn.relu(hidden_pre)).astype(jnp.bfloat16)
    grad_w_ffn_value = outer_sum(hidden, grad_values)
    grad_w_ffn_key = outer_sum(ffn_key_in, grad_pre)
    grad_w_ffn_recept = outer_sum(ffn_recept_in, grad_gate)
    grad_normed_ffn, grad_edge_ffn, ffn_mix_grads = ffn_mix_pull(
        (matmul_back(grad_pre, w_ffn_key), matmul_back(grad_gate, w_ffn_recept))
    )
    from_right_ffn = from_behind(grad_edge_ffn, "seq", -1)
    grad_normed_ffn = grad_normed_ffn.at[:, -1, :].add(from_right_ffn)
    grad_middle, grad_ln2_gain, grad_ln2_bias = norm_ffn_pull(grad_normed_ffn)
    grad_middle = grad_middle + grad_out
    grad_attended = grad_middle.astype(jnp.bfloat16)
    grad_w_output = outer_sum(gated_low, grad_attended)
    grad_recept_full, grad_mixed = gate_pull(matmul_back(grad_attended, w_output))
    grad_recept = grad_recept_full.astype(jnp.bfloat16)
    zero_state = (zero_rows, zero_rows, zero_rows)
    first_pass = wkv_pull((grad_mixed, zero_state))
    unscale = jnp.exp(-in_max)
    local_grad_num = first_pass[4] * unscale
    local_grad_den = first_pass[5] * unscale
    later_grads = prefix(
        (local_grad_num, local_grad_den, device_span),
        "seq",
        combine_grads,
        (zero_rows, zero_rows, zero_rows),
        True,
    )
    exit_num, exit_den = (later_grads[0], later_grads[1])
    out_num, out_den, out_max = state_out
    lifting = jnp.exp(out_max)
    exit_cotangent = (
        exit_num * lifting,
        exit_den * lifting,
        (exit_num * out_num + exit_den * out_den) * lifting,
    )
    second_pass = wkv_pull((jnp.zeros_like(grad_mixed), exit_cotangent))
    grad_key_rows = (first_pass[0] + second_pass[0]).astype(jnp.bfloat16)
    grad_value_rows = (first_pass[1] + second_pass[1]).astype(jnp.bfloat16)
    grad_time_decay = first_pass[2] + second_pass[2]
    grad_time_first = first_pass[3] + second_pass[3]
    grad_start_num = first_pass[4] + second_pass[4]
    grad_start_den = first_pass[5] + second_pass[5]
    grad_start_max = first_pass[6] + second_pass[6]
    grad_w_key = outer_sum(key_in, grad_key_rows)
    grad_w_value = outer_sum(value_in, grad_value_rows)
    grad_w_recept = outer_sum(recept_in, grad_recept)
    grad_normed, grad_edge_att, mix_grads = mix_pull(
        (
            matmul_back(grad_key_rows, w_key),
            matmul_back(grad_value_rows, w_value),
            matmul_back(grad_recept, w_recept),
        )
    )
    from_right = from_behind(grad_edge_att, "seq", -1)
    grad_normed = grad_normed.at[:, -1, :].add(from_right)
    grad_input_ln, grad_ln1_gain, grad_ln1_bias = norm_pull(grad_normed)
    input_grad = (grad_input_ln + grad_middle).astype(jnp.bfloat16)
    start_num_grad = jnp.where(is_first, grad_start_num, 0.0).T
    start_den_grad = jnp.where(is_first, grad_start_den, 0.0).T
    start_max_grad = jnp.where(is_first, grad_start_max, 0.0).T
    edge_att_grad = jnp.where(is_first, grad_edge_att, 0.0).T
    edge_ffn_grad = jnp.where(is_first, grad_edge_ffn, 0.0).T
    row_parts = (
        lax.psum_scatter(grad_w_key, "seq", scatter_dimension=0, tiled=True),
        lax.psum_scatter(grad_w_value, "seq", scatter_dimension=0, tiled=True),
        lax.psum_scatter(grad_w_recept, "seq", scatter_dimension=0, tiled=True),
        lax.psum_scatter(grad_w_output, "seq", scatter_dimension=0, tiled=True),
        lax.psum_scatter(grad_w_ffn_key, "seq", scatter_dimension=0, tiled=True),
        lax.psum_scatter(grad_w_ffn_value, "seq", scatter_dimension=0, tiled=True),
        lax.psum_scatter(grad_w_ffn_recept, "seq", scatter_dimension=0, tiled=True),
        lax.psum_scatter(grad_ln1_gain, "seq", scatter_dimension=0, tiled=True),
        lax.psum_scatter(grad_ln1_bias, "seq", scatter_dimension=0, tiled=True),
        lax.psum_scatter(mix_grads[0], "seq", scatter_dimension=0, tiled=True),
        lax.psum_scatter(mix_grads[1], "seq", scatter_dimension=0, tiled=True),
        lax.psum_scatter(mix_grads[2], "seq", scatter_dimension=0, tiled=True),
        lax.psum_scatter(grad_time_decay, "seq", scatter_dimension=0, tiled=True),
        lax.psum_scatter(grad_time_first, "seq", scatter_dimension=0, tiled=True),
        lax.psum_scatter(grad_ln2_gain, "seq", scatter_dimension=0, tiled=True),
        lax.psum_scatter(grad_ln2_bias, "seq", scatter_dimension=0, tiled=True),
        lax.psum_scatter(ffn_mix_grads[0], "seq", scatter_dimension=0, tiled=True),
        lax.psum_scatter(ffn_mix_grads[1], "seq", scatter_dimension=0, tiled=True),
        lax.psum_scatter(start_num_grad, "seq", scatter_dimension=0, tiled=True),
        lax.psum_scatter(start_den_grad, "seq", scatter_dimension=0, tiled=True),
        lax.psum_scatter(start_max_grad, "seq", scatter_dimension=0, tiled=True),
        lax.psum_scatter(edge_att_grad, "seq", scatter_dimension=0, tiled=True),
        lax.psum_scatter(edge_ffn_grad, "seq", scatter_dimension=0, tiled=True),
    )
    matrix_parts = (
        lax.psum_scatter(row_parts[0], "batch", scatter_dimension=1, tiled=True),
        lax.psum_scatter(row_parts[1], "batch", scatter_dimension=1, tiled=True),
        lax.psum_scatter(row_parts[2], "batch", scatter_dimension=1, tiled=True),
        lax.psum_scatter(row_parts[3], "batch", scatter_dimension=1, tiled=True),
        lax.psum_scatter(row_parts[4], "batch", scatter_dimension=1, tiled=True),
        lax.psum_scatter(row_parts[5], "batch", scatter_dimension=1, tiled=True),
        lax.psum_scatter(row_parts[6], "batch", scatter_dimension=1, tiled=True),
    )
    vector_parts = lax.psum(
        (
            row_parts[7],
            row_parts[8],
            row_parts[9],
            row_parts[10],
            row_parts[11],
            row_parts[12],
            row_parts[13],
            row_parts[14],
            row_parts[15],
            row_parts[16],
            row_parts[17],
        ),
        "batch",
    )
    start_parts = (row_parts[18], row_parts[19], row_parts[20], row_parts[21], row_parts[22])
    return (
        block_out,
        input_grad,
        matrix_parts[0],
        matrix_parts[1],
        matrix_parts[2],
        matrix_parts[3],
        matrix_parts[4],
        matrix_parts[5],
        matrix_parts[6],
        vector_parts[0],
        vector_parts[1],
        vector_parts[2],
        vector_parts[3],
        vector_parts[4],
        vector_parts[5],
        vector_parts[6],
        vector_parts[7],
        vector_parts[8],
        vector_parts[9],
        vector_parts[10],
        start_parts[0],
        start_parts[1],
        start_parts[2],
        start_parts[3],
        start_parts[4],
    )


def solution(mesh):
    placed = (
        P("batch", "seq", None),
        P(),
        P(),
        P(),
        P(),
        P(),
        P(),
        P(),
        P(),
        P(),
        P(),
        P(),
        P(),
        P(),
        P(),
        P(),
        P(),
        P(),
        P(),
        P(None, "batch"),
        P(None, "batch"),
        P(None, "batch"),
        P(None, "batch"),
        P(None, "batch"),
        P("batch", "seq", None),
    )
    return jax.shard_map(
        local if fits(mesh) else local_plain,
        mesh=mesh,
        in_specs=placed,
        out_specs=(
            P("batch", "seq", None),
            P("batch", "seq", None),
            P("seq", "batch"),
            P("seq", "batch"),
            P("seq", "batch"),
            P("seq", "batch"),
            P("seq", "batch"),
            P("seq", "batch"),
            P("seq", "batch"),
            P("seq"),
            P("seq"),
            P("seq"),
            P("seq"),
            P("seq"),
            P("seq"),
            P("seq"),
            P("seq"),
            P("seq"),
            P("seq"),
            P("seq"),
            P("seq", "batch"),
            P("seq", "batch"),
            P("seq", "batch"),
            P("seq", "batch"),
            P("seq", "batch"),
        ),
        check_vma=False,
    )
```

```python
import functools
from functools import partial

import jax
import jax.numpy as jnp
from jax import lax
from jax.experimental import pallas as pl
from jax.experimental.pallas import tpu as pltpu
from jax.sharding import PartitionSpec as P

MESH = pl.DeviceIdType.MESH
F32 = jnp.float32
BF = jnp.bfloat16
NS = 8
T = 512
D = 1024
SUB = T // 8

NZ = 4
NM = 13
NK = 2 * NM
WIN = 10
WINZ = 8
WINF = 4
RA = 48
RE = 128 - RA
LAGS = [3, 5, 4, 5, 6, 6, 7, 8, 8]
RETIRE = 9
STOP = False


def normalize(v, gain, bias):
    mean = jnp.mean(v, axis=-1, keepdims=True)
    cen = v - mean
    var = jnp.mean(cen * cen, axis=-1, keepdims=True)
    return cen * lax.rsqrt(var + 1e-5) * gain + bias


def step_weights(delta):
    e = jnp.exp(-jnp.abs(delta))
    up = delta >= 0
    return jnp.where(up, 1.0, e), jnp.where(up, e, 1.0)


def join(early, late, span):
    em, en, ed = early
    lm, ln, ld = late
    a, b = step_weights(em + span - lm)
    return jnp.maximum(em + span, lm), a * en + b * ln, a * ed + b * ld


def contract0(a, b):
    return lax.dot_general(a, b, (((0,), (0,)), ((), ())), preferred_element_type=F32)


def contract1(a, b):
    return lax.dot_general(a, b, (((1,), (1,)), ((), ())), preferred_element_type=F32)


def pick(m, table):
    out = jnp.int32(table[0])
    for i, v in enumerate(table[1:], 1):
        out = jnp.where(m == i, v, out)
    return out


LEFT = (0, 9, 1, 9, 2, 9, 3, 9, 10, 4, 5, 8, 7)
RIGHT = (8, 4, 8, 5, 8, 6, 8, 7, 0, 1, 2, 3, 6)


class Place:
    def __init__(self):
        self.s, self.b = lax.axis_index("seq"), lax.axis_index("batch")
        self.z, self.x = self.s // 2, self.s % 2
        self.y, self.c = self.b // 2, self.b % 2

    def at(self, z=None, x=None, y=None, c=None):
        z = self.z if z is None else z
        x = self.x if x is None else x
        y = self.y if y is None else y
        c = self.c if c is None else c
        return (z * 2 + x, y * 2 + c)


def rcopy(src, dst, ss, rs, dev):
    return pltpu.make_async_remote_copy(src_ref=src, dst_ref=dst, send_sem=ss, recv_sem=rs, device_id=dev, device_id_type=MESH)


def block_kernel(*refs):
    x_h, cot_h, wk_h, wv_h, wr_h, wo_h, wfk_h, wfv_h, wfr_h = refs[:9]
    small_h = refs[9:25]
    o_blk, o_inp = refs[25:27]
    outs = refs[27:34]
    sm_out = refs[34]
    kin_h, vin_h, rin_h, gat_h, k_h, v_h, r_h, mix_h, m_h, n_h, d_h = refs[35:46]
    (ob, wbuf, Y, G, V, K, X, lanes, lanes2, st, sums, RS, es, er, fs, fr, ws, wr, edges, as_, ar, bs_, br_, us, ur,
     acc, sbuf, rF, rSA, rSE, rZA, rZE, smb, smr,
     obsem, wsem, stsem, bigsem, outsem, spsem, esem, fsem, asem, bsem, wssem, wrsem,
     s0s, s0r, sFs, sFr, sSs, sSr, sZs, sZr, osem, msem, mss, msr, vsem) = refs[46:-16]
    (g1, b1, mk, mv, mr, td, tf, g2, b2, fmk, fmr, sn, sd, sm, pa, pf) = refs[-16:]
    small_loads = [pltpu.make_async_copy(src, dst, vsem) for src, dst in zip(small_h, refs[-16:])]
    for cp in small_loads:
        cp.start()
    me = Place()
    z, x, y, c, s = me.z, me.x, me.y, me.c, me.s
    left, right = (jnp.maximum(s - 1, 0), me.b), (jnp.minimum(s + 1, NS - 1), me.b)

    bar = pltpu.get_barrier_semaphore()

    def sig(dev):
        pl.semaphore_signal(bar, inc=1, device_id=dev, device_id_type=MESH)

    sig(me.at(c=1 - c))
    sig(me.at(y=1 - y))
    for i in range(1, NS):
        sig((lax.rem(s + i, NS), me.b))

    def local(src, dst, sem):
        return pltpu.make_async_copy(src, dst, sem)

    def op_load(src, slot):
        return local(src, ob.at[slot], obsem.at[slot])

    def slab_columns(src, j, dst, sem):
        return [local(src.at[:, pl.ds(i * 512 + j * 128, 128)], dst.at[:, pl.ds(i * 128, 128)], sem) for i in range(8)]

    def slab_rows(src, j, dst, sem):
        return [local(src.at[pl.ds(i * 512 + j * 128, 128), :], dst.at[pl.ds(i * 128, 128), :], sem) for i in range(8)]

    weights = [("p", wk_h), ("p", wv_h), ("p", wr_h), ("p", wo_h), ("p", wfr_h)]
    for j in range(4):
        weights += [("c", wfk_h, j), ("r", wfv_h, j)]
    weights += [("p", wfr_h), ("p", wo_h), ("p", wr_h), ("p", wv_h), ("p", wk_h)]

    def w_start(i):
        if i >= len(weights):
            return
        kind, src, *j = weights[i]
        dst, sem = wbuf.at[i % 3], wsem.at[i % 3]
        if kind == "p":
            local(src, dst, sem).start()
        else:
            for cp in (slab_columns if kind == "c" else slab_rows)(src, j[0], dst, sem):
                cp.start()

    def w_wait(i):
        local(wo_h, wbuf.at[i % 3], wsem.at[i % 3]).wait()

    def fs_of(k):
        h = lax.rem(k, 2)
        return jnp.where(h == 0, x, y), jnp.where(h == 0, y, x)

    def partner(h):
        a, b = me.at(x=1 - x), me.at(y=1 - y)
        return (jnp.where(h == 0, a[0], b[0]), jnp.where(h == 0, a[1], b[1]))

    def copy0(k):
        return rcopy(sbuf.at[lax.rem(k, 2)], acc.at[lax.rem(k, WIN)], s0s.at[lax.rem(k, 2)], s0r.at[lax.rem(k, WIN)], me.at(c=1 - c))

    def copyF(k):
        f, _ = fs_of(k)
        return rcopy(acc.at[lax.rem(k, WIN), 1 - f], rF.at[lax.rem(k, WINF)], sFs.at[lax.rem(k, WIN)], sFr.at[lax.rem(k, WINF)], partner(lax.rem(k, 2)))

    def copySA(k):
        f, g = fs_of(k)
        w, v = lax.rem(k, WIN), lax.rem(k, WINZ)
        return rcopy(acc.at[w, f, 1 - g, :, pl.ds(0, RA)], rSA.at[v], sSs.at[v, 0], sSr.at[v, 0], partner(1 - lax.rem(k, 2)))

    def copySE(k):
        f, g = fs_of(k)
        w, v = lax.rem(k, WIN), lax.rem(k, WINZ)
        return rcopy(acc.at[w, f, 1 - g, z, pl.ds(RA, RE)], rSE.at[v], sSs.at[v, 1], sSr.at[v, 1], partner(1 - lax.rem(k, 2)))

    def unit(k, q, late):
        f, g = fs_of(k)
        w = lax.rem(k, WIN)
        return acc.at[w, f, g, q, pl.ds(0, RA)] if late else acc.at[w, f, :, q, pl.ds(RA, RE)]

    def zbuf(k, slot, late):
        return (rZA if late else rZE).at[lax.rem(k, WINZ), slot]

    def copyR(k, q, late):
        i = int(late)
        return rcopy(unit(k, q, late), zbuf(k, q + 1, late), sZs.at[lax.rem(k, WINZ), i], sZr.at[lax.rem(k, WINZ), i, q + 1], me.at(z=z + 1))

    def copyL(k, q, late):
        i = int(late)
        return rcopy(unit(k, q, late), zbuf(k, q, late), sZs.at[lax.rem(k, WINZ), i], sZr.at[lax.rem(k, WINZ), i, q], me.at(z=z - 1))

    def add_into(dst, src):
        dst[...] = dst[...] + src[...]

    def zsub(k, tau, late):
        @pl.when(z <= tau)
        def _():
            q = NZ - 1 - tau + z

            @pl.when(z > 0)
            def _():
                copyR(k, q, late).wait_recv()
                add_into(unit(k, q, late), zbuf(k, q + 1, late))

            copyR(k, q, late).start()

        @pl.when(NZ - 1 - z <= tau)
        def _():
            q = tau - (NZ - 1 - z)

            @pl.when(z < NZ - 1)
            def _():
                copyL(k, q, late).wait_recv()
                add_into(unit(k, q, late), zbuf(k, q, late))

            copyL(k, q, late).start()

    def zfin(k, late):
        @pl.when(z > 0)
        def _():
            copyR(k, z, late).wait_recv()
            add_into(unit(k, z, late), zbuf(k, z + 1, late))

        @pl.when(z < NZ - 1)
        def _():
            copyL(k, z, late).wait_recv()
            add_into(unit(k, z, late), zbuf(k, z, late))

    def gradient(k, core, write):
        h, m = lax.rem(k, 2), k // 2
        ls, rs = pick(m, LEFT), pick(m, RIGHT)
        cols = jnp.concatenate(
            [ob[rs, :, pl.ds(pl.multiple_of((2 * yy + core) * 256 + h * 128, 128), 128)] for yy in range(2)], axis=1)

        def group(g, _):
            res = contract0(ob[ls, :, pl.ds(pl.multiple_of(g * 512, 512), 512)], cols)
            for i in range(4):
                zz, xx = g * 2 + i // 2, i % 2
                for yy in range(2):
                    f = jnp.where(h == 0, xx, yy)
                    g2_ = jnp.where(h == 0, yy, xx)
                    write(f, g2_, zz, res[i * 128:(i + 1) * 128, yy * 128:(yy + 1) * 128])
            return 0

        lax.fori_loop(0, 2, group, 0)

    def taskP(k):
        @pl.when(k >= 2)
        def _():
            copy0(k - 2).wait_send()

        slot = lax.rem(k, 2)

        def write(f, g, zz, v):
            sbuf[slot, f, g, zz] = v

        gradient(k, 1 - c, write)
        copy0(k).start()

    def task1(k):
        copy0(k).wait_recv()
        w = lax.rem(k, WIN)

        def write(f, g, zz, v):
            acc[w, f, g, zz] = acc[w, f, g, zz] + v

        gradient(k, c, write)
        copyF(k).start()

    def task2(k):
        copyF(k).wait_recv()
        f, _ = fs_of(k)
        w = lax.rem(k, WIN)

        def body(i, _):
            add_into(acc.at[w, f, i // NZ, lax.rem(i, NZ)], rF.at[lax.rem(k, WINF), i // NZ, lax.rem(i, NZ)])
            return 0

        lax.fori_loop(0, 2 * NZ, body, 0)
        copySA(k).start()
        zsub(k, 0, False)

    def taskSA(k):
        copySA(k).wait_recv()
        f, g = fs_of(k)
        w = lax.rem(k, WIN)
        add_into(acc.at[w, f, g, :, pl.ds(0, RA)], rSA.at[lax.rem(k, WINZ)])
        zsub(k, 0, True)

    def taskFinE(k):
        zfin(k, False)
        copySE(k).start()

    def taskSE(k):
        copySE(k).wait_recv()
        f, g = fs_of(k)
        w = lax.rem(k, WIN)
        add_into(acc.at[w, f, g, z, pl.ds(RA, RE)], rSE.at[lax.rem(k, WINZ)])
        src = acc.at[w, f, g, z]
        h, m = lax.rem(k, 2), k // 2
        half = pl.ds(pl.multiple_of(h * 128, 128), 128)
        for j in range(4):
            @pl.when(m == 2 * j)
            def _(j=j):
                local(src, outs[5].at[pl.ds(j * 128, 128), half], osem.at[lax.rem(k, WIN)]).start()

            @pl.when(m == 2 * j + 1)
            def _(j=j):
                local(src, outs[4].at[:, pl.ds(pl.multiple_of(h * 512 + j * 128, 128), 128)], osem.at[lax.rem(k, WIN)]).start()
        for mm, i in ((8, 6), (9, 3), (10, 2), (11, 1), (12, 0)):
            @pl.when(m == mm)
            def _(i=i):
                local(src, outs[i].at[:, half], osem.at[lax.rem(k, WIN)]).start()

    def retire(k):
        copyF(k).wait_send()
        copySA(k).wait_send()
        copySE(k).wait_send()
        f, g = fs_of(k)
        w, v = lax.rem(k, WIN), lax.rem(k, WINZ)
        for late in (False, True):
            others = pl.ds(0, NZ - 1)
            sent = acc.at[w, f, g, others, pl.ds(0, RA)] if late else acc.at[w, f, :, others, pl.ds(RA, RE)]
            rcopy(sent, sent, sZs.at[v, int(late)], sZr.at[v, int(late), 0], me.at(c=1 - c)).wait_send()
        local(acc.at[lax.rem(k, WIN), 0, 0, 0], outs[0].at[:, pl.ds(0, 128)], osem.at[lax.rem(k, WIN)]).wait()

    stages = [
        (RETIRE, retire),
        (LAGS[7], lambda k: zfin(k, True)),
        (LAGS[8], taskSE),
        (LAGS[6], lambda k: zsub(k, 2, True)),
        (LAGS[5], lambda k: zsub(k, 1, True)),
        (LAGS[4], taskFinE),
        (LAGS[3], lambda k: zsub(k, 2, False)),
        (LAGS[2], lambda k: zsub(k, 1, False)),
        (LAGS[1], taskSA),
        (LAGS[0], task2),
        (1, task1),
        (0, taskP),
    ]

    def sm_copy(step):
        if step == 0:
            return rcopy(smb.at[0], smr.at[0], mss.at[0], msr.at[0], me.at(c=1 - c))
        if step == 1:
            return rcopy(smb.at[2], smr.at[1], mss.at[1], msr.at[1], me.at(y=1 - y))
        return rcopy(smb.at[1, 1 - x], smr.at[2, 0], mss.at[2], msr.at[2], me.at(x=1 - x))

    def sm_z(q, to_right):
        if to_right:
            return rcopy(smb.at[1, x, q], smr.at[3, 0, q], mss.at[3 + q], msr.at[3 + q], me.at(z=z + 1))
        return rcopy(smb.at[1, x, q], smr.at[3, 1, q], mss.at[3 + q], msr.at[3 + NZ + q], me.at(z=z - 1))

    vec = lax.broadcasted_iota(jnp.int32, (2, NZ, 16, 128), 2) < 11

    def sm1():
        sm_copy(0).wait_recv()
        smb[2] = smb[0] + jnp.where(vec, smr[0], 0.0)
        sm_copy(1).start()

    def sm2():
        sm_copy(1).wait_recv()
        smb[1] = smb[2] + jnp.where(vec, smr[1], 0.0)
        sm_copy(2).start()

    def sm3():
        sm_copy(2).wait_recv()
        smb[1, x] = smb[1, x] + smr[2, 0]

    def smz(tau):
        @pl.when(z <= tau)
        def _():
            q = NZ - 1 - tau + z

            @pl.when(z > 0)
            def _():
                sm_z(q, True).wait_recv()
                smb[1, x, q] = smb[1, x, q] + smr[3, 0, q]

            sm_z(q, True).start()

        @pl.when(NZ - 1 - z <= tau)
        def _():
            q = tau - (NZ - 1 - z)

            @pl.when(z < NZ - 1)
            def _():
                sm_z(q, False).wait_recv()
                smb[1, x, q] = smb[1, x, q] + smr[3, 1, q]

            sm_z(q, False).start()

    def sm_fin():
        @pl.when(z > 0)
        def _():
            sm_z(z, True).wait_recv()
            smb[1, x, z] = smb[1, x, z] + smr[3, 0, z]

        @pl.when(z < NZ - 1)
        def _():
            sm_z(z, False).wait_recv()
            smb[1, x, z] = smb[1, x, z] + smr[3, 1, z]

        local(smb.at[1, x, z], sm_out, msem).start()

    def tiles(n, rows, body):
        def step(i, _):
            body(i, pl.ds(pl.multiple_of(i * rows, rows), rows))
            return 0

        lax.fori_loop(0, n, step, 0)

    def widen(slot):
        def body(i, rows):
            for g in range(8):
                lanes[g, rows, :] = ob[slot, rows, g * 128:g * 128 + 128].astype(F32)

        tiles(T // 64, 64, body)

    def spread(i, count):
        return jnp.concatenate(
            [jnp.concatenate([lanes[g, pl.ds(i * count + a, 8, stride=SUB), :] for g in range(8)], axis=1) for a in range(count)], axis=0)

    def unspread(i, count, value):
        for a in range(count):
            for g in range(8):
                lanes2[g, pl.ds(i * count + a, 8, stride=SUB), :] = value[a * 8:a * 8 + 8, g * 128:g * 128 + 128]

    def narrow(slot, dst, sem):
        def body(i, rows):
            for g in range(8):
                ob[slot, rows, g * 128:g * 128 + 128] = lanes2[g, rows, :].astype(BF)

        tiles(T // 64, 64, body)
        local(ob.at[slot], dst, sem).start()

    def halves(body):
        tiles(2, 512, body)

    def gate_step():
        w_wait(4)

        def mm(i, cols):
            G[:, cols] = jnp.dot(ob[10], wbuf[4 % 3, :, cols], preferred_element_type=F32)

        halves(mm)
        w_start(7)

        def body(i, rows):
            gate = jax.nn.sigmoid(G[rows, :])
            G[rows, :] = gate
            ob[8, rows, :] = (spread(i, 4) * gate).astype(BF)

        tiles(T // 32, 32, body)

    def hid(j):
        w_wait(5 + 2 * j)
        slot = (5 + 2 * j) % 3

        def mm(i, cols):
            up = jnp.maximum(jnp.dot(ob[9], wbuf[slot, :, cols], preferred_element_type=F32), 0.0)
            X[pl.ds(0, T), cols] = up
            ob[j, :, cols] = (up * up).astype(BF)

        halves(mm)

    def gpre(j):
        w_wait(6 + 2 * j)
        slot = (6 + 2 * j) % 3

        def mm(i, cols):
            back = contract1(ob[8], wbuf[slot, cols, :])
            ob[4 + j, :, cols] = (back * 2.0 * X[pl.ds(0, T), cols]).astype(BF)

        halves(mm)

    def gk_step(j):
        slot = (5 + 2 * j) % 3

        def mm(i, cols):
            part = contract1(ob[4 + j], wbuf[slot, cols, :])
            K[pl.ds(0, T), cols] = part if j == 0 else K[pl.ds(0, T), cols] + part

        halves(mm)
        w_start(5 + 2 * j + 3)

    def ffv(j):
        slot = (6 + 2 * j) % 3

        def mm(i, cols):
            part = jnp.dot(ob[j], wbuf[slot, :, cols], preferred_element_type=F32)
            V[pl.ds(0, T), cols] = part if j == 0 else V[pl.ds(0, T), cols] + part

        halves(mm)
        w_start(6 + 2 * j + 3)

    def big_load(src, dst, i):
        return local(src, dst.at[pl.ds(0, T)], bigsem.at[i])

    def block_step():
        def body(i, rows):
            gate, values = G[rows, :], V[rows, :]
            unspread(i, 4, Y[rows, :] + gate * values)
            ob[0, rows, :] = (spread(i, 4) * values * gate * (1.0 - gate)).astype(BF)

        tiles(T // 32, 32, body)
        narrow(5, o_blk, outsem.at[0])

    row8 = lax.broadcasted_iota(jnp.int32, (8, D), 0)

    def tail(buf):
        buf[T:T + 8, :] = jnp.where(row8 == 7, 0.0, pltpu.roll(buf[0:8, :], 7, 0))

    def edge(src, dst, sem, dev):
        return rcopy(src, dst, sem.at[0], sem.at[1], dev)

    def recept_back():
        w_wait(13)

        def mm(i, cols):
            V[pl.ds(0, T), cols] = contract1(ob[0], wbuf[13 % 3, cols, :])

        halves(mm)
        w_start(16)
        tail(K)
        tail(V)
        es[...] = K[0:8, :] * (1.0 - fmk[...]) + V[0:8, :] * (1.0 - fmr[...])

        @pl.when(s > 0)
        def _():
            edge(es, er, esem, left).start()

    def fold(v):
        return v[0:8] + v[8:16] + v[16:24] + v[24:32]

    row32 = lax.broadcasted_iota(jnp.int32, (32, D), 0)

    def centre(v):
        mean = jnp.mean(v, axis=-1, keepdims=True)
        cen = v - mean
        inv = lax.rsqrt(jnp.mean(cen * cen, axis=-1, keepdims=True) + 1e-5)
        return cen * inv, inv

    def ln_back(grad, n, inv, gain):
        h = grad * gain[...]
        return inv * (h - jnp.mean(h, axis=-1, keepdims=True) - n * jnp.mean(h * n, axis=-1, keepdims=True))

    def ln_tile(i, rows, n, gain, bias, parts, arrived, sum_rows, ln_sums):
        later = pl.ds(pl.multiple_of(i * 32 + 8, 8), 32)
        normed = n * gain[...] + bias[...]
        grad = 0.0
        if arrived is not None:
            grad = jnp.where(jnp.logical_and(row32 == 31, i == T // 32 - 1), arrived, 0.0)
        for (buf, w), r in zip(parts, sum_rows):
            now, nxt = buf[rows, :], buf[later, :]
            grad = grad + now * w[...] + nxt * (1.0 - w[...])
            sums[r] = sums[r] + fold(normed * (now - nxt))
        sums[ln_sums[0]] = sums[ln_sums[0]] + fold(grad * n)
        sums[ln_sums[1]] = sums[ln_sums[1]] + fold(grad)
        return grad

    def wait_from_right(cp):
        @pl.when(s < NS - 1)
        def _():
            cp.wait_recv()

    def middle_back(lo, hi):
        arrived = jnp.where(s == NS - 1, 0.0, er[0:1, :]) if hi == T // 32 else None

        def body(i, _):
            rows = pl.ds(pl.multiple_of(i * 32, 32), 32)
            n, inv = centre(Y[rows, :])
            grad = ln_tile(i, rows, n, g2, b2, ((K, fmk), (V, fmr)), arrived, (9, 10), (7, 8))
            gm = spread(i, 4) + ln_back(grad, n, inv, g2)
            G[rows, :] = gm
            ob[1, rows, :] = gm.astype(BF)
            return 0

        lax.fori_loop(lo, hi, body, 0)

    def middle_end():
        for r, buf in ((9, K), (10, V)):
            sums[r, 0:1, :] = sums[r, 0:1, :] - buf[0:1, :] * edges[8:9, :]
        sums[15, 0:1, :] = es[0:1, :]

    def gated_back():
        w_wait(14)

        def mm(i, cols):
            V[pl.ds(0, T), cols] = contract1(ob[1], wbuf[14 % 3, cols, :])

        halves(mm)
        w_start(17)
        big_load(r_h, X, 0).wait()
        big_load(mix_h, K, 1).wait()

        def body(i, rows):
            sg = jax.nn.sigmoid(X[rows, :])
            gg = V[rows, :]
            ob[2, rows, :] = (gg * K[rows, :] * sg * (1.0 - sg)).astype(BF)
            V[rows, :] = gg * sg

        tiles(T // 32, 32, body)

    streams = (k_h, m_h, d_h, n_h, v_h)

    def st_copies(blk, slot, count):
        rows = pl.ds(pl.multiple_of(blk * 64, 64), 64)
        return [local(src.at[rows, :], st.at[slot, i], stsem.at[slot, i]) for i, src in enumerate(streams[:count])]

    def st_start(blk, count):
        for cp in st_copies(blk, lax.rem(blk, 2), count):
            cp.start()

    def st_next(blk, count):
        for cp in st_copies(blk, lax.rem(blk, 2), count):
            cp.wait()

        @pl.when(blk > 0)
        def _():
            st_start(blk - 1, count)


    def wide(v, cols):
        return jnp.broadcast_to(v[:, cols], (8, 512))

    def first_pass(lo):
        def block(i, _):
            blk = 7 - lo - i
            slot = lax.rem(blk, 2)
            st_next(blk, 3)
            for h in range(2):
                cols = slice(h * 512, h * 512 + 512)
                w, bonus = wide(decay, cols), wide(tf[...], cols)

                def step(jj, carry):
                    R, S = carry
                    j = 7 - jj
                    at = pl.ds(pl.multiple_of(j * 8, 8), 8)
                    rows = pl.ds(pl.multiple_of(blk * 64 + j * 8, 8), 8)
                    k, m, d = st[slot, 0, at, cols], st[slot, 1, at, cols], st[slot, 2, at, cols]
                    p, u = step_weights(m - (bonus + k))
                    q = V[rows, cols] / (p * d + u)
                    qp = p * q
                    V[rows, cols] = qp
                    X[rows, cols] = u * q
                    a, _ = step_weights(m + w - k)
                    return qp + a * R, qp * K[rows, cols] + a * S

                R, S = lax.fori_loop(0, 8, step, (RS[0, :, cols], RS[1, :, cols]), unroll=2)
                RS[0, :, cols] = R
                RS[1, :, cols] = S

                @pl.when(blk == 7)
                def _():
                    RS[2, :, cols] = jnp.maximum(st[slot, 1, 56:64, cols] + w, st[slot, 0, 56:64, cols])

                @pl.when(blk == 0)
                def _():
                    RS[3, :, cols] = st[slot, 1, 0:8, cols]
            return 0

        lax.fori_loop(0, 4, block, 0)

    def suffix(value, dist, fill):
        return jnp.where(row8 >= 8 - dist, fill, pltpu.roll(value, 8 - dist, 0))


    def state_copy(src, dst):
        return rcopy(ws, wr.at[src], wssem.at[dst], wrsem.at[src], (dst, me.b))

    def first_end():
        A = jnp.exp(jnp.minimum(RS[3] + span - RS[2], 0.0))
        R, S = RS[0], RS[1]
        for dist in (1, 2, 4):
            R = R + A * suffix(R, dist, 0.0)
            S = S + A * suffix(S, dist, 0.0)
            A = A * suffix(A, dist, 1.0)
        RS[0], RS[1], RS[4] = R, S, A
        ws[...] = jnp.where(row8 == 0, R[0:1], jnp.where(row8 == 1, S[0:1], RS[3, 0:1, :]))
        for i in range(NS - 1):
            @pl.when(i < s)
            def _(i=i):
                state_copy(s, i).start()

    def second_start():
        RS[5] = jnp.zeros((8, D), F32)
        RS[6] = jnp.zeros((8, D), F32)
        for i in range(1, NS):
            @pl.when(i > s)
            def _(i=i):
                state_copy(i, 0).wait_recv()
                far = jnp.exp(jnp.minimum(RS[2, 7:8, :] + (i - s - 1).astype(F32) * (8.0 * span) - wr[i, 2:3, :], 0.0))
                RS[5, 0:1, :] = RS[5, 0:1, :] + far * wr[i, 0:1, :]
                RS[6, 0:1, :] = RS[6, 0:1, :] + far * wr[i, 1:2, :]
        Rin, Sin = RS[5, 0:1, :], RS[6, 0:1, :]
        A = RS[4]
        R = RS[0] + A * Rin
        S = RS[1] + A * Sin
        RS[0] = jnp.where(row8 == 7, Rin, pltpu.roll(R, 7, 0))
        RS[1] = jnp.where(row8 == 7, Sin, pltpu.roll(S, 7, 0))

    def second_pass(lo, n):
        def block(i, _):
            blk = 7 - lo - i
            slot = lax.rem(blk, 2)
            st_next(blk, 5)
            for h in range(2):
                cols = slice(h * 512, h * 512 + 512)
                w = wide(decay, cols)

                def one(j, carry):
                    R, S, first, slow = carry
                    at = pl.ds(pl.multiple_of(j * 8, 8), 8)
                    rows = pl.ds(pl.multiple_of(blk * 64 + j * 8, 8), 8)
                    k, m, d, n_, v = (st[slot, q, at, cols] for q in range(5))
                    mixed, qp, uq = K[rows, cols], V[rows, cols], X[rows, cols]
                    a, b = step_weights(m + w - k)
                    own = uq * (v - mixed)
                    gv = uq + b * R
                    gk = own + b * (v * R - S)
                    first = first + own
                    slow = slow + a * (n_ * R - d * S)
                    return (qp + a * R, qp * mixed + a * S, first, slow), gk, gv

                def step(jj, carry):
                    j = 3 - jj
                    carry, gk1, gv1 = one(2 * j + 1, carry)
                    carry, gk0, gv0 = one(2 * j, carry)
                    pair = pl.ds(pl.multiple_of(blk * 64 + j * 16, 16), 16)
                    ob[6, pair, cols] = jnp.concatenate([gk0, gk1], axis=0).astype(BF)
                    ob[3, pair, cols] = jnp.concatenate([gv0, gv1], axis=0).astype(BF)
                    return carry

                R, S, first, slow = lax.fori_loop(0, 4, step, (RS[0, :, cols], RS[1, :, cols], sums[6, :, cols], sums[5, :, cols]))
                RS[0, :, cols] = R
                RS[1, :, cols] = S
                sums[6, :, cols] = first
                sums[5, :, cols] = slow
            return 0

        lax.fori_loop(0, n, block, 0)

    def second_end():
        gn, gd = RS[0, 0:1, :], -RS[1, 0:1, :]
        sums[11, 0:1, :] = gn
        sums[12, 0:1, :] = gd
        sums[13, 0:1, :] = sn[...] * gn + sd[...] * gd
        sums[5] = sums[5] * decay

    def input_mm(i, slot, buf):
        w_wait(i)

        def mm(_, cols):
            buf[pl.ds(0, T), cols] = contract1(ob[slot], wbuf[i % 3, cols, :])

        halves(mm)
        tail(buf)

    def input_edge():
        fs[...] = K[0:8, :] * (1.0 - mk[...]) + V[0:8, :] * (1.0 - mv[...]) + X[0:8, :] * (1.0 - mr[...])

        @pl.when(s > 0)
        def _():
            edge(fs, fr, fsem, left).start()

    def input_back(lo, hi):
        arrived = jnp.where(s == NS - 1, 0.0, fr[0:1, :]) if hi == T // 32 else None

        def body(i, _):
            rows = pl.ds(pl.multiple_of(i * 32, 32), 32)
            n, inv = centre(spread(i, 4))
            grad = ln_tile(i, rows, n, g1, b1, ((K, mk), (V, mv), (X, mr)), arrived, (2, 3, 4), (0, 1))
            unspread(i, 4, G[rows, :] + ln_back(grad, n, inv, g1))
            return 0

        lax.fori_loop(lo, hi, body, 0)

    def input_end():
        for r, buf in ((2, K), (3, V), (4, X)):
            sums[r, 0:1, :] = sums[r, 0:1, :] - buf[0:1, :] * edges[0:1, :]
        sums[14, 0:1, :] = fs[0:1, :]
        narrow(0, o_inp, outsem.at[1])
        alone = jnp.where(s == 0, 1.0, 0.0)
        rows = [jnp.sum(sums[r], axis=0, keepdims=True) for r in range(11)] + [jnp.where(s == 0, sums[r, 0:1, :], 0.0) for r in range(11, 16)]
        table = jnp.concatenate(rows, axis=0)
        for g in range(8):
            smb[0, g % 2, g // 2] = table[:, g * 128:g * 128 + 128]
        sm_copy(0).start()

    def start_all(*copies):
        for cp in copies:
            cp.start()

    compute = {
        1: [lambda: gpre(0), lambda: gk_step(0), lambda: hid(1)],
        2: [lambda: ffv(0), lambda: gpre(1)],
        3: [lambda: gk_step(1), lambda: hid(2)],
        4: [lambda: ffv(1), lambda: gpre(2)],
        5: [lambda: gk_step(2), lambda: hid(3), lambda: start_all(op_load(gat_h, 4))],
        6: [lambda: ffv(2), lambda: gpre(3)],
        7: [lambda: gk_step(3), lambda: ffv(3)],
        8: [block_step],
        9: [recept_back],
        10: [lambda: middle_back(0, 8)],
        11: [lambda: start_all(big_load(r_h, X, 0)), lambda: wait_from_right(edge(es, er, esem, left)), lambda: middle_back(8, 16), middle_end,
             lambda: start_all(big_load(mix_h, K, 1)), lambda: st_start(7, 3),
             lambda: local(ob.at[5], o_blk, outsem.at[0]).wait(), lambda: start_all(op_load(rin_h, 5))],
        12: [gated_back],
        13: [lambda: first_pass(0)],
        14: [lambda: first_pass(4), first_end, lambda: st_start(7, 5)],
        15: [second_start, lambda: second_pass(0, 2), lambda: start_all(op_load(vin_h, 8))],
        16: [lambda: second_pass(2, 3)],
        17: [lambda: second_pass(5, 3), second_end, lambda: start_all(op_load(kin_h, 7), op_load(x_h, 9))],
        18: [lambda: input_mm(15, 2, X), lambda: input_mm(16, 3, V)],
        19: [lambda: input_mm(17, 6, K), input_edge, lambda: op_load(x_h, 9).wait(), lambda: widen(9)],
        20: [lambda: input_back(0, 8)],
        21: [lambda: wait_from_right(edge(fs, fr, fsem, left)), lambda: input_back(8, 16), input_end],
        23: [sm1],
        24: [sm2],
        25: [sm3, lambda: smz(0)],
        27: [lambda: smz(1)],
        29: [lambda: smz(2)],
        31: [sm_fin],
    }
    landed = {18: (gat_h, 4), 20: (rin_h, 5), 22: (vin_h, 8), 24: (kin_h, 7)}

    def spill(src, dst, i):
        return local(src, dst, spsem.at[i])

    kb, vb, rb, nb = G, V, X, K
    to_next = rcopy(as_, ar, asem.at[0], asem.at[1], right)
    to_next2 = rcopy(bs_, br_, bsem.at[0], bsem.at[1], right)

    def wait_from_left(cp):
        @pl.when(s > 0)
        def _():
            cp.wait_recv()

    def send_right(cp):
        @pl.when(s < NS - 1)
        def _():
            cp.start()

    def norm1(i, rows):
        v = spread(i, 8)
        Y[rows, :] = v
        nb[pl.ds(pl.multiple_of(i * 64 + 8, 8), 64), :] = normalize(v, g1[...], b1[...])

    def header(start_row):
        nb[0:8, :] = jnp.where(row8 == 0, start_row, pltpu.roll(nb[T:T + 8, :], 1, 0))

    def mix(pairs, i):
        rows = pl.ds(pl.multiple_of(i * 64, 64), 64)
        before = nb[rows, :]
        now = nb[pl.ds(pl.multiple_of(i * 64 + 8, 8), 64), :]
        for slot, w in pairs:
            ob[slot, rows, :] = (now * w[...] + before * (1.0 - w[...])).astype(BF)

    def project(i, slot, dst):
        w_wait(i)
        dst[pl.ds(0, T), :] = jnp.dot(ob[slot], wbuf[i % 3], preferred_element_type=F32)
        w_start(i + 3)

    start_all(op_load(x_h, 4), op_load(cot_h, 5))
    for i in range(3):
        w_start(i)
    local(K.at[pl.ds(0, 16)], V.at[pl.ds(0, 16)], vsem).wait()
    decay = -jnp.exp(td[...])
    span = SUB * decay
    op_load(x_h, 4).wait()
    as_[...] = normalize(ob[4, T - 16:T, :].astype(F32), g1[...], b1[...])[8:16, :]
    pl.semaphore_wait(bar, NS + 1)
    send_right(to_next)
    widen(4)
    tiles(T // 64, 64, norm1)
    wait_from_left(to_next)
    header(jnp.where(s == 0, pa[...], ar[7:8, :]))
    edges[0:8, :] = nb[0:8, :]
    tiles(T // 64, 64, lambda i, rows: mix(((0, mk), (1, mv), (2, mr)), i))
    start_all(spill(ob.at[0], kin_h, 0), spill(ob.at[1], vin_h, 1), spill(ob.at[2], rin_h, 2))
    project(0, 0, kb)
    project(1, 1, vb)
    start_all(spill(kb, k_h, 3), spill(vb.at[pl.ds(0, T)], v_h, 4))

    wide_decay = jnp.broadcast_to(decay, (8, D))

    def own_step(j, state):
        rows = pl.ds(pl.multiple_of(j * 8, 8), 8)
        m, n, d = state
        k, v = kb[rows, :], vb[rows, :]
        low = m + wide_decay
        a, b = step_weights(low - k)
        return jnp.maximum(low, k), a * n + b * v, a * d + b

    total = lax.fori_loop(1, SUB, own_step, (kb[0:8, :], vb[0:8, :], jnp.ones((8, D), F32)), unroll=7)

    def earlier(state, dist):
        m, n, d = (pltpu.roll(p, dist, 0) for p in state)
        out = row8 < dist
        return jnp.where(out, -1e30, m), jnp.where(out, 0.0, n), jnp.where(out, 0.0, d)

    for dist in (1, 2, 4):
        total = join(earlier(total, dist), total, dist * span)
    before_own = earlier(total, 1)
    us[...] = jnp.where(row8 == 0, total[0][7:8], jnp.where(row8 == 1, total[1][7:8], total[2][7:8]))

    def reach_copy(src, dst):
        return rcopy(us, ur.at[src], wssem.at[dst], wrsem.at[src], (dst, me.b))

    for i in range(1, NS):
        @pl.when(s < i)
        def _(i=i):
            reach_copy(s, i).start()

    project(2, 2, rb)
    start_all(spill(rb.at[pl.ds(0, T)], r_h, 5))
    op_load(cot_h, 5).wait()
    widen(5)
    RS[0, 0:1, :] = sm[...]
    RS[1, 0:1, :] = sn[...]
    RS[2, 0:1, :] = sd[...]
    for i in range(NS - 1):
        @pl.when(i < s)
        def _(i=i):
            reach_copy(i, NS - 1).wait_recv()
            now = join(tuple(RS[r, 0:1, :] for r in range(3)), tuple(ur[i, r:r + 1, :] for r in range(3)), 8.0 * span)
            for r in range(3):
                RS[r, 0:1, :] = now[r]

    base = tuple(RS[r, 0:1, :] for r in range(3))
    lifted = (base[0] + row8.astype(F32) * span, jnp.broadcast_to(base[1], (8, D)), jnp.broadcast_to(base[2], (8, D)))
    for r, v in enumerate(join(lifted, before_own, 0.0)):
        RS[r] = v

    def state_spills(blk, slot):
        rows = pl.ds(pl.multiple_of(blk * 64, 64), 64)
        return [local(st.at[slot, q], dst.at[rows, :], stsem.at[slot, q]) for q, dst in enumerate((mix_h, m_h, n_h, d_h))]

    def outputs(blk, _):
        slot = lax.rem(blk, 2)

        @pl.when(blk >= 2)
        def _():
            for cp in state_spills(blk - 2, slot):
                cp.wait()

        for h in range(2):
            cols = slice(h * 512, h * 512 + 512)
            w, bonus = wide(decay, cols), wide(tf[...], cols)

            def one(j, state):
                at = pl.ds(pl.multiple_of(j * 8, 8), 8)
                rows = pl.ds(pl.multiple_of(blk * 64 + j * 8, 8), 8)
                m, n, d = state
                k, v = kb[rows, cols], vb[rows, cols]
                p, u = step_weights(m - (bonus + k))
                mixed = (p * n + u * v) / (p * d + u)
                for q, val in enumerate((mixed, m, n, d)):
                    st[slot, q, at, cols] = val
                low = m + w
                a, b = step_weights(low - k)
                return (jnp.maximum(low, k), a * n + b * v, a * d + b), jax.nn.sigmoid(rb[rows, cols]) * mixed

            def two(i, state):
                state, ga = one(2 * i, state)
                state, gb = one(2 * i + 1, state)
                ob[3, pl.ds(pl.multiple_of(blk * 64 + i * 16, 16), 16), cols] = jnp.concatenate([ga, gb], axis=0).astype(BF)
                return state

            for r, v in enumerate(lax.fori_loop(0, 4, two, tuple(RS[r, :, cols] for r in range(3)), unroll=4)):
                RS[r, :, cols] = v
        start_all(*state_spills(blk, slot))
        return 0

    lax.fori_loop(0, 8, outputs, 0)
    start_all(spill(ob.at[3], gat_h, 6))
    spill(kb, k_h, 3).wait()
    project(3, 3, G)

    def norm2(i, rows):
        v = Y[rows, :] + G[rows, :]
        Y[rows, :] = v
        nb[pl.ds(pl.multiple_of(i * 64 + 8, 8), 64), :] = normalize(v, g2[...], b2[...])

    norm2(T // 64 - 1, pl.ds(T - 64, 64))
    bs_[...] = nb[T:T + 8, :]
    send_right(to_next2)
    tiles(T // 64 - 1, 64, norm2)

    def mix2(i, _):
        mix(((9, fmk), (10, fmr)), i)
        return 0

    lax.fori_loop(1, T // 64, mix2, 0)
    wait_from_left(to_next2)
    header(jnp.where(s == 0, pf[...], br_[7:8, :]))
    edges[8:16, :] = nb[0:8, :]
    mix2(0, 0)

    sums[...] = jnp.zeros_like(sums)
    gate_step()
    spill(ob.at[0], kin_h, 0).wait()
    spill(rb.at[pl.ds(0, T)], r_h, 5).wait()
    hid(0)
    RS[...] = jnp.zeros_like(RS)
    for i, (src, dst) in enumerate(((ob.at[1], vin_h), (ob.at[2], rin_h))):
        spill(src, dst, 1 + i).wait()
    spill(vb.at[pl.ds(0, T)], v_h, 4).wait()
    spill(ob.at[3], gat_h, 6).wait()
    for blk in (6, 7):
        for cp in state_spills(blk, blk % 2):
            cp.wait()

    def tick(t, _):
        for at, (src, slot) in landed.items():
            @pl.when(t == at)
            def _(src=src, slot=slot):
                op_load(src, slot).wait()

        for lag, task in stages:
            k = t - lag

            @pl.when(jnp.logical_and(k >= (2 if lag < 2 else 0), k < NK))
            def _(k=k, task=task):
                task(k)

        for at, steps in compute.items():
            @pl.when(t == at)
            def _(steps=steps):
                for step in steps:
                    step()
        return 0

    for k in range(2):
        taskP(jnp.int32(k))
    for k in range(2):
        task1(jnp.int32(k))
    lax.fori_loop(1, NK + RETIRE, tick, 0)

    copy0(NK - 2).wait_send()
    copy0(NK - 1).wait_send()
    for i in range(3):
        sm_copy(i).wait_send()
    for q in range(NZ):
        @pl.when(q != z)
        def _(q=q):
            sm_z(q, True).wait_send()

    @pl.when(s > 0)
    def _():
        edge(es, er, esem, left).wait_send()
        edge(fs, fr, fsem, left).wait_send()

    @pl.when(s < NS - 1)
    def _():
        to_next.wait_send()
        to_next2.wait_send()

    for i in range(NS):
        @pl.when(i < s)
        def _(i=i):
            state_copy(s, i).wait_send()

        @pl.when(i > s)
        def _(i=i):
            reach_copy(s, i).wait_send()
    local(smb.at[1, x, z], sm_out, msem).wait()
    local(ob.at[0], o_inp, outsem.at[1]).wait()


def block_call(x, cot, mats, vectors, states):
    anyspec = pl.BlockSpec(memory_space=pl.ANY)
    S = jax.ShapeDtypeStruct
    sem = pltpu.SemaphoreType.DMA
    M = pltpu.VMEM
    row = M((8, D), F32)
    return pl.pallas_call(
        block_kernel,
        out_shape=[S((T, D), BF)] * 2 + [S((128, 256), F32)] * 4 + [S((128, 1024), F32), S((512, 256), F32), S((128, 256), F32), S((16, 128), F32)]
        + [S((T, D), BF)] * 4 + [S((T, D), F32)] * 7,
        in_specs=[anyspec] * 25,
        out_specs=[anyspec] * 21,
        scratch_shapes=[
            M((11, T, D), BF), M((3, D, D), BF), M((T, D), F32), M((T, D), F32), M((T + 8, D), F32), M((T + 8, D), F32), M((T + 8, D), F32),
            M((8, T, 128), F32), M((8, T, 128), F32), M((2, 5, 64, D), F32), M((16, 8, D), F32), M((7, 8, D), F32),
            row, row, row, row, row, M((NS, 8, D), F32), M((16, D), F32), row, row, row, row, row, M((NS, 8, D), F32),
            M((WIN, 2, 2, NZ, 128, 128), F32), M((2, 2, 2, NZ, 128, 128), F32), M((WINF, 2, NZ, 128, 128), F32),
            M((WINZ, NZ, RA, 128), F32), M((WINZ, RE, 128), F32), M((WINZ, NZ + 1, RA, 128), F32), M((WINZ, NZ + 1, 2, RE, 128), F32),
            M((3, 2, NZ, 16, 128), F32), M((4, 2, NZ, 16, 128), F32),
            sem((11,)), sem((3,)), sem((2, 5)), sem((2,)), sem((2,)), sem((7,)), sem((2,)), sem((2,)), sem((2,)), sem((2,)), sem((NS,)), sem((NS,)),
            sem((2,)), sem((WIN,)), sem((WIN,)), sem((WINF,)), sem((WINZ, 2)), sem((WINZ, 2)),
            sem((WINZ, 2)), sem((WINZ, 2, NZ + 1)), sem((WIN,)), sem, sem((3 + NZ,)), sem((3 + 2 * NZ,)), sem,
        ] + [M((1, D), F32)] * 16,
        compiler_params=pltpu.CompilerParams(collective_id=0, has_side_effects=True, vmem_limit_bytes=67043328),
        name="block",
    )(x, cot, *mats, *vectors, *states)[:10]

def finish_kernel(*refs):
    ins, outs, (scratch, sems) = refs[:10], refs[10:35], (refs[35:-2], refs[-2:])
    into, out = sems
    loads = [pltpu.make_async_copy(src, buf, into.at[i]) for i, (src, buf) in enumerate(zip(ins, scratch))]
    for cp in loads:
        cp.start()
    stores = []
    for i in (9, 2, 3, 4, 5, 8, 6, 7, 0, 1):
        loads[i].wait()
        if i < 9:
            stores.append(pltpu.make_async_copy(scratch[i], outs[i], out.at[i]))
            stores[-1].start()
        else:
            for r in range(16):
                stores.append(pltpu.make_async_copy(scratch[i].at[pl.ds(r, 1)], outs[9 + r], out.at[9 + r]))
                stores[-1].start()
    for cp in stores:
        cp.wait()


def finish_call(parts):
    anyspec = pl.BlockSpec(memory_space=pl.ANY)
    return pl.pallas_call(
        finish_kernel,
        out_shape=[jax.ShapeDtypeStruct(p.shape, p.dtype) for p in parts[:9]] + [jax.ShapeDtypeStruct((1, 128), F32)] * 16,
        in_specs=[anyspec] * 10,
        out_specs=[anyspec] * 25,
        scratch_shapes=[pltpu.VMEM(p.shape, p.dtype) for p in parts] + [pltpu.SemaphoreType.DMA((10,)), pltpu.SemaphoreType.DMA((25,))],
        name="finish",
    )(*parts)


def fits(mesh):
    return (mesh.shape["seq"], mesh.shape["batch"]) == (2 * NZ, 4)


def local(
    inputs,
    w_key,
    w_value,
    w_recept,
    w_output,
    w_ffn_key,
    w_ffn_value,
    w_ffn_recept,
    ln1_gain,
    ln1_bias,
    mix_key,
    mix_value,
    mix_recept,
    time_decay,
    time_first,
    ln2_gain,
    ln2_bias,
    ffn_mix_key,
    ffn_mix_recept,
    state_num,
    state_den,
    state_max,
    prev_att,
    prev_ffn,
    cotangent,
):
    rows = inputs.reshape(T, D)
    vectors = [
        v.reshape(1, D)
        for v in (
            ln1_gain,
            ln1_bias,
            mix_key,
            mix_value,
            mix_recept,
            time_decay,
            time_first,
            ln2_gain,
            ln2_bias,
            ffn_mix_key,
            ffn_mix_recept,
        )
    ]
    states = [v.reshape(1, D) for v in (state_num, state_den, state_max, prev_att, prev_ffn)]
    parts = block_call(
        rows,
        cotangent.reshape(T, D),
        [w_key, w_value, w_recept, w_output, w_ffn_key, w_ffn_value, w_ffn_recept],
        vectors,
        states,
    )
    block_out, input_grad, *rest = finish_call(parts)
    return (
        block_out.reshape(inputs.shape),
        input_grad.reshape(inputs.shape),
        *rest[:7],
        *[v.reshape(128) for v in rest[7:18]],
        *[v.reshape(128, 1) for v in rest[18:]],
    )


BLOCK = 64


far_below = -1e30


def from_behind(block, axis, distance):
    devices = range(lax.axis_size(axis))
    route = [(i - distance, i) for i in devices if i - distance in devices]
    return lax.ppermute(block, axis, route)


def prefix(value, axis, join, neutral, backward):
    count, mine = (lax.axis_size(axis), lax.axis_index(axis))
    pieces = jax.tree.map(lambda part: lax.all_gather(part, axis), value)
    if backward:
        pieces = jax.tree.map(lambda part: part[::-1], pieces)
        mine = count - 1 - mine
    total = jax.tree.map(
        lambda part, zero: jnp.full_like(part, 0) + jnp.asarray(zero, part.dtype), value, neutral
    )

    def turn(position, total):
        longer = join(total, jax.tree.map(lambda part: part[position], pieces))
        return jax.tree.map(lambda new, old: jnp.where(position < mine, new, old), longer, total)

    return lax.fori_loop(0, count - 1, turn, total)


def layer_norm(values, ln_gain, ln_bias):
    centred = values - jnp.mean(values, axis=-1, keepdims=True)
    spread = jnp.mean(centred * centred, axis=-1, keepdims=True)
    return centred * lax.rsqrt(spread + 1e-05) * ln_gain + ln_bias


def matmul(operand, matrix):
    return lax.dot_general(
        operand, matrix, (((operand.ndim - 1,), (0,)), ((), ())), preferred_element_type=jnp.float32
    )


def matmul_back(gradient, matrix):
    return lax.dot_general(
        gradient,
        matrix,
        (((gradient.ndim - 1,), (1,)), ((), ())),
        preferred_element_type=jnp.float32,
    )


def outer_sum(operand, gradient):
    flat_operand = operand.reshape(-1, operand.shape[-1])
    flat_gradient = gradient.reshape(-1, gradient.shape[-1])
    return lax.dot_general(
        flat_operand, flat_gradient, (((0,), (0,)), ((), ())), preferred_element_type=jnp.float32
    )


def token_mix(normed, edge_row, mix_vectors):
    earlier = jnp.concatenate([edge_row[:, None, :], normed[:, :-1, :]], axis=1)
    return tuple((normed * member + earlier * (1.0 - member) for member in mix_vectors))


def gate_rows(recept_rows, mixed_rows):
    return jax.nn.sigmoid(recept_rows) * mixed_rows


def wkv_block(decay_rate, time_first, state_in, inputs_now):
    numerator, denominator, running_max = state_in
    key_rows, value_rows = inputs_now
    length = key_rows.shape[1]
    places = jnp.arange(length, dtype=jnp.float32)[None, :, None]
    own_terms = time_first + key_rows
    anchor = jnp.maximum(
        jnp.maximum(running_max, jnp.max(key_rows, axis=1)), jnp.max(own_terms, axis=1)
    )
    scaled = jnp.exp(key_rows - anchor[:, None, :] - (places + 1.0) * decay_rate)
    running_num = jnp.cumsum(scaled * value_rows, axis=1)
    running_den = jnp.cumsum(scaled, axis=1)
    past_num = jnp.concatenate([jnp.zeros_like(running_num[:, :1]), running_num[:, :-1]], axis=1)
    past_den = jnp.concatenate([jnp.zeros_like(running_den[:, :1]), running_den[:, :-1]], axis=1)
    fading = jnp.exp(places * decay_rate)
    carried = jnp.exp(running_max[:, None, :] + places * decay_rate - anchor[:, None, :])
    own_weight = jnp.exp(own_terms - anchor[:, None, :])
    top_num = past_num * fading + own_weight * value_rows + carried * numerator[:, None, :]
    top_den = past_den * fading + own_weight + carried * denominator[:, None, :]
    outputs = top_num / top_den
    final_terms = key_rows + (length - 1.0 - places) * decay_rate
    kept_max = running_max + length * decay_rate
    new_max = jnp.maximum(kept_max, jnp.max(final_terms, axis=1))
    final_weights = jnp.exp(final_terms - new_max[:, None, :])
    kept_weight = jnp.exp(kept_max - new_max)
    new_num = jnp.sum(final_weights * value_rows, axis=1) + kept_weight * numerator
    new_den = jnp.sum(final_weights, axis=1) + kept_weight * denominator
    return ((new_num, new_den, new_max), outputs)


def wkv_local(key_rows, value_rows, time_decay, time_first, in_num, in_den, in_max):
    decay_rate = -jnp.exp(time_decay)
    block_count = key_rows.shape[1] // BLOCK

    def arrange(values):
        return jnp.moveaxis(
            values.reshape(values.shape[0], block_count, BLOCK, values.shape[2]), 1, 0
        )

    block_step = jax.checkpoint(partial(wkv_block, decay_rate, time_first))
    state_out, outputs = lax.scan(
        block_step, (in_num, in_den, in_max), (arrange(key_rows), arrange(value_rows))
    )
    outputs = jnp.moveaxis(outputs, 0, 1).reshape(key_rows.shape)
    return (outputs, state_out)


def local_summary(key_rows, value_rows, decay_rate):
    length = key_rows.shape[1]
    places = jnp.arange(length, dtype=jnp.float32)[None, :, None]
    terms = key_rows + (length - 1.0 - places) * decay_rate
    top_term = jnp.max(terms, axis=1)
    weights_now = jnp.exp(terms - top_term[:, None, :])
    return (jnp.sum(weights_now * value_rows, axis=1), jnp.sum(weights_now, axis=1), top_term)


def combine_states(earlier_one, later_one):
    earlier_num, earlier_den, earlier_max, earlier_span = earlier_one
    later_num, later_den, later_max, later_span = later_one
    shifted_max = earlier_max + later_span
    top_both = jnp.maximum(shifted_max, later_max)
    weight_early = jnp.exp(shifted_max - top_both)
    weight_late = jnp.exp(later_max - top_both)
    return (
        earlier_num * weight_early + later_num * weight_late,
        earlier_den * weight_early + later_den * weight_late,
        top_both,
        earlier_span + later_span,
    )


def combine_grads(earlier_one, later_one):
    earlier_num, earlier_den, earlier_span = earlier_one
    later_num, later_den, later_span = later_one
    factor = jnp.exp(later_span)
    return (
        later_num + factor * earlier_num,
        later_den + factor * earlier_den,
        earlier_span + later_span,
    )


def local_plain(
    inputs,
    w_key,
    w_value,
    w_recept,
    w_output,
    w_ffn_key,
    w_ffn_value,
    w_ffn_recept,
    ln1_gain,
    ln1_bias,
    mix_key,
    mix_value,
    mix_recept,
    time_decay,
    time_first,
    ln2_gain,
    ln2_bias,
    ffn_mix_key,
    ffn_mix_recept,
    state_num,
    state_den,
    state_max,
    prev_att,
    prev_ffn,
    cotangent,
):
    position = lax.axis_index("seq")
    is_first = position == 0
    start_num = state_num.T
    start_den = state_den.T
    start_max = state_max.T
    before_att = prev_att.T
    before_ffn = prev_ffn.T
    input_rows = inputs.astype(jnp.float32)
    normed, norm_pull = jax.vjp(layer_norm, input_rows, ln1_gain, ln1_bias)
    from_left = from_behind(normed[:, -1, :], "seq", 1)
    edge_att = jnp.where(is_first, before_att, from_left)
    mixed_inputs, mix_pull = jax.vjp(token_mix, normed, edge_att, (mix_key, mix_value, mix_recept))
    key_in = mixed_inputs[0].astype(jnp.bfloat16)
    value_in = mixed_inputs[1].astype(jnp.bfloat16)
    recept_in = mixed_inputs[2].astype(jnp.bfloat16)
    key_rows = matmul(key_in, w_key)
    value_rows = matmul(value_in, w_value)
    recept_rows = matmul(recept_in, w_recept)
    decay_rate = -jnp.exp(time_decay)
    local_len = key_rows.shape[1]
    device_span = jnp.broadcast_to(local_len * decay_rate, start_num.shape)
    own_num, own_den, own_max = local_summary(key_rows, value_rows, decay_rate)
    first_element = combine_states(
        (start_num, start_den, start_max, jnp.zeros_like(device_span)),
        (own_num, own_den, own_max, device_span),
    )
    element_num = jnp.where(is_first, first_element[0], own_num)
    element_den = jnp.where(is_first, first_element[1], own_den)
    element_max = jnp.where(is_first, first_element[2], own_max)
    zero_rows = jnp.zeros_like(start_num)
    identity = (zero_rows, zero_rows, jnp.full_like(start_num, far_below), zero_rows)
    incoming = prefix(
        (element_num, element_den, element_max, device_span), "seq", combine_states, identity, False
    )
    prior_num, prior_den, prior_max = (incoming[0], incoming[1], incoming[2])
    in_num = jnp.where(is_first, start_num, prior_num)
    in_den = jnp.where(is_first, start_den, prior_den)
    in_max = jnp.where(is_first, start_max, prior_max)
    (mixed_rows, state_out), wkv_pull = jax.vjp(
        wkv_local, key_rows, value_rows, time_decay, time_first, in_num, in_den, in_max
    )
    gated, gate_pull = jax.vjp(gate_rows, recept_rows, mixed_rows)
    gated_low = gated.astype(jnp.bfloat16)
    attended = matmul(gated_low, w_output)
    middle = input_rows + attended
    normed_ffn, norm_ffn_pull = jax.vjp(layer_norm, middle, ln2_gain, ln2_bias)
    from_left_ffn = from_behind(normed_ffn[:, -1, :], "seq", 1)
    edge_ffn = jnp.where(is_first, before_ffn, from_left_ffn)
    ffn_inputs, ffn_mix_pull = jax.vjp(
        token_mix, normed_ffn, edge_ffn, (ffn_mix_key, ffn_mix_recept)
    )
    ffn_key_in = ffn_inputs[0].astype(jnp.bfloat16)
    ffn_recept_in = ffn_inputs[1].astype(jnp.bfloat16)
    hidden_pre = matmul(ffn_key_in, w_ffn_key)
    hidden = jnp.square(jax.nn.relu(hidden_pre)).astype(jnp.bfloat16)
    ffn_values = matmul(hidden, w_ffn_value)
    gate_now = jax.nn.sigmoid(matmul(ffn_recept_in, w_ffn_recept))
    block_out = (middle + gate_now * ffn_values).astype(jnp.bfloat16)
    grad_out = cotangent.astype(jnp.float32)
    grad_values = (grad_out * gate_now).astype(jnp.bfloat16)
    grad_gate = (grad_out * ffn_values * gate_now * (1.0 - gate_now)).astype(jnp.bfloat16)
    grad_hidden = matmul_back(grad_values, w_ffn_value)
    grad_pre = (grad_hidden * 2.0 * jax.nn.relu(hidden_pre)).astype(jnp.bfloat16)
    grad_w_ffn_value = outer_sum(hidden, grad_values)
    grad_w_ffn_key = outer_sum(ffn_key_in, grad_pre)
    grad_w_ffn_recept = outer_sum(ffn_recept_in, grad_gate)
    grad_normed_ffn, grad_edge_ffn, ffn_mix_grads = ffn_mix_pull(
        (matmul_back(grad_pre, w_ffn_key), matmul_back(grad_gate, w_ffn_recept))
    )
    from_right_ffn = from_behind(grad_edge_ffn, "seq", -1)
    grad_normed_ffn = grad_normed_ffn.at[:, -1, :].add(from_right_ffn)
    grad_middle, grad_ln2_gain, grad_ln2_bias = norm_ffn_pull(grad_normed_ffn)
    grad_middle = grad_middle + grad_out
    grad_attended = grad_middle.astype(jnp.bfloat16)
    grad_w_output = outer_sum(gated_low, grad_attended)
    grad_recept_full, grad_mixed = gate_pull(matmul_back(grad_attended, w_output))
    grad_recept = grad_recept_full.astype(jnp.bfloat16)
    zero_state = (zero_rows, zero_rows, zero_rows)
    first_pass = wkv_pull((grad_mixed, zero_state))
    unscale = jnp.exp(-in_max)
    local_grad_num = first_pass[4] * unscale
    local_grad_den = first_pass[5] * unscale
    later_grads = prefix(
        (local_grad_num, local_grad_den, device_span),
        "seq",
        combine_grads,
        (zero_rows, zero_rows, zero_rows),
        True,
    )
    exit_num, exit_den = (later_grads[0], later_grads[1])
    out_num, out_den, out_max = state_out
    lifting = jnp.exp(out_max)
    exit_cotangent = (
        exit_num * lifting,
        exit_den * lifting,
        (exit_num * out_num + exit_den * out_den) * lifting,
    )
    second_pass = wkv_pull((jnp.zeros_like(grad_mixed), exit_cotangent))
    grad_key_rows = (first_pass[0] + second_pass[0]).astype(jnp.bfloat16)
    grad_value_rows = (first_pass[1] + second_pass[1]).astype(jnp.bfloat16)
    grad_time_decay = first_pass[2] + second_pass[2]
    grad_time_first = first_pass[3] + second_pass[3]
    grad_start_num = first_pass[4] + second_pass[4]
    grad_start_den = first_pass[5] + second_pass[5]
    grad_start_max = first_pass[6] + second_pass[6]
    grad_w_key = outer_sum(key_in, grad_key_rows)
    grad_w_value = outer_sum(value_in, grad_value_rows)
    grad_w_recept = outer_sum(recept_in, grad_recept)
    grad_normed, grad_edge_att, mix_grads = mix_pull(
        (
            matmul_back(grad_key_rows, w_key),
            matmul_back(grad_value_rows, w_value),
            matmul_back(grad_recept, w_recept),
        )
    )
    from_right = from_behind(grad_edge_att, "seq", -1)
    grad_normed = grad_normed.at[:, -1, :].add(from_right)
    grad_input_ln, grad_ln1_gain, grad_ln1_bias = norm_pull(grad_normed)
    input_grad = (grad_input_ln + grad_middle).astype(jnp.bfloat16)
    start_num_grad = jnp.where(is_first, grad_start_num, 0.0).T
    start_den_grad = jnp.where(is_first, grad_start_den, 0.0).T
    start_max_grad = jnp.where(is_first, grad_start_max, 0.0).T
    edge_att_grad = jnp.where(is_first, grad_edge_att, 0.0).T
    edge_ffn_grad = jnp.where(is_first, grad_edge_ffn, 0.0).T
    row_parts = (
        lax.psum_scatter(grad_w_key, "seq", scatter_dimension=0, tiled=True),
        lax.psum_scatter(grad_w_value, "seq", scatter_dimension=0, tiled=True),
        lax.psum_scatter(grad_w_recept, "seq", scatter_dimension=0, tiled=True),
        lax.psum_scatter(grad_w_output, "seq", scatter_dimension=0, tiled=True),
        lax.psum_scatter(grad_w_ffn_key, "seq", scatter_dimension=0, tiled=True),
        lax.psum_scatter(grad_w_ffn_value, "seq", scatter_dimension=0, tiled=True),
        lax.psum_scatter(grad_w_ffn_recept, "seq", scatter_dimension=0, tiled=True),
        lax.psum_scatter(grad_ln1_gain, "seq", scatter_dimension=0, tiled=True),
        lax.psum_scatter(grad_ln1_bias, "seq", scatter_dimension=0, tiled=True),
        lax.psum_scatter(mix_grads[0], "seq", scatter_dimension=0, tiled=True),
        lax.psum_scatter(mix_grads[1], "seq", scatter_dimension=0, tiled=True),
        lax.psum_scatter(mix_grads[2], "seq", scatter_dimension=0, tiled=True),
        lax.psum_scatter(grad_time_decay, "seq", scatter_dimension=0, tiled=True),
        lax.psum_scatter(grad_time_first, "seq", scatter_dimension=0, tiled=True),
        lax.psum_scatter(grad_ln2_gain, "seq", scatter_dimension=0, tiled=True),
        lax.psum_scatter(grad_ln2_bias, "seq", scatter_dimension=0, tiled=True),
        lax.psum_scatter(ffn_mix_grads[0], "seq", scatter_dimension=0, tiled=True),
        lax.psum_scatter(ffn_mix_grads[1], "seq", scatter_dimension=0, tiled=True),
        lax.psum_scatter(start_num_grad, "seq", scatter_dimension=0, tiled=True),
        lax.psum_scatter(start_den_grad, "seq", scatter_dimension=0, tiled=True),
        lax.psum_scatter(start_max_grad, "seq", scatter_dimension=0, tiled=True),
        lax.psum_scatter(edge_att_grad, "seq", scatter_dimension=0, tiled=True),
        lax.psum_scatter(edge_ffn_grad, "seq", scatter_dimension=0, tiled=True),
    )
    matrix_parts = (
        lax.psum_scatter(row_parts[0], "batch", scatter_dimension=1, tiled=True),
        lax.psum_scatter(row_parts[1], "batch", scatter_dimension=1, tiled=True),
        lax.psum_scatter(row_parts[2], "batch", scatter_dimension=1, tiled=True),
        lax.psum_scatter(row_parts[3], "batch", scatter_dimension=1, tiled=True),
        lax.psum_scatter(row_parts[4], "batch", scatter_dimension=1, tiled=True),
        lax.psum_scatter(row_parts[5], "batch", scatter_dimension=1, tiled=True),
        lax.psum_scatter(row_parts[6], "batch", scatter_dimension=1, tiled=True),
    )
    vector_parts = lax.psum(
        (
            row_parts[7],
            row_parts[8],
            row_parts[9],
            row_parts[10],
            row_parts[11],
            row_parts[12],
            row_parts[13],
            row_parts[14],
            row_parts[15],
            row_parts[16],
            row_parts[17],
        ),
        "batch",
    )
    start_parts = (row_parts[18], row_parts[19], row_parts[20], row_parts[21], row_parts[22])
    return (
        block_out,
        input_grad,
        matrix_parts[0],
        matrix_parts[1],
        matrix_parts[2],
        matrix_parts[3],
        matrix_parts[4],
        matrix_parts[5],
        matrix_parts[6],
        vector_parts[0],
        vector_parts[1],
        vector_parts[2],
        vector_parts[3],
        vector_parts[4],
        vector_parts[5],
        vector_parts[6],
        vector_parts[7],
        vector_parts[8],
        vector_parts[9],
        vector_parts[10],
        start_parts[0],
        start_parts[1],
        start_parts[2],
        start_parts[3],
        start_parts[4],
    )


def solution(mesh):
    placed = (
        P("batch", "seq", None),
        P(),
        P(),
        P(),
        P(),
        P(),
        P(),
        P(),
        P(),
        P(),
        P(),
        P(),
        P(),
        P(),
        P(),
        P(),
        P(),
        P(),
        P(),
        P(None, "batch"),
        P(None, "batch"),
        P(None, "batch"),
        P(None, "batch"),
        P(None, "batch"),
        P("batch", "seq", None),
    )
    return jax.shard_map(
        local if fits(mesh) else local_plain,
        mesh=mesh,
        in_specs=placed,
        out_specs=(
            P("batch", "seq", None),
            P("batch", "seq", None),
            P("seq", "batch"),
            P("seq", "batch"),
            P("seq", "batch"),
            P("seq", "batch"),
            P("seq", "batch"),
            P("seq", "batch"),
            P("seq", "batch"),
            P("seq"),
            P("seq"),
            P("seq"),
            P("seq"),
            P("seq"),
            P("seq"),
            P("seq"),
            P("seq"),
            P("seq"),
            P("seq"),
            P("seq"),
            P("seq", "batch"),
            P("seq", "batch"),
            P("seq", "batch"),
            P("seq", "batch"),
            P("seq", "batch"),
        ),
        check_vma=False,
    )
```

```python
import functools
from functools import partial

import jax
import jax.numpy as jnp
from jax import lax
from jax.experimental import pallas as pl
from jax.experimental.pallas import tpu as pltpu
from jax.sharding import PartitionSpec as P

MESH = pl.DeviceIdType.MESH
F32 = jnp.float32
BF = jnp.bfloat16
NS = 8
T = 512
D = 1024
SUB = T // 8

NZ = 4
NM = 13
NK = 2 * NM
WIN = 10
WINZ = 8
WINF = 8
RA = 48
RE = 128 - RA
LAGS = [3, 5, 4, 5, 6, 6, 7, 8, 8]
RETIRE = 9
ROWS = 64


def normalize(v, gain, bias):
    mean = jnp.mean(v, axis=-1, keepdims=True)
    cen = v - mean
    var = jnp.mean(cen * cen, axis=-1, keepdims=True)
    return cen * lax.rsqrt(var + 1e-5) * gain + bias


def step_weights(delta):
    e = jnp.exp(-jnp.abs(delta))
    up = delta >= 0
    return jnp.where(up, 1.0, e), jnp.where(up, e, 1.0)


def join(early, late, span):
    em, en, ed = early
    lm, ln, ld = late
    a, b = step_weights(em + span - lm)
    return jnp.maximum(em + span, lm), a * en + b * ln, a * ed + b * ld


def contract0(a, b):
    return lax.dot_general(a, b, (((0,), (0,)), ((), ())), preferred_element_type=F32)


def contract1(a, b):
    return lax.dot_general(a, b, (((1,), (1,)), ((), ())), preferred_element_type=F32)


def pick(m, table):
    out = jnp.int32(table[0])
    for i, v in enumerate(table[1:], 1):
        out = jnp.where(m == i, v, out)
    return out


LEFT = (0, 9, 1, 9, 2, 9, 3, 9, 10, 4, 5, 8, 7)
RIGHT = (8, 4, 8, 5, 8, 6, 8, 7, 0, 1, 2, 3, 6)


class Place:
    def __init__(self):
        self.s, self.b = lax.axis_index("seq"), lax.axis_index("batch")
        self.z, self.x = self.s // 2, self.s % 2
        self.y, self.c = self.b // 2, self.b % 2

    def at(self, z=None, x=None, y=None, c=None):
        z = self.z if z is None else z
        x = self.x if x is None else x
        y = self.y if y is None else y
        c = self.c if c is None else c
        return (z * 2 + x, y * 2 + c)


def rcopy(src, dst, ss, rs, dev):
    return pltpu.make_async_remote_copy(src_ref=src, dst_ref=dst, send_sem=ss, recv_sem=rs, device_id=dev, device_id_type=MESH)


def block_kernel(*refs):
    x_h, cot_h, wk_h, wv_h, wr_h, wo_h, wfk_h, wfv_h, wfr_h = refs[:9]
    small_h = refs[9:25]
    o_blk, o_inp = refs[25:27]
    outs = refs[27:34]
    sm_out = refs[34]
    kin_h, vin_h, rin_h, gat_h, k_h, v_h, r_h, mix_h, m_h, n_h, d_h = refs[35:46]
    (ob, wbuf, Y, G, V, K, X, lanes, lanes2, st, sums, RS, es, er, fs, fr, ws, wr, edges, as_, ar, bs_, br_, us, ur,
     acc, sbuf, rF, rSA, rSE, rZA, rZE, smb, smr,
     obsem, wsem, stsem, bigsem, outsem, spsem, esem, fsem, asem, bsem, wssem, wrsem,
     s0s, s0r, sFs, sFr, sSs, sSr, sZs, sZr, osem, msem, mss, msr, vsem) = refs[46:-16]
    (g1, b1, mk, mv, mr, td, tf, g2, b2, fmk, fmr, sn, sd, sm, pa, pf) = refs[-16:]
    small_loads = [pltpu.make_async_copy(src, dst, vsem) for src, dst in zip(small_h, refs[-16:])]
    for cp in small_loads:
        cp.start()
    me = Place()
    z, x, y, c, s = me.z, me.x, me.y, me.c, me.s
    left, right = (jnp.maximum(s - 1, 0), me.b), (jnp.minimum(s + 1, NS - 1), me.b)

    bar = pltpu.get_barrier_semaphore()

    def sig(dev):
        pl.semaphore_signal(bar, inc=1, device_id=dev, device_id_type=MESH)

    sig(me.at(c=1 - c))
    sig(me.at(y=1 - y))
    for i in range(1, NS):
        sig((lax.rem(s + i, NS), me.b))

    def local(src, dst, sem):
        return pltpu.make_async_copy(src, dst, sem)

    def op_load(src, slot):
        return local(src, ob.at[slot], obsem.at[slot])

    def slab_columns(src, j, dst, sem):
        return [local(src.at[:, pl.ds(i * 512 + j * 128, 128)], dst.at[:, pl.ds(i * 128, 128)], sem) for i in range(8)]

    def slab_rows(src, j, dst, sem):
        return [local(src.at[pl.ds(i * 512 + j * 128, 128), :], dst.at[pl.ds(i * 128, 128), :], sem) for i in range(8)]

    weights = [("p", wk_h), ("p", wv_h), ("p", wr_h), ("p", wo_h), ("p", wfr_h)]
    for j in range(4):
        weights += [("c", wfk_h, j), ("r", wfv_h, j)]
    weights += [("p", wfr_h), ("p", wo_h), ("p", wr_h), ("p", wv_h), ("p", wk_h)]

    def w_start(i):
        if i >= len(weights):
            return
        kind, src, *j = weights[i]
        dst, sem = wbuf.at[i % 3], wsem.at[i % 3]
        if kind == "p":
            local(src, dst, sem).start()
        else:
            for cp in (slab_columns if kind == "c" else slab_rows)(src, j[0], dst, sem):
                cp.start()

    def w_wait(i):
        local(wo_h, wbuf.at[i % 3], wsem.at[i % 3]).wait()

    def fs_of(k):
        h = lax.rem(k, 2)
        return jnp.where(h == 0, x, y), jnp.where(h == 0, y, x)

    def partner(h):
        a, b = me.at(x=1 - x), me.at(y=1 - y)
        return (jnp.where(h == 0, a[0], b[0]), jnp.where(h == 0, a[1], b[1]))

    def copy0(k):
        return rcopy(sbuf.at[lax.rem(k, 2)], acc.at[lax.rem(k, WIN)], s0s.at[lax.rem(k, 2)], s0r.at[lax.rem(k, WIN)], me.at(c=1 - c))

    def copyF(k):
        f, _ = fs_of(k)
        return rcopy(acc.at[lax.rem(k, WIN), 1 - f], rF.at[lax.rem(k, WINF)], sFs.at[lax.rem(k, WIN)], sFr.at[lax.rem(k, WINF)], partner(lax.rem(k, 2)))

    def copySA(k):
        f, g = fs_of(k)
        w, v = lax.rem(k, WIN), lax.rem(k, WINZ)
        return rcopy(acc.at[w, f, 1 - g, :, pl.ds(0, RA)], rSA.at[v], sSs.at[v, 0], sSr.at[v, 0], partner(1 - lax.rem(k, 2)))

    def copySE(k):
        f, g = fs_of(k)
        w, v = lax.rem(k, WIN), lax.rem(k, WINZ)
        return rcopy(acc.at[w, f, 1 - g, z, pl.ds(RA, RE)], rSE.at[v], sSs.at[v, 1], sSr.at[v, 1], partner(1 - lax.rem(k, 2)))

    def unit(k, q, late):
        f, g = fs_of(k)
        w = lax.rem(k, WIN)
        return acc.at[w, f, g, q, pl.ds(0, RA)] if late else acc.at[w, f, :, q, pl.ds(RA, RE)]

    def zbuf(k, slot, late):
        return (rZA if late else rZE).at[lax.rem(k, WINZ), slot]

    def copyR(k, q, late):
        i = int(late)
        return rcopy(unit(k, q, late), zbuf(k, q + 1, late), sZs.at[lax.rem(k, WINZ), i], sZr.at[lax.rem(k, WINZ), i, q + 1], me.at(z=z + 1))

    def copyL(k, q, late):
        i = int(late)
        return rcopy(unit(k, q, late), zbuf(k, q, late), sZs.at[lax.rem(k, WINZ), i], sZr.at[lax.rem(k, WINZ), i, q], me.at(z=z - 1))

    def add_into(dst, src):
        dst[...] = dst[...] + src[...]

    def zsub(k, tau, late):
        @pl.when(z <= tau)
        def _():
            q = NZ - 1 - tau + z

            @pl.when(z > 0)
            def _():
                copyR(k, q, late).wait_recv()
                add_into(unit(k, q, late), zbuf(k, q + 1, late))

            copyR(k, q, late).start()

        @pl.when(NZ - 1 - z <= tau)
        def _():
            q = tau - (NZ - 1 - z)

            @pl.when(z < NZ - 1)
            def _():
                copyL(k, q, late).wait_recv()
                add_into(unit(k, q, late), zbuf(k, q, late))

            copyL(k, q, late).start()

    def zfin(k, late):
        @pl.when(z > 0)
        def _():
            copyR(k, z, late).wait_recv()
            add_into(unit(k, z, late), zbuf(k, z + 1, late))

        @pl.when(z < NZ - 1)
        def _():
            copyL(k, z, late).wait_recv()
            add_into(unit(k, z, late), zbuf(k, z, late))

    def gradient(k, core, write):
        h, m = lax.rem(k, 2), k // 2
        ls, rs = pick(m, LEFT), pick(m, RIGHT)
        cols = jnp.concatenate(
            [ob[rs, :, pl.ds(pl.multiple_of((2 * yy + core) * 256 + h * 128, 128), 128)] for yy in range(2)], axis=1)

        def group(g, _):
            res = contract0(ob[ls, :, pl.ds(pl.multiple_of(g * 512, 512), 512)], cols)
            for i in range(4):
                zz, xx = g * 2 + i // 2, i % 2
                for yy in range(2):
                    f = jnp.where(h == 0, xx, yy)
                    g2_ = jnp.where(h == 0, yy, xx)
                    write(f, g2_, zz, res[i * 128:(i + 1) * 128, yy * 128:(yy + 1) * 128])
            return 0

        lax.fori_loop(0, 2, group, 0)

    def taskP(k):
        @pl.when(k >= 2)
        def _():
            copy0(k - 2).wait_send()

        slot = lax.rem(k, 2)

        def write(f, g, zz, v):
            sbuf[slot, f, g, zz] = v

        gradient(k, 1 - c, write)
        copy0(k).start()

    def task1(k):
        copy0(k).wait_recv()
        w = lax.rem(k, WIN)

        def write(f, g, zz, v):
            acc[w, f, g, zz] = acc[w, f, g, zz] + v

        gradient(k, c, write)
        copyF(k).start()

    def task2(k):
        copyF(k).wait_recv()
        f, _ = fs_of(k)
        w = lax.rem(k, WIN)

        def body(i, _):
            add_into(acc.at[w, f, i // NZ, lax.rem(i, NZ)], rF.at[lax.rem(k, WINF), i // NZ, lax.rem(i, NZ)])
            return 0

        lax.fori_loop(0, 2 * NZ, body, 0)
        copySA(k).start()
        zsub(k, 0, False)

    def taskSA(k):
        copySA(k).wait_recv()
        f, g = fs_of(k)
        w = lax.rem(k, WIN)
        add_into(acc.at[w, f, g, :, pl.ds(0, RA)], rSA.at[lax.rem(k, WINZ)])
        zsub(k, 0, True)

    def taskFinE(k):
        zfin(k, False)
        copySE(k).start()

    def taskSE(k):
        copySE(k).wait_recv()
        f, g = fs_of(k)
        w = lax.rem(k, WIN)
        add_into(acc.at[w, f, g, z, pl.ds(RA, RE)], rSE.at[lax.rem(k, WINZ)])
        src = acc.at[w, f, g, z]
        h, m = lax.rem(k, 2), k // 2
        half = pl.ds(pl.multiple_of(h * 128, 128), 128)
        for j in range(4):
            @pl.when(m == 2 * j)
            def _(j=j):
                local(src, outs[5].at[pl.ds(j * 128, 128), half], osem.at[lax.rem(k, WIN)]).start()

            @pl.when(m == 2 * j + 1)
            def _(j=j):
                local(src, outs[4].at[:, pl.ds(pl.multiple_of(h * 512 + j * 128, 128), 128)], osem.at[lax.rem(k, WIN)]).start()
        for mm, i in ((8, 6), (9, 3), (10, 2), (11, 1), (12, 0)):
            @pl.when(m == mm)
            def _(i=i):
                local(src, outs[i].at[:, half], osem.at[lax.rem(k, WIN)]).start()

    def retire(k):
        copyF(k).wait_send()
        copySA(k).wait_send()
        copySE(k).wait_send()
        f, g = fs_of(k)
        w, v = lax.rem(k, WIN), lax.rem(k, WINZ)
        for late in (False, True):
            others = pl.ds(0, NZ - 1)
            sent = acc.at[w, f, g, others, pl.ds(0, RA)] if late else acc.at[w, f, :, others, pl.ds(RA, RE)]
            rcopy(sent, sent, sZs.at[v, int(late)], sZr.at[v, int(late), 0], me.at(c=1 - c)).wait_send()
        local(acc.at[lax.rem(k, WIN), 0, 0, 0], outs[0].at[:, pl.ds(0, 128)], osem.at[lax.rem(k, WIN)]).wait()

    stages = [
        (RETIRE, retire),
        (LAGS[7], lambda k: zfin(k, True)),
        (LAGS[8], taskSE),
        (LAGS[6], lambda k: zsub(k, 2, True)),
        (LAGS[5], lambda k: zsub(k, 1, True)),
        (LAGS[4], taskFinE),
        (LAGS[3], lambda k: zsub(k, 2, False)),
        (LAGS[2], lambda k: zsub(k, 1, False)),
        (LAGS[1], taskSA),
        (1, task1),
        (LAGS[0], task2),
        (0, taskP),
    ]

    def sm_copy(step):
        if step == 0:
            return rcopy(smb.at[0], smr.at[0], mss.at[0], msr.at[0], me.at(c=1 - c))
        if step == 1:
            return rcopy(smb.at[2], smr.at[1], mss.at[1], msr.at[1], me.at(y=1 - y))
        return rcopy(smb.at[1, 1 - x], smr.at[2, 0], mss.at[2], msr.at[2], me.at(x=1 - x))

    def sm_z(q, to_right):
        if to_right:
            return rcopy(smb.at[1, x, q], smr.at[3, 0, q], mss.at[3 + q], msr.at[3 + q], me.at(z=z + 1))
        return rcopy(smb.at[1, x, q], smr.at[3, 1, q], mss.at[3 + q], msr.at[3 + NZ + q], me.at(z=z - 1))

    vec = lax.broadcasted_iota(jnp.int32, (2, NZ, 16, 128), 2) < 11

    def sm1():
        sm_copy(0).wait_recv()
        smb[2] = smb[0] + jnp.where(vec, smr[0], 0.0)
        sm_copy(1).start()

    def sm2():
        sm_copy(1).wait_recv()
        smb[1] = smb[2] + jnp.where(vec, smr[1], 0.0)
        sm_copy(2).start()

    def sm3():
        sm_copy(2).wait_recv()
        smb[1, x] = smb[1, x] + smr[2, 0]

    def smz(tau):
        @pl.when(z <= tau)
        def _():
            q = NZ - 1 - tau + z

            @pl.when(z > 0)
            def _():
                sm_z(q, True).wait_recv()
                smb[1, x, q] = smb[1, x, q] + smr[3, 0, q]

            sm_z(q, True).start()

        @pl.when(NZ - 1 - z <= tau)
        def _():
            q = tau - (NZ - 1 - z)

            @pl.when(z < NZ - 1)
            def _():
                sm_z(q, False).wait_recv()
                smb[1, x, q] = smb[1, x, q] + smr[3, 1, q]

            sm_z(q, False).start()

    def sm_fin():
        @pl.when(z > 0)
        def _():
            sm_z(z, True).wait_recv()
            smb[1, x, z] = smb[1, x, z] + smr[3, 0, z]

        @pl.when(z < NZ - 1)
        def _():
            sm_z(z, False).wait_recv()
            smb[1, x, z] = smb[1, x, z] + smr[3, 1, z]

        local(smb.at[1, x, z], sm_out, msem).start()

    def tiles(n, rows, body):
        def step(i, _):
            body(i, pl.ds(pl.multiple_of(i * rows, rows), rows))
            return 0

        lax.fori_loop(0, n, step, 0)

    def widen(slot):
        def body(i, rows):
            for g in range(8):
                lanes[g, rows, :] = ob[slot, rows, g * 128:g * 128 + 128].astype(F32)

        tiles(T // 64, 64, body)

    def spread(i, count):
        return jnp.concatenate(
            [jnp.concatenate([lanes[g, pl.ds(i * count + a, 8, stride=SUB), :] for g in range(8)], axis=1) for a in range(count)], axis=0)

    def unspread(i, count, value):
        for a in range(count):
            for g in range(8):
                lanes2[g, pl.ds(i * count + a, 8, stride=SUB), :] = value[a * 8:a * 8 + 8, g * 128:g * 128 + 128]

    def narrow(slot, dst, sem):
        def body(i, rows):
            for g in range(8):
                ob[slot, rows, g * 128:g * 128 + 128] = lanes2[g, rows, :].astype(BF)

        tiles(T // 64, 64, body)
        local(ob.at[slot], dst, sem).start()

    def halves(body):
        tiles(2, 512, body)

    def gate_step():
        w_wait(4)

        def mm(i, cols):
            G[:, cols] = jnp.dot(ob[10], wbuf[4 % 3, :, cols], preferred_element_type=F32)

        halves(mm)
        w_start(7)

        def body(i, rows):
            gate = jax.nn.sigmoid(G[rows, :])
            G[rows, :] = gate
            ob[8, rows, :] = (spread(i, 4) * gate).astype(BF)

        tiles(T // 32, 32, body)

    def hid(j):
        w_wait(5 + 2 * j)
        slot = (5 + 2 * j) % 3

        def mm(i, cols):
            up = jnp.maximum(jnp.dot(ob[9], wbuf[slot, :, cols], preferred_element_type=F32), 0.0)
            X[pl.ds(0, T), cols] = up
            ob[j, :, cols] = (up * up).astype(BF)

        halves(mm)

    def gpre(j):
        w_wait(6 + 2 * j)
        slot = (6 + 2 * j) % 3

        def mm(i, cols):
            back = contract1(ob[8], wbuf[slot, cols, :])
            ob[4 + j, :, cols] = (back * 2.0 * X[pl.ds(0, T), cols]).astype(BF)

        halves(mm)

    def gk_step(j):
        slot = (5 + 2 * j) % 3

        def mm(i, cols):
            part = contract1(ob[4 + j], wbuf[slot, cols, :])
            K[pl.ds(0, T), cols] = part if j == 0 else K[pl.ds(0, T), cols] + part

        halves(mm)
        w_start(5 + 2 * j + 3)

    def ffv(j):
        slot = (6 + 2 * j) % 3

        def mm(i, cols):
            part = jnp.dot(ob[j], wbuf[slot, :, cols], preferred_element_type=F32)
            V[pl.ds(0, T), cols] = part if j == 0 else V[pl.ds(0, T), cols] + part

        halves(mm)
        w_start(6 + 2 * j + 3)

    def big_load(src, dst, i):
        return local(src, dst.at[pl.ds(0, T)], bigsem.at[i])

    def block_step():
        def body(i, rows):
            gate, values = G[rows, :], V[rows, :]
            unspread(i, 4, Y[rows, :] + gate * values)
            ob[0, rows, :] = (spread(i, 4) * values * gate * (1.0 - gate)).astype(BF)

        tiles(T // 32, 32, body)
        narrow(5, o_blk, outsem.at[0])

    row8 = lax.broadcasted_iota(jnp.int32, (8, D), 0)

    def tail(buf):
        buf[T:T + 8, :] = jnp.where(row8 == 7, 0.0, pltpu.roll(buf[0:8, :], 7, 0))

    def edge(src, dst, sem, dev):
        return rcopy(src, dst, sem.at[0], sem.at[1], dev)

    def recept_back():
        w_wait(13)

        def mm(i, cols):
            V[pl.ds(0, T), cols] = contract1(ob[0], wbuf[13 % 3, cols, :])

        halves(mm)
        w_start(16)
        tail(K)
        tail(V)
        es[...] = K[0:8, :] * (1.0 - fmk[...]) + V[0:8, :] * (1.0 - fmr[...])

        @pl.when(s > 0)
        def _():
            edge(es, er, esem, left).start()

    def fold(v):
        return sum(v[i:i + 8] for i in range(8, ROWS, 8)) + v[0:8]

    row_of = lax.broadcasted_iota(jnp.int32, (ROWS, D), 0)

    def centre(v):
        mean = jnp.mean(v, axis=-1, keepdims=True)
        cen = v - mean
        inv = lax.rsqrt(jnp.mean(cen * cen, axis=-1, keepdims=True) + 1e-5)
        return cen * inv, inv

    def ln_back(grad, n, inv, gain):
        h = grad * gain[...]
        return inv * (h - jnp.mean(h, axis=-1, keepdims=True) - n * jnp.mean(h * n, axis=-1, keepdims=True))

    def ln_tile(i, rows, n, gain, bias, parts, arrived, sum_rows, ln_sums):
        later = pl.ds(pl.multiple_of(i * ROWS + 8, 8), ROWS)
        normed = n * gain[...] + bias[...]
        grad = 0.0
        if arrived is not None:
            grad = jnp.where(jnp.logical_and(row_of == ROWS - 1, i == T // ROWS - 1), arrived, 0.0)
        for (buf, w), r in zip(parts, sum_rows):
            now, nxt = buf[rows, :], buf[later, :]
            grad = grad + now * w[...] + nxt * (1.0 - w[...])
            sums[r] = sums[r] + fold(normed * (now - nxt))
        sums[ln_sums[0]] = sums[ln_sums[0]] + fold(grad * n)
        sums[ln_sums[1]] = sums[ln_sums[1]] + fold(grad)
        return grad

    def wait_from_right(cp):
        @pl.when(s < NS - 1)
        def _():
            cp.wait_recv()

    def middle_back(lo, hi):
        arrived = jnp.where(s == NS - 1, 0.0, er[0:1, :]) if hi == T // ROWS else None

        def body(i, _):
            rows = pl.ds(pl.multiple_of(i * ROWS, ROWS), ROWS)
            n, inv = centre(Y[rows, :])
            grad = ln_tile(i, rows, n, g2, b2, ((K, fmk), (V, fmr)), arrived, (9, 10), (7, 8))
            gm = spread(i, ROWS // 8) + ln_back(grad, n, inv, g2)
            G[rows, :] = gm
            ob[1, rows, :] = gm.astype(BF)
            return 0

        lax.fori_loop(lo, hi, body, 0)

    def middle_end():
        for r, buf in ((9, K), (10, V)):
            sums[r, 0:1, :] = sums[r, 0:1, :] - buf[0:1, :] * edges[8:9, :]
        sums[15, 0:1, :] = es[0:1, :]

    def gated_back():
        w_wait(14)

        def mm(i, cols):
            V[pl.ds(0, T), cols] = contract1(ob[1], wbuf[14 % 3, cols, :])

        halves(mm)
        w_start(17)
        big_load(r_h, X, 0).wait()
        big_load(mix_h, K, 1).wait()

        def body(i, rows):
            sg = jax.nn.sigmoid(X[rows, :])
            gg = V[rows, :]
            ob[2, rows, :] = (gg * K[rows, :] * sg * (1.0 - sg)).astype(BF)
            V[rows, :] = gg * sg

        tiles(T // 32, 32, body)

    streams = (k_h, m_h, d_h, n_h, v_h)

    def st_copies(blk, slot, count):
        rows = pl.ds(pl.multiple_of(blk * 64, 64), 64)
        return [local(src.at[rows, :], st.at[slot, i], stsem.at[slot, i]) for i, src in enumerate(streams[:count])]

    def st_start(blk, count):
        for cp in st_copies(blk, lax.rem(blk, 2), count):
            cp.start()

    def st_next(blk, count):
        for cp in st_copies(blk, lax.rem(blk, 2), count):
            cp.wait()

        @pl.when(blk > 0)
        def _():
            st_start(blk - 1, count)


    def wide(v, cols):
        return jnp.broadcast_to(v[:, cols], (8, 512))

    def first_pass(lo):
        def block(i, _):
            blk = 7 - lo - i
            slot = lax.rem(blk, 2)
            st_next(blk, 3)
            for h in range(2):
                cols = slice(h * 512, h * 512 + 512)
                w, bonus = wide(decay, cols), wide(tf[...], cols)

                def step(jj, carry):
                    R, S = carry
                    j = 7 - jj
                    at = pl.ds(pl.multiple_of(j * 8, 8), 8)
                    rows = pl.ds(pl.multiple_of(blk * 64 + j * 8, 8), 8)
                    k, m, d = st[slot, 0, at, cols], st[slot, 1, at, cols], st[slot, 2, at, cols]
                    p, u = step_weights(m - (bonus + k))
                    q = V[rows, cols] / (p * d + u)
                    qp = p * q
                    V[rows, cols] = qp
                    X[rows, cols] = u * q
                    a, _ = step_weights(m + w - k)
                    return qp + a * R, qp * K[rows, cols] + a * S

                R, S = lax.fori_loop(0, 8, step, (RS[0, :, cols], RS[1, :, cols]), unroll=2)
                RS[0, :, cols] = R
                RS[1, :, cols] = S

                @pl.when(blk == 7)
                def _():
                    RS[2, :, cols] = jnp.maximum(st[slot, 1, 56:64, cols] + w, st[slot, 0, 56:64, cols])

                @pl.when(blk == 0)
                def _():
                    RS[3, :, cols] = st[slot, 1, 0:8, cols]
            return 0

        lax.fori_loop(0, 4, block, 0)

    def suffix(value, dist, fill):
        return jnp.where(row8 >= 8 - dist, fill, pltpu.roll(value, 8 - dist, 0))


    def state_copy(src, dst):
        return rcopy(ws, wr.at[src], wssem.at[dst], wrsem.at[src], (dst, me.b))

    def first_end():
        A = jnp.exp(jnp.minimum(RS[3] + span - RS[2], 0.0))
        R, S = RS[0], RS[1]
        for dist in (1, 2, 4):
            R = R + A * suffix(R, dist, 0.0)
            S = S + A * suffix(S, dist, 0.0)
            A = A * suffix(A, dist, 1.0)
        RS[0], RS[1], RS[4] = R, S, A
        ws[...] = jnp.where(row8 == 0, R[0:1], jnp.where(row8 == 1, S[0:1], RS[3, 0:1, :]))
        for i in range(NS - 1):
            @pl.when(i < s)
            def _(i=i):
                state_copy(s, i).start()

    def second_start():
        RS[5] = jnp.zeros((8, D), F32)
        RS[6] = jnp.zeros((8, D), F32)
        for i in range(1, NS):
            @pl.when(i > s)
            def _(i=i):
                state_copy(i, 0).wait_recv()
                far = jnp.exp(jnp.minimum(RS[2, 7:8, :] + (i - s - 1).astype(F32) * (8.0 * span) - wr[i, 2:3, :], 0.0))
                RS[5, 0:1, :] = RS[5, 0:1, :] + far * wr[i, 0:1, :]
                RS[6, 0:1, :] = RS[6, 0:1, :] + far * wr[i, 1:2, :]
        Rin, Sin = RS[5, 0:1, :], RS[6, 0:1, :]
        A = RS[4]
        R = RS[0] + A * Rin
        S = RS[1] + A * Sin
        RS[0] = jnp.where(row8 == 7, Rin, pltpu.roll(R, 7, 0))
        RS[1] = jnp.where(row8 == 7, Sin, pltpu.roll(S, 7, 0))

    def second_pass(lo, n):
        def block(i, _):
            blk = 7 - lo - i
            slot = lax.rem(blk, 2)
            st_next(blk, 5)
            for h in range(2):
                cols = slice(h * 512, h * 512 + 512)
                w = wide(decay, cols)

                def one(j, carry):
                    R, S, first, slow = carry
                    at = pl.ds(pl.multiple_of(j * 8, 8), 8)
                    rows = pl.ds(pl.multiple_of(blk * 64 + j * 8, 8), 8)
                    k, m, d, n_, v = (st[slot, q, at, cols] for q in range(5))
                    mixed, qp, uq = K[rows, cols], V[rows, cols], X[rows, cols]
                    a, b = step_weights(m + w - k)
                    own = uq * (v - mixed)
                    gv = uq + b * R
                    gk = own + b * (v * R - S)
                    first = first + own
                    slow = slow + a * (n_ * R - d * S)
                    return (qp + a * R, qp * mixed + a * S, first, slow), gk, gv

                def step(jj, carry):
                    j = 3 - jj
                    carry, gk1, gv1 = one(2 * j + 1, carry)
                    carry, gk0, gv0 = one(2 * j, carry)
                    pair = pl.ds(pl.multiple_of(blk * 64 + j * 16, 16), 16)
                    ob[6, pair, cols] = jnp.concatenate([gk0, gk1], axis=0).astype(BF)
                    ob[3, pair, cols] = jnp.concatenate([gv0, gv1], axis=0).astype(BF)
                    return carry

                R, S, first, slow = lax.fori_loop(0, 4, step, (RS[0, :, cols], RS[1, :, cols], sums[6, :, cols], sums[5, :, cols]))
                RS[0, :, cols] = R
                RS[1, :, cols] = S
                sums[6, :, cols] = first
                sums[5, :, cols] = slow
            return 0

        lax.fori_loop(0, n, block, 0)

    def second_end():
        gn, gd = RS[0, 0:1, :], -RS[1, 0:1, :]
        sums[11, 0:1, :] = gn
        sums[12, 0:1, :] = gd
        sums[13, 0:1, :] = sn[...] * gn + sd[...] * gd
        sums[5] = sums[5] * decay

    def input_mm(i, slot, buf):
        w_wait(i)

        def mm(_, cols):
            buf[pl.ds(0, T), cols] = contract1(ob[slot], wbuf[i % 3, cols, :])

        halves(mm)
        tail(buf)

    def input_edge():
        fs[...] = K[0:8, :] * (1.0 - mk[...]) + V[0:8, :] * (1.0 - mv[...]) + X[0:8, :] * (1.0 - mr[...])

        @pl.when(s > 0)
        def _():
            edge(fs, fr, fsem, left).start()

    def input_back(lo, hi):
        arrived = jnp.where(s == NS - 1, 0.0, fr[0:1, :]) if hi == T // ROWS else None

        def body(i, _):
            rows = pl.ds(pl.multiple_of(i * ROWS, ROWS), ROWS)
            n, inv = centre(spread(i, ROWS // 8))
            grad = ln_tile(i, rows, n, g1, b1, ((K, mk), (V, mv), (X, mr)), arrived, (2, 3, 4), (0, 1))
            unspread(i, ROWS // 8, G[rows, :] + ln_back(grad, n, inv, g1))
            return 0

        lax.fori_loop(lo, hi, body, 0)

    def input_end():
        for r, buf in ((2, K), (3, V), (4, X)):
            sums[r, 0:1, :] = sums[r, 0:1, :] - buf[0:1, :] * edges[0:1, :]
        sums[14, 0:1, :] = fs[0:1, :]
        narrow(0, o_inp, outsem.at[1])
        alone = jnp.where(s == 0, 1.0, 0.0)
        rows = [jnp.sum(sums[r], axis=0, keepdims=True) for r in range(11)] + [jnp.where(s == 0, sums[r, 0:1, :], 0.0) for r in range(11, 16)]
        table = jnp.concatenate(rows, axis=0)
        for g in range(8):
            smb[0, g % 2, g // 2] = table[:, g * 128:g * 128 + 128]
        sm_copy(0).start()

    def start_all(*copies):
        for cp in copies:
            cp.start()

    compute = {
        1: [lambda: gpre(0), lambda: gk_step(0), lambda: hid(1)],
        2: [lambda: ffv(0), lambda: gpre(1)],
        3: [lambda: gk_step(1), lambda: hid(2)],
        4: [lambda: ffv(1), lambda: gpre(2)],
        5: [lambda: gk_step(2), lambda: hid(3), lambda: start_all(op_load(gat_h, 4))],
        6: [lambda: ffv(2), lambda: gpre(3)],
        7: [lambda: gk_step(3), lambda: ffv(3)],
        8: [block_step],
        9: [recept_back],
        10: [lambda: middle_back(0, 4)],
        11: [lambda: start_all(big_load(r_h, X, 0)), lambda: wait_from_right(edge(es, er, esem, left)), lambda: middle_back(4, 8), middle_end,
             lambda: start_all(big_load(mix_h, K, 1)), lambda: st_start(7, 3),
             lambda: local(ob.at[5], o_blk, outsem.at[0]).wait(), lambda: start_all(op_load(rin_h, 5))],
        12: [gated_back],
        13: [lambda: first_pass(0)],
        14: [lambda: first_pass(4), first_end, lambda: st_start(7, 5)],
        15: [second_start, lambda: second_pass(0, 2), lambda: start_all(op_load(vin_h, 8))],
        16: [lambda: second_pass(2, 3)],
        17: [lambda: second_pass(5, 3), second_end, lambda: start_all(op_load(kin_h, 7), op_load(x_h, 9))],
        18: [lambda: input_mm(15, 2, X), lambda: input_mm(16, 3, V)],
        19: [lambda: input_mm(17, 6, K), input_edge, lambda: op_load(x_h, 9).wait(), lambda: widen(9)],
        20: [lambda: input_back(0, 4)],
        21: [lambda: wait_from_right(edge(fs, fr, fsem, left)), lambda: input_back(4, 8), input_end],
        23: [sm1],
        24: [sm2],
        25: [sm3, lambda: smz(0)],
        26: [lambda: smz(1)],
        27: [lambda: smz(2)],
        28: [sm_fin],
    }
    landed = {18: (gat_h, 4), 20: (rin_h, 5), 22: (vin_h, 8), 24: (kin_h, 7)}

    def spill(src, dst, i):
        return local(src, dst, spsem.at[i])

    kb, vb, rb, nb = G, V, X, K
    to_next = rcopy(as_, ar, asem.at[0], asem.at[1], right)
    to_next2 = rcopy(bs_, br_, bsem.at[0], bsem.at[1], right)

    def wait_from_left(cp):
        @pl.when(s > 0)
        def _():
            cp.wait_recv()

    def send_right(cp):
        @pl.when(s < NS - 1)
        def _():
            cp.start()

    def norm1(i, rows):
        v = spread(i, 8)
        Y[rows, :] = v
        nb[pl.ds(pl.multiple_of(i * 64 + 8, 8), 64), :] = normalize(v, g1[...], b1[...])

    def header(start_row):
        nb[0:8, :] = jnp.where(row8 == 0, start_row, pltpu.roll(nb[T:T + 8, :], 1, 0))

    def mix(pairs, i):
        rows = pl.ds(pl.multiple_of(i * 64, 64), 64)
        before = nb[rows, :]
        now = nb[pl.ds(pl.multiple_of(i * 64 + 8, 8), 64), :]
        for slot, w in pairs:
            ob[slot, rows, :] = (now * w[...] + before * (1.0 - w[...])).astype(BF)

    def project(i, slot, dst):
        w_wait(i)
        dst[pl.ds(0, T), :] = jnp.dot(ob[slot], wbuf[i % 3], preferred_element_type=F32)
        w_start(i + 3)

    start_all(op_load(x_h, 4), op_load(cot_h, 5))
    for i in range(3):
        w_start(i)
    local(K.at[pl.ds(0, 16)], V.at[pl.ds(0, 16)], vsem).wait()
    decay = -jnp.exp(td[...])
    span = SUB * decay
    op_load(x_h, 4).wait()
    as_[...] = normalize(ob[4, T - 16:T, :].astype(F32), g1[...], b1[...])[8:16, :]
    pl.semaphore_wait(bar, NS + 1)
    send_right(to_next)
    widen(4)
    tiles(T // 64, 64, norm1)
    wait_from_left(to_next)
    header(jnp.where(s == 0, pa[...], ar[7:8, :]))
    edges[0:8, :] = nb[0:8, :]
    tiles(T // 64, 64, lambda i, rows: mix(((0, mk), (1, mv), (2, mr)), i))
    start_all(spill(ob.at[0], kin_h, 0), spill(ob.at[1], vin_h, 1), spill(ob.at[2], rin_h, 2))
    project(0, 0, kb)
    project(1, 1, vb)
    start_all(spill(kb, k_h, 3), spill(vb.at[pl.ds(0, T)], v_h, 4))

    wide_decay = jnp.broadcast_to(decay, (8, D))

    def own_step(j, state):
        rows = pl.ds(pl.multiple_of(j * 8, 8), 8)
        m, n, d = state
        k, v = kb[rows, :], vb[rows, :]
        low = m + wide_decay
        a, b = step_weights(low - k)
        return jnp.maximum(low, k), a * n + b * v, a * d + b

    total = lax.fori_loop(1, SUB, own_step, (kb[0:8, :], vb[0:8, :], jnp.ones((8, D), F32)), unroll=7)

    def earlier(state, dist):
        m, n, d = (pltpu.roll(p, dist, 0) for p in state)
        out = row8 < dist
        return jnp.where(out, -1e30, m), jnp.where(out, 0.0, n), jnp.where(out, 0.0, d)

    for dist in (1, 2, 4):
        total = join(earlier(total, dist), total, dist * span)
    before_own = earlier(total, 1)
    us[...] = jnp.where(row8 == 0, total[0][7:8], jnp.where(row8 == 1, total[1][7:8], total[2][7:8]))

    def reach_copy(src, dst):
        return rcopy(us, ur.at[src], wssem.at[dst], wrsem.at[src], (dst, me.b))

    for i in range(1, NS):
        @pl.when(s < i)
        def _(i=i):
            reach_copy(s, i).start()

    project(2, 2, rb)
    start_all(spill(rb.at[pl.ds(0, T)], r_h, 5))
    op_load(cot_h, 5).wait()
    widen(5)
    RS[0, 0:1, :] = sm[...]
    RS[1, 0:1, :] = sn[...]
    RS[2, 0:1, :] = sd[...]
    for i in range(NS - 1):
        @pl.when(i < s)
        def _(i=i):
            reach_copy(i, NS - 1).wait_recv()
            now = join(tuple(RS[r, 0:1, :] for r in range(3)), tuple(ur[i, r:r + 1, :] for r in range(3)), 8.0 * span)
            for r in range(3):
                RS[r, 0:1, :] = now[r]

    base = tuple(RS[r, 0:1, :] for r in range(3))
    lifted = (base[0] + row8.astype(F32) * span, jnp.broadcast_to(base[1], (8, D)), jnp.broadcast_to(base[2], (8, D)))
    for r, v in enumerate(join(lifted, before_own, 0.0)):
        RS[r] = v

    def state_spills(blk, slot):
        rows = pl.ds(pl.multiple_of(blk * 64, 64), 64)
        return [local(st.at[slot, q], dst.at[rows, :], stsem.at[slot, q]) for q, dst in enumerate((mix_h, m_h, n_h, d_h))]

    def outputs(blk, _):
        slot = lax.rem(blk, 2)

        @pl.when(blk >= 2)
        def _():
            for cp in state_spills(blk - 2, slot):
                cp.wait()

        for h in range(2):
            cols = slice(h * 512, h * 512 + 512)
            w, bonus = wide(decay, cols), wide(tf[...], cols)

            def one(j, state):
                at = pl.ds(pl.multiple_of(j * 8, 8), 8)
                rows = pl.ds(pl.multiple_of(blk * 64 + j * 8, 8), 8)
                m, n, d = state
                k, v = kb[rows, cols], vb[rows, cols]
                p, u = step_weights(m - (bonus + k))
                mixed = (p * n + u * v) / (p * d + u)
                for q, val in enumerate((mixed, m, n, d)):
                    st[slot, q, at, cols] = val
                low = m + w
                a, b = step_weights(low - k)
                return (jnp.maximum(low, k), a * n + b * v, a * d + b), jax.nn.sigmoid(rb[rows, cols]) * mixed

            def two(i, state):
                state, ga = one(2 * i, state)
                state, gb = one(2 * i + 1, state)
                ob[3, pl.ds(pl.multiple_of(blk * 64 + i * 16, 16), 16), cols] = jnp.concatenate([ga, gb], axis=0).astype(BF)
                return state

            for r, v in enumerate(lax.fori_loop(0, 4, two, tuple(RS[r, :, cols] for r in range(3)), unroll=4)):
                RS[r, :, cols] = v
        start_all(*state_spills(blk, slot))
        return 0

    lax.fori_loop(0, 8, outputs, 0)
    start_all(spill(ob.at[3], gat_h, 6))
    spill(kb, k_h, 3).wait()
    project(3, 3, G)

    def norm2(i, rows):
        v = Y[rows, :] + G[rows, :]
        Y[rows, :] = v
        nb[pl.ds(pl.multiple_of(i * 64 + 8, 8), 64), :] = normalize(v, g2[...], b2[...])

    norm2(T // 64 - 1, pl.ds(T - 64, 64))
    bs_[...] = nb[T:T + 8, :]
    send_right(to_next2)
    tiles(T // 64 - 1, 64, norm2)

    def mix2(i, _):
        mix(((9, fmk), (10, fmr)), i)
        return 0

    lax.fori_loop(1, T // 64, mix2, 0)
    wait_from_left(to_next2)
    header(jnp.where(s == 0, pf[...], br_[7:8, :]))
    edges[8:16, :] = nb[0:8, :]
    mix2(0, 0)

    sums[...] = jnp.zeros_like(sums)
    gate_step()
    spill(ob.at[0], kin_h, 0).wait()
    spill(rb.at[pl.ds(0, T)], r_h, 5).wait()
    hid(0)
    RS[...] = jnp.zeros_like(RS)
    for i, (src, dst) in enumerate(((ob.at[1], vin_h), (ob.at[2], rin_h))):
        spill(src, dst, 1 + i).wait()
    spill(vb.at[pl.ds(0, T)], v_h, 4).wait()
    spill(ob.at[3], gat_h, 6).wait()
    for blk in (6, 7):
        for cp in state_spills(blk, blk % 2):
            cp.wait()

    def tick(t, _):
        for at, (src, slot) in landed.items():
            @pl.when(t == at)
            def _(src=src, slot=slot):
                op_load(src, slot).wait()

        for lag, task in stages:
            k = t - lag

            @pl.when(jnp.logical_and(k >= (2 if lag < 2 else 0), k < NK))
            def _(k=k, task=task):
                task(k)

        for at, steps in compute.items():
            @pl.when(t == at)
            def _(steps=steps):
                for step in steps:
                    step()
        return 0

    for k in range(2):
        taskP(jnp.int32(k))
    for k in range(2):
        task1(jnp.int32(k))
    lax.fori_loop(1, NK + RETIRE, tick, 0)

    copy0(NK - 2).wait_send()
    copy0(NK - 1).wait_send()
    for i in range(3):
        sm_copy(i).wait_send()
    for q in range(NZ):
        @pl.when(q != z)
        def _(q=q):
            sm_z(q, True).wait_send()

    @pl.when(s > 0)
    def _():
        edge(es, er, esem, left).wait_send()
        edge(fs, fr, fsem, left).wait_send()

    @pl.when(s < NS - 1)
    def _():
        to_next.wait_send()
        to_next2.wait_send()

    for i in range(NS):
        @pl.when(i < s)
        def _(i=i):
            state_copy(s, i).wait_send()

        @pl.when(i > s)
        def _(i=i):
            reach_copy(s, i).wait_send()
    local(smb.at[1, x, z], sm_out, msem).wait()
    local(ob.at[0], o_inp, outsem.at[1]).wait()


def block_call(x, cot, mats, vectors, states):
    anyspec = pl.BlockSpec(memory_space=pl.ANY)
    S = jax.ShapeDtypeStruct
    sem = pltpu.SemaphoreType.DMA
    M = pltpu.VMEM
    row = M((8, D), F32)
    return pl.pallas_call(
        block_kernel,
        out_shape=[S((T, D), BF)] * 2 + [S((128, 256), F32)] * 4 + [S((128, 1024), F32), S((512, 256), F32), S((128, 256), F32), S((16, 128), F32)]
        + [S((T, D), BF)] * 4 + [S((T, D), F32)] * 7,
        in_specs=[anyspec] * 25,
        out_specs=[anyspec] * 21,
        scratch_shapes=[
            M((11, T, D), BF), M((3, D, D), BF), M((T, D), F32), M((T, D), F32), M((T + 8, D), F32), M((T + 8, D), F32), M((T + 8, D), F32),
            M((8, T, 128), F32), M((8, T, 128), F32), M((2, 5, 64, D), F32), M((16, 8, D), F32), M((7, 8, D), F32),
            row, row, row, row, row, M((NS, 8, D), F32), M((16, D), F32), row, row, row, row, row, M((NS, 8, D), F32),
            M((WIN, 2, 2, NZ, 128, 128), F32), M((2, 2, 2, NZ, 128, 128), F32), M((WINF, 2, NZ, 128, 128), F32),
            M((WINZ, NZ, RA, 128), F32), M((WINZ, RE, 128), F32), M((WINZ, NZ + 1, RA, 128), F32), M((WINZ, NZ + 1, 2, RE, 128), F32),
            M((3, 2, NZ, 16, 128), F32), M((4, 2, NZ, 16, 128), F32),
            sem((11,)), sem((3,)), sem((2, 5)), sem((2,)), sem((2,)), sem((7,)), sem((2,)), sem((2,)), sem((2,)), sem((2,)), sem((NS,)), sem((NS,)),
            sem((2,)), sem((WIN,)), sem((WIN,)), sem((WINF,)), sem((WINZ, 2)), sem((WINZ, 2)),
            sem((WINZ, 2)), sem((WINZ, 2, NZ + 1)), sem((WIN,)), sem, sem((3 + NZ,)), sem((3 + 2 * NZ,)), sem,
        ] + [M((1, D), F32)] * 16,
        compiler_params=pltpu.CompilerParams(collective_id=0, has_side_effects=True, vmem_limit_bytes=67043328),
        name="block",
    )(x, cot, *mats, *vectors, *states)[:10]

def finish_kernel(*refs):
    ins, outs, (scratch, sems) = refs[:10], refs[10:35], (refs[35:-2], refs[-2:])
    into, out = sems
    loads = [pltpu.make_async_copy(src, buf, into.at[i]) for i, (src, buf) in enumerate(zip(ins, scratch))]
    for cp in loads:
        cp.start()
    stores = []
    for i in range(10):
        loads[i].wait()
        if i < 9:
            stores.append(pltpu.make_async_copy(scratch[i], outs[i], out.at[i]))
            stores[-1].start()
        else:
            for r in range(16):
                stores.append(pltpu.make_async_copy(scratch[i].at[pl.ds(r, 1)], outs[9 + r], out.at[9 + r]))
                stores[-1].start()
    for cp in stores:
        cp.wait()


def finish_call(parts):
    anyspec = pl.BlockSpec(memory_space=pl.ANY)
    return pl.pallas_call(
        finish_kernel,
        out_shape=[jax.ShapeDtypeStruct(p.shape, p.dtype) for p in parts[:9]] + [jax.ShapeDtypeStruct((1, 128), F32)] * 16,
        in_specs=[anyspec] * 10,
        out_specs=[anyspec] * 25,
        scratch_shapes=[pltpu.VMEM(p.shape, p.dtype) for p in parts] + [pltpu.SemaphoreType.DMA((10,)), pltpu.SemaphoreType.DMA((25,))],
        name="finish",
    )(*parts)


def fits(mesh):
    return (mesh.shape["seq"], mesh.shape["batch"]) == (2 * NZ, 4)


def local(
    inputs,
    w_key,
    w_value,
    w_recept,
    w_output,
    w_ffn_key,
    w_ffn_value,
    w_ffn_recept,
    ln1_gain,
    ln1_bias,
    mix_key,
    mix_value,
    mix_recept,
    time_decay,
    time_first,
    ln2_gain,
    ln2_bias,
    ffn_mix_key,
    ffn_mix_recept,
    state_num,
    state_den,
    state_max,
    prev_att,
    prev_ffn,
    cotangent,
):
    rows = inputs.reshape(T, D)
    vectors = [
        v.reshape(1, D)
        for v in (
            ln1_gain,
            ln1_bias,
            mix_key,
            mix_value,
            mix_recept,
            time_decay,
            time_first,
            ln2_gain,
            ln2_bias,
            ffn_mix_key,
            ffn_mix_recept,
        )
    ]
    states = [v.reshape(1, D) for v in (state_num, state_den, state_max, prev_att, prev_ffn)]
    parts = block_call(
        rows,
        cotangent.reshape(T, D),
        [w_key, w_value, w_recept, w_output, w_ffn_key, w_ffn_value, w_ffn_recept],
        vectors,
        states,
    )
    block_out, input_grad, *rest = finish_call(parts)
    return (
        block_out.reshape(inputs.shape),
        input_grad.reshape(inputs.shape),
        *rest[:7],
        *[v.reshape(128) for v in rest[7:18]],
        *[v.reshape(128, 1) for v in rest[18:]],
    )


BLOCK = 64


far_below = -1e30


def from_behind(block, axis, distance):
    devices = range(lax.axis_size(axis))
    route = [(i - distance, i) for i in devices if i - distance in devices]
    return lax.ppermute(block, axis, route)


def prefix(value, axis, join, neutral, backward):
    count, mine = (lax.axis_size(axis), lax.axis_index(axis))
    pieces = jax.tree.map(lambda part: lax.all_gather(part, axis), value)
    if backward:
        pieces = jax.tree.map(lambda part: part[::-1], pieces)
        mine = count - 1 - mine
    total = jax.tree.map(
        lambda part, zero: jnp.full_like(part, 0) + jnp.asarray(zero, part.dtype), value, neutral
    )

    def turn(position, total):
        longer = join(total, jax.tree.map(lambda part: part[position], pieces))
        return jax.tree.map(lambda new, old: jnp.where(position < mine, new, old), longer, total)

    return lax.fori_loop(0, count - 1, turn, total)


def layer_norm(values, ln_gain, ln_bias):
    centred = values - jnp.mean(values, axis=-1, keepdims=True)
    spread = jnp.mean(centred * centred, axis=-1, keepdims=True)
    return centred * lax.rsqrt(spread + 1e-05) * ln_gain + ln_bias


def matmul(operand, matrix):
    return lax.dot_general(
        operand, matrix, (((operand.ndim - 1,), (0,)), ((), ())), preferred_element_type=jnp.float32
    )


def matmul_back(gradient, matrix):
    return lax.dot_general(
        gradient,
        matrix,
        (((gradient.ndim - 1,), (1,)), ((), ())),
        preferred_element_type=jnp.float32,
    )


def outer_sum(operand, gradient):
    flat_operand = operand.reshape(-1, operand.shape[-1])
    flat_gradient = gradient.reshape(-1, gradient.shape[-1])
    return lax.dot_general(
        flat_operand, flat_gradient, (((0,), (0,)), ((), ())), preferred_element_type=jnp.float32
    )


def token_mix(normed, edge_row, mix_vectors):
    earlier = jnp.concatenate([edge_row[:, None, :], normed[:, :-1, :]], axis=1)
    return tuple((normed * member + earlier * (1.0 - member) for member in mix_vectors))


def gate_rows(recept_rows, mixed_rows):
    return jax.nn.sigmoid(recept_rows) * mixed_rows


def wkv_block(decay_rate, time_first, state_in, inputs_now):
    numerator, denominator, running_max = state_in
    key_rows, value_rows = inputs_now
    length = key_rows.shape[1]
    places = jnp.arange(length, dtype=jnp.float32)[None, :, None]
    own_terms = time_first + key_rows
    anchor = jnp.maximum(
        jnp.maximum(running_max, jnp.max(key_rows, axis=1)), jnp.max(own_terms, axis=1)
    )
    scaled = jnp.exp(key_rows - anchor[:, None, :] - (places + 1.0) * decay_rate)
    running_num = jnp.cumsum(scaled * value_rows, axis=1)
    running_den = jnp.cumsum(scaled, axis=1)
    past_num = jnp.concatenate([jnp.zeros_like(running_num[:, :1]), running_num[:, :-1]], axis=1)
    past_den = jnp.concatenate([jnp.zeros_like(running_den[:, :1]), running_den[:, :-1]], axis=1)
    fading = jnp.exp(places * decay_rate)
    carried = jnp.exp(running_max[:, None, :] + places * decay_rate - anchor[:, None, :])
    own_weight = jnp.exp(own_terms - anchor[:, None, :])
    top_num = past_num * fading + own_weight * value_rows + carried * numerator[:, None, :]
    top_den = past_den * fading + own_weight + carried * denominator[:, None, :]
    outputs = top_num / top_den
    final_terms = key_rows + (length - 1.0 - places) * decay_rate
    kept_max = running_max + length * decay_rate
    new_max = jnp.maximum(kept_max, jnp.max(final_terms, axis=1))
    final_weights = jnp.exp(final_terms - new_max[:, None, :])
    kept_weight = jnp.exp(kept_max - new_max)
    new_num = jnp.sum(final_weights * value_rows, axis=1) + kept_weight * numerator
    new_den = jnp.sum(final_weights, axis=1) + kept_weight * denominator
    return ((new_num, new_den, new_max), outputs)


def wkv_local(key_rows, value_rows, time_decay, time_first, in_num, in_den, in_max):
    decay_rate = -jnp.exp(time_decay)
    block_count = key_rows.shape[1] // BLOCK

    def arrange(values):
        return jnp.moveaxis(
            values.reshape(values.shape[0], block_count, BLOCK, values.shape[2]), 1, 0
        )

    block_step = jax.checkpoint(partial(wkv_block, decay_rate, time_first))
    state_out, outputs = lax.scan(
        block_step, (in_num, in_den, in_max), (arrange(key_rows), arrange(value_rows))
    )
    outputs = jnp.moveaxis(outputs, 0, 1).reshape(key_rows.shape)
    return (outputs, state_out)


def local_summary(key_rows, value_rows, decay_rate):
    length = key_rows.shape[1]
    places = jnp.arange(length, dtype=jnp.float32)[None, :, None]
    terms = key_rows + (length - 1.0 - places) * decay_rate
    top_term = jnp.max(terms, axis=1)
    weights_now = jnp.exp(terms - top_term[:, None, :])
    return (jnp.sum(weights_now * value_rows, axis=1), jnp.sum(weights_now, axis=1), top_term)


def combine_states(earlier_one, later_one):
    earlier_num, earlier_den, earlier_max, earlier_span = earlier_one
    later_num, later_den, later_max, later_span = later_one
    shifted_max = earlier_max + later_span
    top_both = jnp.maximum(shifted_max, later_max)
    weight_early = jnp.exp(shifted_max - top_both)
    weight_late = jnp.exp(later_max - top_both)
    return (
        earlier_num * weight_early + later_num * weight_late,
        earlier_den * weight_early + later_den * weight_late,
        top_both,
        earlier_span + later_span,
    )


def combine_grads(earlier_one, later_one):
    earlier_num, earlier_den, earlier_span = earlier_one
    later_num, later_den, later_span = later_one
    factor = jnp.exp(later_span)
    return (
        later_num + factor * earlier_num,
        later_den + factor * earlier_den,
        earlier_span + later_span,
    )


def local_plain(
    inputs,
    w_key,
    w_value,
    w_recept,
    w_output,
    w_ffn_key,
    w_ffn_value,
    w_ffn_recept,
    ln1_gain,
    ln1_bias,
    mix_key,
    mix_value,
    mix_recept,
    time_decay,
    time_first,
    ln2_gain,
    ln2_bias,
    ffn_mix_key,
    ffn_mix_recept,
    state_num,
    state_den,
    state_max,
    prev_att,
    prev_ffn,
    cotangent,
):
    position = lax.axis_index("seq")
    is_first = position == 0
    start_num = state_num.T
    start_den = state_den.T
    start_max = state_max.T
    before_att = prev_att.T
    before_ffn = prev_ffn.T
    input_rows = inputs.astype(jnp.float32)
    normed, norm_pull = jax.vjp(layer_norm, input_rows, ln1_gain, ln1_bias)
    from_left = from_behind(normed[:, -1, :], "seq", 1)
    edge_att = jnp.where(is_first, before_att, from_left)
    mixed_inputs, mix_pull = jax.vjp(token_mix, normed, edge_att, (mix_key, mix_value, mix_recept))
    key_in = mixed_inputs[0].astype(jnp.bfloat16)
    value_in = mixed_inputs[1].astype(jnp.bfloat16)
    recept_in = mixed_inputs[2].astype(jnp.bfloat16)
    key_rows = matmul(key_in, w_key)
    value_rows = matmul(value_in, w_value)
    recept_rows = matmul(recept_in, w_recept)
    decay_rate = -jnp.exp(time_decay)
    local_len = key_rows.shape[1]
    device_span = jnp.broadcast_to(local_len * decay_rate, start_num.shape)
    own_num, own_den, own_max = local_summary(key_rows, value_rows, decay_rate)
    first_element = combine_states(
        (start_num, start_den, start_max, jnp.zeros_like(device_span)),
        (own_num, own_den, own_max, device_span),
    )
    element_num = jnp.where(is_first, first_element[0], own_num)
    element_den = jnp.where(is_first, first_element[1], own_den)
    element_max = jnp.where(is_first, first_element[2], own_max)
    zero_rows = jnp.zeros_like(start_num)
    identity = (zero_rows, zero_rows, jnp.full_like(start_num, far_below), zero_rows)
    incoming = prefix(
        (element_num, element_den, element_max, device_span), "seq", combine_states, identity, False
    )
    prior_num, prior_den, prior_max = (incoming[0], incoming[1], incoming[2])
    in_num = jnp.where(is_first, start_num, prior_num)
    in_den = jnp.where(is_first, start_den, prior_den)
    in_max = jnp.where(is_first, start_max, prior_max)
    (mixed_rows, state_out), wkv_pull = jax.vjp(
        wkv_local, key_rows, value_rows, time_decay, time_first, in_num, in_den, in_max
    )
    gated, gate_pull = jax.vjp(gate_rows, recept_rows, mixed_rows)
    gated_low = gated.astype(jnp.bfloat16)
    attended = matmul(gated_low, w_output)
    middle = input_rows + attended
    normed_ffn, norm_ffn_pull = jax.vjp(layer_norm, middle, ln2_gain, ln2_bias)
    from_left_ffn = from_behind(normed_ffn[:, -1, :], "seq", 1)
    edge_ffn = jnp.where(is_first, before_ffn, from_left_ffn)
    ffn_inputs, ffn_mix_pull = jax.vjp(
        token_mix, normed_ffn, edge_ffn, (ffn_mix_key, ffn_mix_recept)
    )
    ffn_key_in = ffn_inputs[0].astype(jnp.bfloat16)
    ffn_recept_in = ffn_inputs[1].astype(jnp.bfloat16)
    hidden_pre = matmul(ffn_key_in, w_ffn_key)
    hidden = jnp.square(jax.nn.relu(hidden_pre)).astype(jnp.bfloat16)
    ffn_values = matmul(hidden, w_ffn_value)
    gate_now = jax.nn.sigmoid(matmul(ffn_recept_in, w_ffn_recept))
    block_out = (middle + gate_now * ffn_values).astype(jnp.bfloat16)
    grad_out = cotangent.astype(jnp.float32)
    grad_values = (grad_out * gate_now).astype(jnp.bfloat16)
    grad_gate = (grad_out * ffn_values * gate_now * (1.0 - gate_now)).astype(jnp.bfloat16)
    grad_hidden = matmul_back(grad_values, w_ffn_value)
    grad_pre = (grad_hidden * 2.0 * jax.nn.relu(hidden_pre)).astype(jnp.bfloat16)
    grad_w_ffn_value = outer_sum(hidden, grad_values)
    grad_w_ffn_key = outer_sum(ffn_key_in, grad_pre)
    grad_w_ffn_recept = outer_sum(ffn_recept_in, grad_gate)
    grad_normed_ffn, grad_edge_ffn, ffn_mix_grads = ffn_mix_pull(
        (matmul_back(grad_pre, w_ffn_key), matmul_back(grad_gate, w_ffn_recept))
    )
    from_right_ffn = from_behind(grad_edge_ffn, "seq", -1)
    grad_normed_ffn = grad_normed_ffn.at[:, -1, :].add(from_right_ffn)
    grad_middle, grad_ln2_gain, grad_ln2_bias = norm_ffn_pull(grad_normed_ffn)
    grad_middle = grad_middle + grad_out
    grad_attended = grad_middle.astype(jnp.bfloat16)
    grad_w_output = outer_sum(gated_low, grad_attended)
    grad_recept_full, grad_mixed = gate_pull(matmul_back(grad_attended, w_output))
    grad_recept = grad_recept_full.astype(jnp.bfloat16)
    zero_state = (zero_rows, zero_rows, zero_rows)
    first_pass = wkv_pull((grad_mixed, zero_state))
    unscale = jnp.exp(-in_max)
    local_grad_num = first_pass[4] * unscale
    local_grad_den = first_pass[5] * unscale
    later_grads = prefix(
        (local_grad_num, local_grad_den, device_span),
        "seq",
        combine_grads,
        (zero_rows, zero_rows, zero_rows),
        True,
    )
    exit_num, exit_den = (later_grads[0], later_grads[1])
    out_num, out_den, out_max = state_out
    lifting = jnp.exp(out_max)
    exit_cotangent = (
        exit_num * lifting,
        exit_den * lifting,
        (exit_num * out_num + exit_den * out_den) * lifting,
    )
    second_pass = wkv_pull((jnp.zeros_like(grad_mixed), exit_cotangent))
    grad_key_rows = (first_pass[0] + second_pass[0]).astype(jnp.bfloat16)
    grad_value_rows = (first_pass[1] + second_pass[1]).astype(jnp.bfloat16)
    grad_time_decay = first_pass[2] + second_pass[2]
    grad_time_first = first_pass[3] + second_pass[3]
    grad_start_num = first_pass[4] + second_pass[4]
    grad_start_den = first_pass[5] + second_pass[5]
    grad_start_max = first_pass[6] + second_pass[6]
    grad_w_key = outer_sum(key_in, grad_key_rows)
    grad_w_value = outer_sum(value_in, grad_value_rows)
    grad_w_recept = outer_sum(recept_in, grad_recept)
    grad_normed, grad_edge_att, mix_grads = mix_pull(
        (
            matmul_back(grad_key_rows, w_key),
            matmul_back(grad_value_rows, w_value),
            matmul_back(grad_recept, w_recept),
        )
    )
    from_right = from_behind(grad_edge_att, "seq", -1)
    grad_normed = grad_normed.at[:, -1, :].add(from_right)
    grad_input_ln, grad_ln1_gain, grad_ln1_bias = norm_pull(grad_normed)
    input_grad = (grad_input_ln + grad_middle).astype(jnp.bfloat16)
    start_num_grad = jnp.where(is_first, grad_start_num, 0.0).T
    start_den_grad = jnp.where(is_first, grad_start_den, 0.0).T
    start_max_grad = jnp.where(is_first, grad_start_max, 0.0).T
    edge_att_grad = jnp.where(is_first, grad_edge_att, 0.0).T
    edge_ffn_grad = jnp.where(is_first, grad_edge_ffn, 0.0).T
    row_parts = (
        lax.psum_scatter(grad_w_key, "seq", scatter_dimension=0, tiled=True),
        lax.psum_scatter(grad_w_value, "seq", scatter_dimension=0, tiled=True),
        lax.psum_scatter(grad_w_recept, "seq", scatter_dimension=0, tiled=True),
        lax.psum_scatter(grad_w_output, "seq", scatter_dimension=0, tiled=True),
        lax.psum_scatter(grad_w_ffn_key, "seq", scatter_dimension=0, tiled=True),
        lax.psum_scatter(grad_w_ffn_value, "seq", scatter_dimension=0, tiled=True),
        lax.psum_scatter(grad_w_ffn_recept, "seq", scatter_dimension=0, tiled=True),
        lax.psum_scatter(grad_ln1_gain, "seq", scatter_dimension=0, tiled=True),
        lax.psum_scatter(grad_ln1_bias, "seq", scatter_dimension=0, tiled=True),
        lax.psum_scatter(mix_grads[0], "seq", scatter_dimension=0, tiled=True),
        lax.psum_scatter(mix_grads[1], "seq", scatter_dimension=0, tiled=True),
        lax.psum_scatter(mix_grads[2], "seq", scatter_dimension=0, tiled=True),
        lax.psum_scatter(grad_time_decay, "seq", scatter_dimension=0, tiled=True),
        lax.psum_scatter(grad_time_first, "seq", scatter_dimension=0, tiled=True),
        lax.psum_scatter(grad_ln2_gain, "seq", scatter_dimension=0, tiled=True),
        lax.psum_scatter(grad_ln2_bias, "seq", scatter_dimension=0, tiled=True),
        lax.psum_scatter(ffn_mix_grads[0], "seq", scatter_dimension=0, tiled=True),
        lax.psum_scatter(ffn_mix_grads[1], "seq", scatter_dimension=0, tiled=True),
        lax.psum_scatter(start_num_grad, "seq", scatter_dimension=0, tiled=True),
        lax.psum_scatter(start_den_grad, "seq", scatter_dimension=0, tiled=True),
        lax.psum_scatter(start_max_grad, "seq", scatter_dimension=0, tiled=True),
        lax.psum_scatter(edge_att_grad, "seq", scatter_dimension=0, tiled=True),
        lax.psum_scatter(edge_ffn_grad, "seq", scatter_dimension=0, tiled=True),
    )
    matrix_parts = (
        lax.psum_scatter(row_parts[0], "batch", scatter_dimension=1, tiled=True),
        lax.psum_scatter(row_parts[1], "batch", scatter_dimension=1, tiled=True),
        lax.psum_scatter(row_parts[2], "batch", scatter_dimension=1, tiled=True),
        lax.psum_scatter(row_parts[3], "batch", scatter_dimension=1, tiled=True),
        lax.psum_scatter(row_parts[4], "batch", scatter_dimension=1, tiled=True),
        lax.psum_scatter(row_parts[5], "batch", scatter_dimension=1, tiled=True),
        lax.psum_scatter(row_parts[6], "batch", scatter_dimension=1, tiled=True),
    )
    vector_parts = lax.psum(
        (
            row_parts[7],
            row_parts[8],
            row_parts[9],
            row_parts[10],
            row_parts[11],
            row_parts[12],
            row_parts[13],
            row_parts[14],
            row_parts[15],
            row_parts[16],
            row_parts[17],
        ),
        "batch",
    )
    start_parts = (row_parts[18], row_parts[19], row_parts[20], row_parts[21], row_parts[22])
    return (
        block_out,
        input_grad,
        matrix_parts[0],
        matrix_parts[1],
        matrix_parts[2],
        matrix_parts[3],
        matrix_parts[4],
        matrix_parts[5],
        matrix_parts[6],
        vector_parts[0],
        vector_parts[1],
        vector_parts[2],
        vector_parts[3],
        vector_parts[4],
        vector_parts[5],
        vector_parts[6],
        vector_parts[7],
        vector_parts[8],
        vector_parts[9],
        vector_parts[10],
        start_parts[0],
        start_parts[1],
        start_parts[2],
        start_parts[3],
        start_parts[4],
    )


def solution(mesh):
    placed = (
        P("batch", "seq", None),
        P(),
        P(),
        P(),
        P(),
        P(),
        P(),
        P(),
        P(),
        P(),
        P(),
        P(),
        P(),
        P(),
        P(),
        P(),
        P(),
        P(),
        P(),
        P(None, "batch"),
        P(None, "batch"),
        P(None, "batch"),
        P(None, "batch"),
        P(None, "batch"),
        P("batch", "seq", None),
    )
    return jax.shard_map(
        local if fits(mesh) else local_plain,
        mesh=mesh,
        in_specs=placed,
        out_specs=(
            P("batch", "seq", None),
            P("batch", "seq", None),
            P("seq", "batch"),
            P("seq", "batch"),
            P("seq", "batch"),
            P("seq", "batch"),
            P("seq", "batch"),
            P("seq", "batch"),
            P("seq", "batch"),
            P("seq"),
            P("seq"),
            P("seq"),
            P("seq"),
            P("seq"),
            P("seq"),
            P("seq"),
            P("seq"),
            P("seq"),
            P("seq"),
            P("seq"),
            P("seq", "batch"),
            P("seq", "batch"),
            P("seq", "batch"),
            P("seq", "batch"),
            P("seq", "batch"),
        ),
        check_vma=False,
    )
```

```python
import functools
from functools import partial

import jax
import jax.numpy as jnp
from jax import lax
from jax.experimental import pallas as pl
from jax.experimental.pallas import tpu as pltpu
from jax.sharding import PartitionSpec as P

MESH = pl.DeviceIdType.MESH
F32 = jnp.float32
BF = jnp.bfloat16
NS = 8
T = 512
D = 1024
SUB = T // 8

NZ = 4
NM = 13
NK = 2 * NM
WIN = 10
WINZ = 8
WINF = 8
RA = 48
RE = 128 - RA
LAGS = [3, 5, 4, 5, 6, 6, 7, 8, 8]
RETIRE = 9
ROWS = 64


def normalize(v, gain, bias):
    mean = jnp.mean(v, axis=-1, keepdims=True)
    cen = v - mean
    var = jnp.mean(cen * cen, axis=-1, keepdims=True)
    return cen * lax.rsqrt(var + 1e-5) * gain + bias


def step_weights(delta):
    e = jnp.exp(-jnp.abs(delta))
    up = delta >= 0
    return jnp.where(up, 1.0, e), jnp.where(up, e, 1.0)


def join(early, late, span):
    em, en, ed = early
    lm, ln, ld = late
    a, b = step_weights(em + span - lm)
    return jnp.maximum(em + span, lm), a * en + b * ln, a * ed + b * ld


def contract0(a, b):
    return lax.dot_general(a, b, (((0,), (0,)), ((), ())), preferred_element_type=F32)


def contract1(a, b):
    return lax.dot_general(a, b, (((1,), (1,)), ((), ())), preferred_element_type=F32)


def pick(m, table):
    out = jnp.int32(table[0])
    for i, v in enumerate(table[1:], 1):
        out = jnp.where(m == i, v, out)
    return out


LEFT = (0, 9, 1, 9, 2, 9, 3, 9, 10, 4, 5, 8, 7)
RIGHT = (8, 4, 8, 5, 8, 6, 8, 7, 0, 1, 2, 3, 6)


class Place:
    def __init__(self):
        self.s, self.b = lax.axis_index("seq"), lax.axis_index("batch")
        self.z, self.x = self.s // 2, self.s % 2
        self.y, self.c = self.b // 2, self.b % 2

    def at(self, z=None, x=None, y=None, c=None):
        z = self.z if z is None else z
        x = self.x if x is None else x
        y = self.y if y is None else y
        c = self.c if c is None else c
        return (z * 2 + x, y * 2 + c)


def rcopy(src, dst, ss, rs, dev):
    return pltpu.make_async_remote_copy(src_ref=src, dst_ref=dst, send_sem=ss, recv_sem=rs, device_id=dev, device_id_type=MESH)


def block_kernel(*refs):
    x_h, cot_h, wk_h, wv_h, wr_h, wo_h, wfk_h, wfv_h, wfr_h = refs[:9]
    small_h = refs[9:25]
    o_blk, o_inp = refs[25:27]
    outs = refs[27:34]
    sm_out = refs[34]
    kin_h, vin_h, rin_h, gat_h, k_h, v_h, r_h, mix_h, m_h, n_h, d_h = refs[35:46]
    (ob, wbuf, Y, G, V, K, X, lanes, lanes2, st, sums, RS, es, er, fs, fr, ws, wr, edges, as_, ar, bs_, br_, us, ur,
     acc, sbuf, rF, rSA, rSE, rZA, rZE, smb, smr,
     obsem, wsem, stsem, bigsem, outsem, spsem, esem, fsem, asem, bsem, wssem, wrsem,
     s0s, s0r, sFs, sFr, sSs, sSr, sZs, sZr, osem, msem, mss, msr, vsem) = refs[46:-16]
    (g1, b1, mk, mv, mr, td, tf, g2, b2, fmk, fmr, sn, sd, sm, pa, pf) = refs[-16:]
    small_loads = [pltpu.make_async_copy(src, dst, vsem) for src, dst in zip(small_h, refs[-16:])]
    for cp in small_loads:
        cp.start()
    me = Place()
    z, x, y, c, s = me.z, me.x, me.y, me.c, me.s
    left, right = (jnp.maximum(s - 1, 0), me.b), (jnp.minimum(s + 1, NS - 1), me.b)

    bar = pltpu.get_barrier_semaphore()

    def sig(dev):
        pl.semaphore_signal(bar, inc=1, device_id=dev, device_id_type=MESH)

    sig(me.at(c=1 - c))
    sig(me.at(y=1 - y))
    for i in range(1, NS):
        sig((lax.rem(s + i, NS), me.b))

    def local(src, dst, sem):
        return pltpu.make_async_copy(src, dst, sem)

    def op_load(src, slot):
        return local(src, ob.at[slot], obsem.at[slot])

    def slab_columns(src, j, dst, sem):
        return [local(src.at[:, pl.ds(i * 512 + j * 128, 128)], dst.at[:, pl.ds(i * 128, 128)], sem) for i in range(8)]

    def slab_rows(src, j, dst, sem):
        return [local(src.at[pl.ds(i * 512 + j * 128, 128), :], dst.at[pl.ds(i * 128, 128), :], sem) for i in range(8)]

    weights = [("p", wk_h), ("p", wv_h), ("p", wr_h), ("p", wo_h), ("p", wfr_h)]
    for j in range(4):
        weights += [("c", wfk_h, j), ("r", wfv_h, j)]
    weights += [("p", wfr_h), ("p", wo_h), ("p", wr_h), ("p", wv_h), ("p", wk_h)]

    def w_start(i):
        if i >= len(weights):
            return
        kind, src, *j = weights[i]
        dst, sem = wbuf.at[i % 3], wsem.at[i % 3]
        if kind == "p":
            local(src, dst, sem).start()
        else:
            for cp in (slab_columns if kind == "c" else slab_rows)(src, j[0], dst, sem):
                cp.start()

    def w_wait(i):
        local(wo_h, wbuf.at[i % 3], wsem.at[i % 3]).wait()

    def fs_of(k):
        h = lax.rem(k, 2)
        return jnp.where(h == 0, x, y), jnp.where(h == 0, y, x)

    def partner(h):
        a, b = me.at(x=1 - x), me.at(y=1 - y)
        return (jnp.where(h == 0, a[0], b[0]), jnp.where(h == 0, a[1], b[1]))

    def copy0(k):
        return rcopy(sbuf.at[lax.rem(k, 2)], acc.at[lax.rem(k, WIN)], s0s.at[lax.rem(k, 2)], s0r.at[lax.rem(k, WIN)], me.at(c=1 - c))

    def copyF(k):
        f, _ = fs_of(k)
        return rcopy(acc.at[lax.rem(k, WIN), 1 - f], rF.at[lax.rem(k, WINF)], sFs.at[lax.rem(k, WIN)], sFr.at[lax.rem(k, WINF)], partner(lax.rem(k, 2)))

    def copySA(k):
        f, g = fs_of(k)
        w, v = lax.rem(k, WIN), lax.rem(k, WINZ)
        return rcopy(acc.at[w, f, 1 - g, :, pl.ds(0, RA)], rSA.at[v], sSs.at[v, 0], sSr.at[v, 0], partner(1 - lax.rem(k, 2)))

    def copySE(k):
        f, g = fs_of(k)
        w, v = lax.rem(k, WIN), lax.rem(k, WINZ)
        return rcopy(acc.at[w, f, 1 - g, z, pl.ds(RA, RE)], rSE.at[v], sSs.at[v, 1], sSr.at[v, 1], partner(1 - lax.rem(k, 2)))

    def unit(k, q, late):
        f, g = fs_of(k)
        w = lax.rem(k, WIN)
        return acc.at[w, f, g, q, pl.ds(0, RA)] if late else acc.at[w, f, :, q, pl.ds(RA, RE)]

    def zbuf(k, slot, late):
        return (rZA if late else rZE).at[lax.rem(k, WINZ), slot]

    def copyR(k, q, late):
        i = int(late)
        return rcopy(unit(k, q, late), zbuf(k, q + 1, late), sZs.at[lax.rem(k, WINZ), i], sZr.at[lax.rem(k, WINZ), i, q + 1], me.at(z=z + 1))

    def copyL(k, q, late):
        i = int(late)
        return rcopy(unit(k, q, late), zbuf(k, q, late), sZs.at[lax.rem(k, WINZ), i], sZr.at[lax.rem(k, WINZ), i, q], me.at(z=z - 1))

    def add_into(dst, src):
        dst[...] = dst[...] + src[...]

    def zsub(k, tau, late):
        @pl.when(z <= tau)
        def _():
            q = NZ - 1 - tau + z

            @pl.when(z > 0)
            def _():
                copyR(k, q, late).wait_recv()
                add_into(unit(k, q, late), zbuf(k, q + 1, late))

            copyR(k, q, late).start()

        @pl.when(NZ - 1 - z <= tau)
        def _():
            q = tau - (NZ - 1 - z)

            @pl.when(z < NZ - 1)
            def _():
                copyL(k, q, late).wait_recv()
                add_into(unit(k, q, late), zbuf(k, q, late))

            copyL(k, q, late).start()

    def zfin(k, late):
        @pl.when(z > 0)
        def _():
            copyR(k, z, late).wait_recv()
            add_into(unit(k, z, late), zbuf(k, z + 1, late))

        @pl.when(z < NZ - 1)
        def _():
            copyL(k, z, late).wait_recv()
            add_into(unit(k, z, late), zbuf(k, z, late))

    def gradient(k, core, write):
        h, m = lax.rem(k, 2), k // 2
        ls, rs = pick(m, LEFT), pick(m, RIGHT)
        cols = jnp.concatenate(
            [ob[rs, :, pl.ds(pl.multiple_of((2 * yy + core) * 256 + h * 128, 128), 128)] for yy in range(2)], axis=1)

        def group(g, _):
            res = contract0(ob[ls, :, pl.ds(pl.multiple_of(g * 512, 512), 512)], cols)
            for i in range(4):
                zz, xx = g * 2 + i // 2, i % 2
                for yy in range(2):
                    f = jnp.where(h == 0, xx, yy)
                    g2_ = jnp.where(h == 0, yy, xx)
                    write(f, g2_, zz, res[i * 128:(i + 1) * 128, yy * 128:(yy + 1) * 128])
            return 0

        lax.fori_loop(0, 2, group, 0)

    def taskP(k):
        @pl.when(k >= 2)
        def _():
            copy0(k - 2).wait_send()

        slot = lax.rem(k, 2)

        def write(f, g, zz, v):
            sbuf[slot, f, g, zz] = v

        gradient(k, 1 - c, write)
        copy0(k).start()

    def task1(k):
        copy0(k).wait_recv()
        w = lax.rem(k, WIN)

        def write(f, g, zz, v):
            acc[w, f, g, zz] = acc[w, f, g, zz] + v

        gradient(k, c, write)
        copyF(k).start()

    def task2(k):
        copyF(k).wait_recv()
        f, _ = fs_of(k)
        w = lax.rem(k, WIN)

        def body(i, _):
            add_into(acc.at[w, f, i // NZ, lax.rem(i, NZ)], rF.at[lax.rem(k, WINF), i // NZ, lax.rem(i, NZ)])
            return 0

        lax.fori_loop(0, 2 * NZ, body, 0)
        copySA(k).start()
        zsub(k, 0, False)

    def taskSA(k):
        copySA(k).wait_recv()
        f, g = fs_of(k)
        w = lax.rem(k, WIN)
        add_into(acc.at[w, f, g, :, pl.ds(0, RA)], rSA.at[lax.rem(k, WINZ)])
        zsub(k, 0, True)

    def taskFinE(k):
        zfin(k, False)
        copySE(k).start()

    def taskSE(k):
        copySE(k).wait_recv()
        f, g = fs_of(k)
        w = lax.rem(k, WIN)
        add_into(acc.at[w, f, g, z, pl.ds(RA, RE)], rSE.at[lax.rem(k, WINZ)])
        src = acc.at[w, f, g, z]
        h, m = lax.rem(k, 2), k // 2
        half = pl.ds(pl.multiple_of(h * 128, 128), 128)
        for j in range(4):
            @pl.when(m == 2 * j)
            def _(j=j):
                local(src, outs[5].at[pl.ds(j * 128, 128), half], osem.at[lax.rem(k, WIN)]).start()

            @pl.when(m == 2 * j + 1)
            def _(j=j):
                local(src, outs[4].at[:, pl.ds(pl.multiple_of(h * 512 + j * 128, 128), 128)], osem.at[lax.rem(k, WIN)]).start()
        for mm, i in ((8, 6), (9, 3), (10, 2), (11, 1), (12, 0)):
            @pl.when(m == mm)
            def _(i=i):
                local(src, outs[i].at[:, half], osem.at[lax.rem(k, WIN)]).start()

    def retire(k):
        copyF(k).wait_send()
        copySA(k).wait_send()
        copySE(k).wait_send()
        f, g = fs_of(k)
        w, v = lax.rem(k, WIN), lax.rem(k, WINZ)
        for late in (False, True):
            others = pl.ds(0, NZ - 1)
            sent = acc.at[w, f, g, others, pl.ds(0, RA)] if late else acc.at[w, f, :, others, pl.ds(RA, RE)]
            rcopy(sent, sent, sZs.at[v, int(late)], sZr.at[v, int(late), 0], me.at(c=1 - c)).wait_send()
        local(acc.at[lax.rem(k, WIN), 0, 0, 0], outs[0].at[:, pl.ds(0, 128)], osem.at[lax.rem(k, WIN)]).wait()

    stages = [
        (RETIRE, retire),
        (LAGS[7], lambda k: zfin(k, True), True),
        (LAGS[8], taskSE, True),
        (LAGS[6], lambda k: zsub(k, 2, True), True),
        (LAGS[5], lambda k: zsub(k, 1, True), True),
        (LAGS[4], taskFinE),
        (LAGS[3], lambda k: zsub(k, 2, False)),
        (LAGS[2], lambda k: zsub(k, 1, False)),
        (LAGS[1], taskSA, True),
        (1, task1),
        (LAGS[0], task2),
        (0, taskP),
    ]

    def sm_copy(step):
        if step == 0:
            return rcopy(smb.at[0], smr.at[0], mss.at[0], msr.at[0], me.at(c=1 - c))
        if step == 1:
            return rcopy(smb.at[2], smr.at[1], mss.at[1], msr.at[1], me.at(y=1 - y))
        return rcopy(smb.at[1, 1 - x], smr.at[2, 0], mss.at[2], msr.at[2], me.at(x=1 - x))

    def sm_z(q, to_right):
        if to_right:
            return rcopy(smb.at[1, x, q], smr.at[3, 0, q], mss.at[3 + q], msr.at[3 + q], me.at(z=z + 1))
        return rcopy(smb.at[1, x, q], smr.at[3, 1, q], mss.at[3 + q], msr.at[3 + NZ + q], me.at(z=z - 1))

    vec = lax.broadcasted_iota(jnp.int32, (2, NZ, 16, 128), 2) < 11

    def sm1():
        sm_copy(0).wait_recv()
        smb[2] = smb[0] + jnp.where(vec, smr[0], 0.0)
        sm_copy(1).start()

    def sm2():
        sm_copy(1).wait_recv()
        smb[1] = smb[2] + jnp.where(vec, smr[1], 0.0)
        sm_copy(2).start()

    def sm3():
        sm_copy(2).wait_recv()
        smb[1, x] = smb[1, x] + smr[2, 0]

    def smz(tau):
        @pl.when(z <= tau)
        def _():
            q = NZ - 1 - tau + z

            @pl.when(z > 0)
            def _():
                sm_z(q, True).wait_recv()
                smb[1, x, q] = smb[1, x, q] + smr[3, 0, q]

            sm_z(q, True).start()

        @pl.when(NZ - 1 - z <= tau)
        def _():
            q = tau - (NZ - 1 - z)

            @pl.when(z < NZ - 1)
            def _():
                sm_z(q, False).wait_recv()
                smb[1, x, q] = smb[1, x, q] + smr[3, 1, q]

            sm_z(q, False).start()

    def sm_fin():
        @pl.when(z > 0)
        def _():
            sm_z(z, True).wait_recv()
            smb[1, x, z] = smb[1, x, z] + smr[3, 0, z]

        @pl.when(z < NZ - 1)
        def _():
            sm_z(z, False).wait_recv()
            smb[1, x, z] = smb[1, x, z] + smr[3, 1, z]

        local(smb.at[1, x, z], sm_out, msem).start()

    def tiles(n, rows, body):
        def step(i, _):
            body(i, pl.ds(pl.multiple_of(i * rows, rows), rows))
            return 0

        lax.fori_loop(0, n, step, 0)

    def widen(slot):
        def body(i, rows):
            for g in range(8):
                lanes[g, rows, :] = ob[slot, rows, g * 128:g * 128 + 128].astype(F32)

        tiles(T // 64, 64, body)

    def spread(i, count):
        return jnp.concatenate(
            [jnp.concatenate([lanes[g, pl.ds(i * count + a, 8, stride=SUB), :] for g in range(8)], axis=1) for a in range(count)], axis=0)

    def unspread(i, count, value):
        for a in range(count):
            for g in range(8):
                lanes2[g, pl.ds(i * count + a, 8, stride=SUB), :] = value[a * 8:a * 8 + 8, g * 128:g * 128 + 128]

    def narrow(slot, dst, sem):
        def body(i, rows):
            for g in range(8):
                ob[slot, rows, g * 128:g * 128 + 128] = lanes2[g, rows, :].astype(BF)

        tiles(T // 64, 64, body)
        local(ob.at[slot], dst, sem).start()

    def halves(body):
        tiles(2, 512, body)

    def gate_step():
        w_wait(4)

        G[...] = jnp.dot(ob[10], wbuf[4 % 3], preferred_element_type=F32)
        w_start(7)

        def body(i, rows):
            gate = jax.nn.sigmoid(G[rows, :])
            G[rows, :] = gate
            ob[8, rows, :] = (spread(i, 8) * gate).astype(BF)

        tiles(T // 64, 64, body)

    def hid(j):
        w_wait(5 + 2 * j)
        slot = (5 + 2 * j) % 3

        up = jnp.maximum(jnp.dot(ob[9], wbuf[slot], preferred_element_type=F32), 0.0)
        X[pl.ds(0, T), :] = up
        ob[j] = (up * up).astype(BF)

    def gpre(j):
        w_wait(6 + 2 * j)
        slot = (6 + 2 * j) % 3

        def mm(i, cols):
            back = contract1(ob[8], wbuf[slot, cols, :])
            ob[4 + j, :, cols] = (back * 2.0 * X[pl.ds(0, T), cols]).astype(BF)

        halves(mm)

    def gk_step(j):
        slot = (5 + 2 * j) % 3

        def mm(i, cols):
            part = contract1(ob[4 + j], wbuf[slot, cols, :])
            K[pl.ds(0, T), cols] = part if j == 0 else K[pl.ds(0, T), cols] + part

        halves(mm)
        w_start(5 + 2 * j + 3)

    def ffv(j):
        slot = (6 + 2 * j) % 3

        def mm(i, cols):
            part = jnp.dot(ob[j], wbuf[slot, :, cols], preferred_element_type=F32)
            V[pl.ds(0, T), cols] = part if j == 0 else V[pl.ds(0, T), cols] + part

        halves(mm)
        w_start(6 + 2 * j + 3)

    def big_load(src, dst, i):
        return local(src, dst.at[pl.ds(0, T)], bigsem.at[i])

    def block_step():
        def body(i, rows):
            gate, values = G[rows, :], V[rows, :]
            unspread(i, 4, Y[rows, :] + gate * values)
            ob[0, rows, :] = (spread(i, 4) * values * gate * (1.0 - gate)).astype(BF)

        tiles(T // 32, 32, body)
        narrow(5, o_blk, outsem.at[0])

    row8 = lax.broadcasted_iota(jnp.int32, (8, D), 0)

    def tail(buf):
        buf[T:T + 8, :] = jnp.where(row8 == 7, 0.0, pltpu.roll(buf[0:8, :], 7, 0))

    def edge(src, dst, sem, dev):
        return rcopy(src, dst, sem.at[0], sem.at[1], dev)

    def recept_back():
        w_wait(13)

        def mm(i, cols):
            V[pl.ds(0, T), cols] = contract1(ob[0], wbuf[13 % 3, cols, :])

        halves(mm)
        w_start(16)
        tail(K)
        tail(V)
        es[...] = K[0:8, :] * (1.0 - fmk[...]) + V[0:8, :] * (1.0 - fmr[...])

        @pl.when(s > 0)
        def _():
            edge(es, er, esem, left).start()

    def fold(v):
        return sum(v[i:i + 8] for i in range(8, ROWS, 8)) + v[0:8]

    row_of = lax.broadcasted_iota(jnp.int32, (ROWS, D), 0)

    def centre(v):
        mean = jnp.mean(v, axis=-1, keepdims=True)
        cen = v - mean
        inv = lax.rsqrt(jnp.mean(cen * cen, axis=-1, keepdims=True) + 1e-5)
        return cen * inv, inv

    def ln_back(grad, n, inv, gain):
        h = grad * gain[...]
        return inv * (h - jnp.mean(h, axis=-1, keepdims=True) - n * jnp.mean(h * n, axis=-1, keepdims=True))

    def ln_tile(i, rows, n, gain, bias, parts, arrived, sum_rows, ln_sums):
        later = pl.ds(pl.multiple_of(i * ROWS + 8, 8), ROWS)
        normed = n * gain[...] + bias[...]
        grad = 0.0
        if arrived is not None:
            grad = jnp.where(jnp.logical_and(row_of == ROWS - 1, i == T // ROWS - 1), arrived, 0.0)
        for (buf, w), r in zip(parts, sum_rows):
            now, nxt = buf[rows, :], buf[later, :]
            grad = grad + now * w[...] + nxt * (1.0 - w[...])
            sums[r] = sums[r] + fold(normed * (now - nxt))
        sums[ln_sums[0]] = sums[ln_sums[0]] + fold(grad * n)
        sums[ln_sums[1]] = sums[ln_sums[1]] + fold(grad)
        return grad

    def wait_from_right(cp):
        @pl.when(s < NS - 1)
        def _():
            cp.wait_recv()

    def middle_back(lo, hi):
        arrived = jnp.where(s == NS - 1, 0.0, er[0:1, :]) if hi == T // ROWS else None

        def body(i, _):
            rows = pl.ds(pl.multiple_of(i * ROWS, ROWS), ROWS)
            n, inv = centre(Y[rows, :])
            grad = ln_tile(i, rows, n, g2, b2, ((K, fmk), (V, fmr)), arrived, (9, 10), (7, 8))
            gm = spread(i, ROWS // 8) + ln_back(grad, n, inv, g2)
            G[rows, :] = gm
            ob[1, rows, :] = gm.astype(BF)
            return 0

        lax.fori_loop(lo, hi, body, 0)

    def middle_end():
        for r, buf in ((9, K), (10, V)):
            sums[r, 0:1, :] = sums[r, 0:1, :] - buf[0:1, :] * edges[8:9, :]
        sums[15, 0:1, :] = es[0:1, :]

    def gated_back():
        w_wait(14)

        def mm(i, cols):
            V[pl.ds(0, T), cols] = contract1(ob[1], wbuf[14 % 3, cols, :])

        halves(mm)
        w_start(17)
        big_load(r_h, X, 0).wait()
        big_load(mix_h, K, 1).wait()

        def body(i, rows):
            sg = jax.nn.sigmoid(X[rows, :])
            gg = V[rows, :]
            ob[2, rows, :] = (gg * K[rows, :] * sg * (1.0 - sg)).astype(BF)
            V[rows, :] = gg * sg

        tiles(T // 32, 32, body)

    streams = (k_h, m_h, d_h, n_h, v_h)

    def st_copies(blk, slot, count):
        rows = pl.ds(pl.multiple_of(blk * 64, 64), 64)
        return [local(src.at[rows, :], st.at[slot, i], stsem.at[slot, i]) for i, src in enumerate(streams[:count])]

    def st_start(blk, count):
        for cp in st_copies(blk, lax.rem(blk, 2), count):
            cp.start()

    def st_next(blk, count):
        for cp in st_copies(blk, lax.rem(blk, 2), count):
            cp.wait()

        @pl.when(blk > 0)
        def _():
            st_start(blk - 1, count)


    def wide(v, cols):
        return jnp.broadcast_to(v[:, cols], (8, 512))

    def first_pass(lo):
        def block(i, _):
            blk = 7 - lo - i
            slot = lax.rem(blk, 2)
            st_next(blk, 3)
            for h in range(2):
                cols = slice(h * 512, h * 512 + 512)
                w, bonus = wide(decay, cols), wide(tf[...], cols)

                def step(jj, carry):
                    R, S = carry
                    j = 7 - jj
                    at = pl.ds(pl.multiple_of(j * 8, 8), 8)
                    rows = pl.ds(pl.multiple_of(blk * 64 + j * 8, 8), 8)
                    k, m, d = st[slot, 0, at, cols], st[slot, 1, at, cols], st[slot, 2, at, cols]
                    p, u = step_weights(m - (bonus + k))
                    q = V[rows, cols] / (p * d + u)
                    qp = p * q
                    V[rows, cols] = qp
                    X[rows, cols] = u * q
                    a, _ = step_weights(m + w - k)
                    return qp + a * R, qp * K[rows, cols] + a * S

                R, S = lax.fori_loop(0, 8, step, (RS[0, :, cols], RS[1, :, cols]), unroll=2)
                RS[0, :, cols] = R
                RS[1, :, cols] = S

                @pl.when(blk == 7)
                def _():
                    RS[2, :, cols] = jnp.maximum(st[slot, 1, 56:64, cols] + w, st[slot, 0, 56:64, cols])

                @pl.when(blk == 0)
                def _():
                    RS[3, :, cols] = st[slot, 1, 0:8, cols]
            return 0

        lax.fori_loop(0, 4, block, 0)

    def suffix(value, dist, fill):
        return jnp.where(row8 >= 8 - dist, fill, pltpu.roll(value, 8 - dist, 0))


    def state_copy(src, dst):
        return rcopy(ws, wr.at[src], wssem.at[dst], wrsem.at[src], (dst, me.b))

    def first_end():
        A = jnp.exp(jnp.minimum(RS[3] + span - RS[2], 0.0))
        R, S = RS[0], RS[1]
        for dist in (1, 2, 4):
            R = R + A * suffix(R, dist, 0.0)
            S = S + A * suffix(S, dist, 0.0)
            A = A * suffix(A, dist, 1.0)
        RS[0], RS[1], RS[4] = R, S, A
        ws[...] = jnp.where(row8 == 0, R[0:1], jnp.where(row8 == 1, S[0:1], RS[3, 0:1, :]))
        for i in range(NS - 1):
            @pl.when(i < s)
            def _(i=i):
                state_copy(s, i).start()

    def second_start():
        RS[5] = jnp.zeros((8, D), F32)
        RS[6] = jnp.zeros((8, D), F32)
        for i in range(1, NS):
            @pl.when(i > s)
            def _(i=i):
                state_copy(i, 0).wait_recv()
                far = jnp.exp(jnp.minimum(RS[2, 7:8, :] + (i - s - 1).astype(F32) * (8.0 * span) - wr[i, 2:3, :], 0.0))
                RS[5, 0:1, :] = RS[5, 0:1, :] + far * wr[i, 0:1, :]
                RS[6, 0:1, :] = RS[6, 0:1, :] + far * wr[i, 1:2, :]
        Rin, Sin = RS[5, 0:1, :], RS[6, 0:1, :]
        A = RS[4]
        R = RS[0] + A * Rin
        S = RS[1] + A * Sin
        RS[0] = jnp.where(row8 == 7, Rin, pltpu.roll(R, 7, 0))
        RS[1] = jnp.where(row8 == 7, Sin, pltpu.roll(S, 7, 0))

    def second_pass(lo, n):
        def block(i, _):
            blk = 7 - lo - i
            slot = lax.rem(blk, 2)
            st_next(blk, 5)
            for h in range(2):
                cols = slice(h * 512, h * 512 + 512)
                w = wide(decay, cols)

                def one(j, carry):
                    R, S, first, slow = carry
                    at = pl.ds(pl.multiple_of(j * 8, 8), 8)
                    rows = pl.ds(pl.multiple_of(blk * 64 + j * 8, 8), 8)
                    k, m, d, n_, v = (st[slot, q, at, cols] for q in range(5))
                    mixed, qp, uq = K[rows, cols], V[rows, cols], X[rows, cols]
                    a, b = step_weights(m + w - k)
                    own = uq * (v - mixed)
                    gv = uq + b * R
                    gk = own + b * (v * R - S)
                    first = first + own
                    slow = slow + a * (n_ * R - d * S)
                    return (qp + a * R, qp * mixed + a * S, first, slow), gk, gv

                def step(jj, carry):
                    j = 3 - jj
                    carry, gk1, gv1 = one(2 * j + 1, carry)
                    carry, gk0, gv0 = one(2 * j, carry)
                    pair = pl.ds(pl.multiple_of(blk * 64 + j * 16, 16), 16)
                    ob[6, pair, cols] = jnp.concatenate([gk0, gk1], axis=0).astype(BF)
                    ob[3, pair, cols] = jnp.concatenate([gv0, gv1], axis=0).astype(BF)
                    return carry

                R, S, first, slow = lax.fori_loop(0, 4, step, (RS[0, :, cols], RS[1, :, cols], sums[6, :, cols], sums[5, :, cols]))
                RS[0, :, cols] = R
                RS[1, :, cols] = S
                sums[6, :, cols] = first
                sums[5, :, cols] = slow
            return 0

        lax.fori_loop(0, n, block, 0)

    def second_end():
        gn, gd = RS[0, 0:1, :], -RS[1, 0:1, :]
        sums[11, 0:1, :] = gn
        sums[12, 0:1, :] = gd
        sums[13, 0:1, :] = sn[...] * gn + sd[...] * gd
        sums[5] = sums[5] * decay

    def input_mm(i, slot, buf):
        w_wait(i)

        def mm(_, cols):
            buf[pl.ds(0, T), cols] = contract1(ob[slot], wbuf[i % 3, cols, :])

        halves(mm)
        tail(buf)

    def input_edge():
        fs[...] = K[0:8, :] * (1.0 - mk[...]) + V[0:8, :] * (1.0 - mv[...]) + X[0:8, :] * (1.0 - mr[...])

        @pl.when(s > 0)
        def _():
            edge(fs, fr, fsem, left).start()

    def input_back(lo, hi):
        arrived = jnp.where(s == NS - 1, 0.0, fr[0:1, :]) if hi == T // ROWS else None

        def body(i, _):
            rows = pl.ds(pl.multiple_of(i * ROWS, ROWS), ROWS)
            n, inv = centre(spread(i, ROWS // 8))
            grad = ln_tile(i, rows, n, g1, b1, ((K, mk), (V, mv), (X, mr)), arrived, (2, 3, 4), (0, 1))
            unspread(i, ROWS // 8, G[rows, :] + ln_back(grad, n, inv, g1))
            return 0

        lax.fori_loop(lo, hi, body, 0)

    def input_end():
        for r, buf in ((2, K), (3, V), (4, X)):
            sums[r, 0:1, :] = sums[r, 0:1, :] - buf[0:1, :] * edges[0:1, :]
        sums[14, 0:1, :] = fs[0:1, :]
        narrow(0, o_inp, outsem.at[1])
        alone = jnp.where(s == 0, 1.0, 0.0)
        rows = [jnp.sum(sums[r], axis=0, keepdims=True) for r in range(11)] + [jnp.where(s == 0, sums[r, 0:1, :], 0.0) for r in range(11, 16)]
        table = jnp.concatenate(rows, axis=0)
        for g in range(8):
            smb[0, g % 2, g // 2] = table[:, g * 128:g * 128 + 128]
        sm_copy(0).start()

    def start_all(*copies):
        for cp in copies:
            cp.start()

    compute = {
        1: [lambda: gpre(0), lambda: gk_step(0), lambda: hid(1)],
        2: [lambda: ffv(0), lambda: gpre(1)],
        3: [lambda: gk_step(1), lambda: hid(2)],
        4: [lambda: ffv(1), lambda: gpre(2)],
        5: [lambda: gk_step(2), lambda: hid(3), lambda: start_all(op_load(gat_h, 4))],
        6: [lambda: ffv(2), lambda: gpre(3)],
        7: [lambda: gk_step(3), lambda: ffv(3)],
        8: [block_step],
        9: [recept_back],
        10: [lambda: middle_back(0, 4)],
        11: [lambda: start_all(big_load(r_h, X, 0)), lambda: wait_from_right(edge(es, er, esem, left)), lambda: middle_back(4, 8), middle_end,
             lambda: start_all(big_load(mix_h, K, 1)), lambda: st_start(7, 3),
             lambda: local(ob.at[5], o_blk, outsem.at[0]).wait(), lambda: start_all(op_load(rin_h, 5))],
        12: [gated_back],
        13: [lambda: first_pass(0)],
        14: [lambda: first_pass(4), first_end, lambda: st_start(7, 5)],
        15: [second_start, lambda: second_pass(0, 2), lambda: start_all(op_load(vin_h, 8))],
        16: [lambda: second_pass(2, 3)],
        17: [lambda: second_pass(5, 3), second_end, lambda: start_all(op_load(kin_h, 7), op_load(x_h, 9))],
        18: [lambda: input_mm(15, 2, X), lambda: input_mm(16, 3, V)],
        19: [lambda: input_mm(17, 6, K), input_edge, lambda: op_load(x_h, 9).wait(), lambda: widen(9)],
        20: [lambda: input_back(0, 4)],
        21: [lambda: wait_from_right(edge(fs, fr, fsem, left)), lambda: input_back(4, 8), input_end],
        23: [sm1],
        24: [sm2],
        25: [sm3, lambda: smz(0)],
        26: [lambda: smz(1)],
        27: [lambda: smz(2)],
        28: [sm_fin],
    }
    landed = {18: (gat_h, 4), 20: (rin_h, 5), 22: (vin_h, 8), 24: (kin_h, 7)}

    def spill(src, dst, i):
        return local(src, dst, spsem.at[i])

    kb, vb, rb, nb = G, V, X, K
    to_next = rcopy(as_, ar, asem.at[0], asem.at[1], right)
    to_next2 = rcopy(bs_, br_, bsem.at[0], bsem.at[1], right)

    def wait_from_left(cp):
        @pl.when(s > 0)
        def _():
            cp.wait_recv()

    def send_right(cp):
        @pl.when(s < NS - 1)
        def _():
            cp.start()

    def norm1(i, rows):
        v = spread(i, 8)
        Y[rows, :] = v
        nb[pl.ds(pl.multiple_of(i * 64 + 8, 8), 64), :] = normalize(v, g1[...], b1[...])

    def header(start_row):
        nb[0:8, :] = jnp.where(row8 == 0, start_row, pltpu.roll(nb[T:T + 8, :], 1, 0))

    def mix(pairs, i):
        rows = pl.ds(pl.multiple_of(i * 64, 64), 64)
        before = nb[rows, :]
        now = nb[pl.ds(pl.multiple_of(i * 64 + 8, 8), 64), :]
        for slot, w in pairs:
            ob[slot, rows, :] = (now * w[...] + before * (1.0 - w[...])).astype(BF)

    def project(i, slot, dst):
        w_wait(i)
        dst[pl.ds(0, T), :] = jnp.dot(ob[slot], wbuf[i % 3], preferred_element_type=F32)
        w_start(i + 3)

    start_all(op_load(x_h, 4), op_load(cot_h, 5))
    for i in range(3):
        w_start(i)
    local(K.at[pl.ds(0, 16)], V.at[pl.ds(0, 16)], vsem).wait()
    decay = -jnp.exp(td[...])
    span = SUB * decay
    op_load(x_h, 4).wait()
    as_[...] = normalize(ob[4, T - 16:T, :].astype(F32), g1[...], b1[...])[8:16, :]
    pl.semaphore_wait(bar, NS + 1)
    send_right(to_next)
    widen(4)
    tiles(T // 64, 64, norm1)
    wait_from_left(to_next)
    header(jnp.where(s == 0, pa[...], ar[7:8, :]))
    edges[0:8, :] = nb[0:8, :]
    tiles(T // 64, 64, lambda i, rows: mix(((0, mk), (1, mv), (2, mr)), i))
    start_all(spill(ob.at[0], kin_h, 0), spill(ob.at[1], vin_h, 1), spill(ob.at[2], rin_h, 2))
    project(0, 0, kb)
    project(1, 1, vb)
    start_all(spill(kb, k_h, 3), spill(vb.at[pl.ds(0, T)], v_h, 4))

    wide_decay = jnp.broadcast_to(decay, (8, D))

    def own_step(j, state):
        rows = pl.ds(pl.multiple_of(j * 8, 8), 8)
        m, n, d = state
        k, v = kb[rows, :], vb[rows, :]
        low = m + wide_decay
        a, b = step_weights(low - k)
        return jnp.maximum(low, k), a * n + b * v, a * d + b

    total = lax.fori_loop(1, SUB, own_step, (kb[0:8, :], vb[0:8, :], jnp.ones((8, D), F32)), unroll=7)

    def earlier(state, dist):
        m, n, d = (pltpu.roll(p, dist, 0) for p in state)
        out = row8 < dist
        return jnp.where(out, -1e30, m), jnp.where(out, 0.0, n), jnp.where(out, 0.0, d)

    for dist in (1, 2, 4):
        total = join(earlier(total, dist), total, dist * span)
    before_own = earlier(total, 1)
    us[...] = jnp.where(row8 == 0, total[0][7:8], jnp.where(row8 == 1, total[1][7:8], total[2][7:8]))

    def reach_copy(src, dst):
        return rcopy(us, ur.at[src], wssem.at[dst], wrsem.at[src], (dst, me.b))

    for i in range(1, NS):
        @pl.when(s < i)
        def _(i=i):
            reach_copy(s, i).start()

    project(2, 2, rb)
    start_all(spill(rb.at[pl.ds(0, T)], r_h, 5))
    op_load(cot_h, 5).wait()
    widen(5)
    RS[0, 0:1, :] = sm[...]
    RS[1, 0:1, :] = sn[...]
    RS[2, 0:1, :] = sd[...]
    for i in range(NS - 1):
        @pl.when(i < s)
        def _(i=i):
            reach_copy(i, NS - 1).wait_recv()
            now = join(tuple(RS[r, 0:1, :] for r in range(3)), tuple(ur[i, r:r + 1, :] for r in range(3)), 8.0 * span)
            for r in range(3):
                RS[r, 0:1, :] = now[r]

    base = tuple(RS[r, 0:1, :] for r in range(3))
    lifted = (base[0] + row8.astype(F32) * span, jnp.broadcast_to(base[1], (8, D)), jnp.broadcast_to(base[2], (8, D)))
    for r, v in enumerate(join(lifted, before_own, 0.0)):
        RS[r] = v

    def state_spills(blk, slot):
        rows = pl.ds(pl.multiple_of(blk * 64, 64), 64)
        return [local(st.at[slot, q], dst.at[rows, :], stsem.at[slot, q]) for q, dst in enumerate((mix_h, m_h, n_h, d_h))]

    def outputs(blk, _):
        slot = lax.rem(blk, 2)

        @pl.when(blk >= 2)
        def _():
            for cp in state_spills(blk - 2, slot):
                cp.wait()

        for h in range(2):
            cols = slice(h * 512, h * 512 + 512)
            w, bonus = wide(decay, cols), wide(tf[...], cols)

            def one(j, state):
                at = pl.ds(pl.multiple_of(j * 8, 8), 8)
                rows = pl.ds(pl.multiple_of(blk * 64 + j * 8, 8), 8)
                m, n, d = state
                k, v = kb[rows, cols], vb[rows, cols]
                p, u = step_weights(m - (bonus + k))
                mixed = (p * n + u * v) / (p * d + u)
                for q, val in enumerate((mixed, m, n, d)):
                    st[slot, q, at, cols] = val
                low = m + w
                a, b = step_weights(low - k)
                return (jnp.maximum(low, k), a * n + b * v, a * d + b), jax.nn.sigmoid(rb[rows, cols]) * mixed

            def two(i, state):
                state, ga = one(2 * i, state)
                state, gb = one(2 * i + 1, state)
                ob[3, pl.ds(pl.multiple_of(blk * 64 + i * 16, 16), 16), cols] = jnp.concatenate([ga, gb], axis=0).astype(BF)
                return state

            for r, v in enumerate(lax.fori_loop(0, 4, two, tuple(RS[r, :, cols] for r in range(3)), unroll=4)):
                RS[r, :, cols] = v
        start_all(*state_spills(blk, slot))
        return 0

    lax.fori_loop(0, 8, outputs, 0)
    start_all(spill(ob.at[3], gat_h, 6))
    spill(kb, k_h, 3).wait()
    project(3, 3, G)

    def norm2(i, rows):
        v = Y[rows, :] + G[rows, :]
        Y[rows, :] = v
        nb[pl.ds(pl.multiple_of(i * 64 + 8, 8), 64), :] = normalize(v, g2[...], b2[...])

    norm2(T // 64 - 1, pl.ds(T - 64, 64))
    bs_[...] = nb[T:T + 8, :]
    send_right(to_next2)
    tiles(T // 64 - 1, 64, norm2)

    def mix2(i, _):
        mix(((9, fmk), (10, fmr)), i)
        return 0

    lax.fori_loop(1, T // 64, mix2, 0)
    wait_from_left(to_next2)
    header(jnp.where(s == 0, pf[...], br_[7:8, :]))
    edges[8:16, :] = nb[0:8, :]
    mix2(0, 0)

    sums[...] = jnp.zeros_like(sums)
    gate_step()
    spill(ob.at[0], kin_h, 0).wait()
    spill(rb.at[pl.ds(0, T)], r_h, 5).wait()
    hid(0)
    RS[...] = jnp.zeros_like(RS)
    for i, (src, dst) in enumerate(((ob.at[1], vin_h), (ob.at[2], rin_h))):
        spill(src, dst, 1 + i).wait()
    spill(vb.at[pl.ds(0, T)], v_h, 4).wait()
    spill(ob.at[3], gat_h, 6).wait()
    for blk in (6, 7):
        for cp in state_spills(blk, blk % 2):
            cp.wait()

    def tick(t, _):
        for at, (src, slot) in landed.items():
            @pl.when(t == at)
            def _(src=src, slot=slot):
                op_load(src, slot).wait()

        for lag, task, *early in stages:
            k = t - lag

            if early:
                def later(k, _, task=task):
                    task(k)
                    return 0

                hurry = jnp.where(k >= NK - 3, 1, 0), jnp.where(k > NK - 3, 1, 0)
                lax.fori_loop(jnp.clip(k + hurry[1], 0, NK), jnp.clip(k + 1 + hurry[0], 0, NK), later, 0)
                continue

            @pl.when(jnp.logical_and(k >= (2 if lag < 2 else 0), k < NK))
            def _(k=k, task=task):
                task(k)

        for at, steps in compute.items():
            @pl.when(t == at)
            def _(steps=steps):
                for step in steps:
                    step()
        return 0

    for k in range(2):
        taskP(jnp.int32(k))
    for k in range(2):
        task1(jnp.int32(k))
    lax.fori_loop(1, NK + RETIRE, tick, 0)

    copy0(NK - 2).wait_send()
    copy0(NK - 1).wait_send()
    for i in range(3):
        sm_copy(i).wait_send()
    for q in range(NZ):
        @pl.when(q != z)
        def _(q=q):
            sm_z(q, True).wait_send()

    @pl.when(s > 0)
    def _():
        edge(es, er, esem, left).wait_send()
        edge(fs, fr, fsem, left).wait_send()

    @pl.when(s < NS - 1)
    def _():
        to_next.wait_send()
        to_next2.wait_send()

    for i in range(NS):
        @pl.when(i < s)
        def _(i=i):
            state_copy(s, i).wait_send()

        @pl.when(i > s)
        def _(i=i):
            reach_copy(s, i).wait_send()
    local(smb.at[1, x, z], sm_out, msem).wait()
    local(ob.at[0], o_inp, outsem.at[1]).wait()


def block_call(x, cot, mats, vectors, states):
    anyspec = pl.BlockSpec(memory_space=pl.ANY)
    S = jax.ShapeDtypeStruct
    sem = pltpu.SemaphoreType.DMA
    M = pltpu.VMEM
    row = M((8, D), F32)
    return pl.pallas_call(
        block_kernel,
        out_shape=[S((T, D), BF)] * 2 + [S((128, 256), F32)] * 4 + [S((128, 1024), F32), S((512, 256), F32), S((128, 256), F32), S((16, 128), F32)]
        + [S((T, D), BF)] * 4 + [S((T, D), F32)] * 7,
        in_specs=[anyspec] * 25,
        out_specs=[anyspec] * 21,
        scratch_shapes=[
            M((11, T, D), BF), M((3, D, D), BF), M((T, D), F32), M((T, D), F32), M((T + 8, D), F32), M((T + 8, D), F32), M((T + 8, D), F32),
            M((8, T, 128), F32), M((8, T, 128), F32), M((2, 5, 64, D), F32), M((16, 8, D), F32), M((7, 8, D), F32),
            row, row, row, row, row, M((NS, 8, D), F32), M((16, D), F32), row, row, row, row, row, M((NS, 8, D), F32),
            M((WIN, 2, 2, NZ, 128, 128), F32), M((2, 2, 2, NZ, 128, 128), F32), M((WINF, 2, NZ, 128, 128), F32),
            M((WINZ, NZ, RA, 128), F32), M((WINZ, RE, 128), F32), M((WINZ, NZ + 1, RA, 128), F32), M((WINZ, NZ + 1, 2, RE, 128), F32),
            M((3, 2, NZ, 16, 128), F32), M((4, 2, NZ, 16, 128), F32),
            sem((11,)), sem((3,)), sem((2, 5)), sem((2,)), sem((2,)), sem((7,)), sem((2,)), sem((2,)), sem((2,)), sem((2,)), sem((NS,)), sem((NS,)),
            sem((2,)), sem((WIN,)), sem((WIN,)), sem((WINF,)), sem((WINZ, 2)), sem((WINZ, 2)),
            sem((WINZ, 2)), sem((WINZ, 2, NZ + 1)), sem((WIN,)), sem, sem((3 + NZ,)), sem((3 + 2 * NZ,)), sem,
        ] + [M((1, D), F32)] * 16,
        compiler_params=pltpu.CompilerParams(collective_id=0, has_side_effects=True, vmem_limit_bytes=67043328),
        name="block",
    )(x, cot, *mats, *vectors, *states)[:10]

def finish_kernel(*refs):
    ins, outs, (scratch, sems) = refs[:10], refs[10:35], (refs[35:-2], refs[-2:])
    into, out = sems
    loads = [pltpu.make_async_copy(src, buf, into.at[i]) for i, (src, buf) in enumerate(zip(ins, scratch))]
    for cp in loads:
        cp.start()
    stores = []
    for i in range(10):
        loads[i].wait()
        if i < 9:
            stores.append(pltpu.make_async_copy(scratch[i], outs[i], out.at[i]))
            stores[-1].start()
        else:
            for r in range(16):
                stores.append(pltpu.make_async_copy(scratch[i].at[pl.ds(r, 1)], outs[9 + r], out.at[9 + r]))
                stores[-1].start()
    for cp in stores:
        cp.wait()


def finish_call(parts):
    anyspec = pl.BlockSpec(memory_space=pl.ANY)
    return pl.pallas_call(
        finish_kernel,
        out_shape=[jax.ShapeDtypeStruct(p.shape, p.dtype) for p in parts[:9]] + [jax.ShapeDtypeStruct((1, 128), F32)] * 16,
        in_specs=[anyspec] * 10,
        out_specs=[anyspec] * 25,
        scratch_shapes=[pltpu.VMEM(p.shape, p.dtype) for p in parts] + [pltpu.SemaphoreType.DMA((10,)), pltpu.SemaphoreType.DMA((25,))],
        name="finish",
    )(*parts)


def fits(mesh):
    return (mesh.shape["seq"], mesh.shape["batch"]) == (2 * NZ, 4)


def local(
    inputs,
    w_key,
    w_value,
    w_recept,
    w_output,
    w_ffn_key,
    w_ffn_value,
    w_ffn_recept,
    ln1_gain,
    ln1_bias,
    mix_key,
    mix_value,
    mix_recept,
    time_decay,
    time_first,
    ln2_gain,
    ln2_bias,
    ffn_mix_key,
    ffn_mix_recept,
    state_num,
    state_den,
    state_max,
    prev_att,
    prev_ffn,
    cotangent,
):
    rows = inputs.reshape(T, D)
    vectors = [
        v.reshape(1, D)
        for v in (
            ln1_gain,
            ln1_bias,
            mix_key,
            mix_value,
            mix_recept,
            time_decay,
            time_first,
            ln2_gain,
            ln2_bias,
            ffn_mix_key,
            ffn_mix_recept,
        )
    ]
    states = [v.reshape(1, D) for v in (state_num, state_den, state_max, prev_att, prev_ffn)]
    parts = block_call(
        rows,
        cotangent.reshape(T, D),
        [w_key, w_value, w_recept, w_output, w_ffn_key, w_ffn_value, w_ffn_recept],
        vectors,
        states,
    )
    block_out, input_grad, *rest = finish_call(parts)
    return (
        block_out.reshape(inputs.shape),
        input_grad.reshape(inputs.shape),
        *rest[:7],
        *[v.reshape(128) for v in rest[7:18]],
        *[v.reshape(128, 1) for v in rest[18:]],
    )


BLOCK = 64


far_below = -1e30


def from_behind(block, axis, distance):
    devices = range(lax.axis_size(axis))
    route = [(i - distance, i) for i in devices if i - distance in devices]
    return lax.ppermute(block, axis, route)


def prefix(value, axis, join, neutral, backward):
    count, mine = (lax.axis_size(axis), lax.axis_index(axis))
    pieces = jax.tree.map(lambda part: lax.all_gather(part, axis), value)
    if backward:
        pieces = jax.tree.map(lambda part: part[::-1], pieces)
        mine = count - 1 - mine
    total = jax.tree.map(
        lambda part, zero: jnp.full_like(part, 0) + jnp.asarray(zero, part.dtype), value, neutral
    )

    def turn(position, total):
        longer = join(total, jax.tree.map(lambda part: part[position], pieces))
        return jax.tree.map(lambda new, old: jnp.where(position < mine, new, old), longer, total)

    return lax.fori_loop(0, count - 1, turn, total)


def layer_norm(values, ln_gain, ln_bias):
    centred = values - jnp.mean(values, axis=-1, keepdims=True)
    spread = jnp.mean(centred * centred, axis=-1, keepdims=True)
    return centred * lax.rsqrt(spread + 1e-05) * ln_gain + ln_bias


def matmul(operand, matrix):
    return lax.dot_general(
        operand, matrix, (((operand.ndim - 1,), (0,)), ((), ())), preferred_element_type=jnp.float32
    )


def matmul_back(gradient, matrix):
    return lax.dot_general(
        gradient,
        matrix,
        (((gradient.ndim - 1,), (1,)), ((), ())),
        preferred_element_type=jnp.float32,
    )


def outer_sum(operand, gradient):
    flat_operand = operand.reshape(-1, operand.shape[-1])
    flat_gradient = gradient.reshape(-1, gradient.shape[-1])
    return lax.dot_general(
        flat_operand, flat_gradient, (((0,), (0,)), ((), ())), preferred_element_type=jnp.float32
    )


def token_mix(normed, edge_row, mix_vectors):
    earlier = jnp.concatenate([edge_row[:, None, :], normed[:, :-1, :]], axis=1)
    return tuple((normed * member + earlier * (1.0 - member) for member in mix_vectors))


def gate_rows(recept_rows, mixed_rows):
    return jax.nn.sigmoid(recept_rows) * mixed_rows


def wkv_block(decay_rate, time_first, state_in, inputs_now):
    numerator, denominator, running_max = state_in
    key_rows, value_rows = inputs_now
    length = key_rows.shape[1]
    places = jnp.arange(length, dtype=jnp.float32)[None, :, None]
    own_terms = time_first + key_rows
    anchor = jnp.maximum(
        jnp.maximum(running_max, jnp.max(key_rows, axis=1)), jnp.max(own_terms, axis=1)
    )
    scaled = jnp.exp(key_rows - anchor[:, None, :] - (places + 1.0) * decay_rate)
    running_num = jnp.cumsum(scaled * value_rows, axis=1)
    running_den = jnp.cumsum(scaled, axis=1)
    past_num = jnp.concatenate([jnp.zeros_like(running_num[:, :1]), running_num[:, :-1]], axis=1)
    past_den = jnp.concatenate([jnp.zeros_like(running_den[:, :1]), running_den[:, :-1]], axis=1)
    fading = jnp.exp(places * decay_rate)
    carried = jnp.exp(running_max[:, None, :] + places * decay_rate - anchor[:, None, :])
    own_weight = jnp.exp(own_terms - anchor[:, None, :])
    top_num = past_num * fading + own_weight * value_rows + carried * numerator[:, None, :]
    top_den = past_den * fading + own_weight + carried * denominator[:, None, :]
    outputs = top_num / top_den
    final_terms = key_rows + (length - 1.0 - places) * decay_rate
    kept_max = running_max + length * decay_rate
    new_max = jnp.maximum(kept_max, jnp.max(final_terms, axis=1))
    final_weights = jnp.exp(final_terms - new_max[:, None, :])
    kept_weight = jnp.exp(kept_max - new_max)
    new_num = jnp.sum(final_weights * value_rows, axis=1) + kept_weight * numerator
    new_den = jnp.sum(final_weights, axis=1) + kept_weight * denominator
    return ((new_num, new_den, new_max), outputs)


def wkv_local(key_rows, value_rows, time_decay, time_first, in_num, in_den, in_max):
    decay_rate = -jnp.exp(time_decay)
    block_count = key_rows.shape[1] // BLOCK

    def arrange(values):
        return jnp.moveaxis(
            values.reshape(values.shape[0], block_count, BLOCK, values.shape[2]), 1, 0
        )

    block_step = jax.checkpoint(partial(wkv_block, decay_rate, time_first))
    state_out, outputs = lax.scan(
        block_step, (in_num, in_den, in_max), (arrange(key_rows), arrange(value_rows))
    )
    outputs = jnp.moveaxis(outputs, 0, 1).reshape(key_rows.shape)
    return (outputs, state_out)


def local_summary(key_rows, value_rows, decay_rate):
    length = key_rows.shape[1]
    places = jnp.arange(length, dtype=jnp.float32)[None, :, None]
    terms = key_rows + (length - 1.0 - places) * decay_rate
    top_term = jnp.max(terms, axis=1)
    weights_now = jnp.exp(terms - top_term[:, None, :])
    return (jnp.sum(weights_now * value_rows, axis=1), jnp.sum(weights_now, axis=1), top_term)


def combine_states(earlier_one, later_one):
    earlier_num, earlier_den, earlier_max, earlier_span = earlier_one
    later_num, later_den, later_max, later_span = later_one
    shifted_max = earlier_max + later_span
    top_both = jnp.maximum(shifted_max, later_max)
    weight_early = jnp.exp(shifted_max - top_both)
    weight_late = jnp.exp(later_max - top_both)
    return (
        earlier_num * weight_early + later_num * weight_late,
        earlier_den * weight_early + later_den * weight_late,
        top_both,
        earlier_span + later_span,
    )


def combine_grads(earlier_one, later_one):
    earlier_num, earlier_den, earlier_span = earlier_one
    later_num, later_den, later_span = later_one
    factor = jnp.exp(later_span)
    return (
        later_num + factor * earlier_num,
        later_den + factor * earlier_den,
        earlier_span + later_span,
    )


def local_plain(
    inputs,
    w_key,
    w_value,
    w_recept,
    w_output,
    w_ffn_key,
    w_ffn_value,
    w_ffn_recept,
    ln1_gain,
    ln1_bias,
    mix_key,
    mix_value,
    mix_recept,
    time_decay,
    time_first,
    ln2_gain,
    ln2_bias,
    ffn_mix_key,
    ffn_mix_recept,
    state_num,
    state_den,
    state_max,
    prev_att,
    prev_ffn,
    cotangent,
):
    position = lax.axis_index("seq")
    is_first = position == 0
    start_num = state_num.T
    start_den = state_den.T
    start_max = state_max.T
    before_att = prev_att.T
    before_ffn = prev_ffn.T
    input_rows = inputs.astype(jnp.float32)
    normed, norm_pull = jax.vjp(layer_norm, input_rows, ln1_gain, ln1_bias)
    from_left = from_behind(normed[:, -1, :], "seq", 1)
    edge_att = jnp.where(is_first, before_att, from_left)
    mixed_inputs, mix_pull = jax.vjp(token_mix, normed, edge_att, (mix_key, mix_value, mix_recept))
    key_in = mixed_inputs[0].astype(jnp.bfloat16)
    value_in = mixed_inputs[1].astype(jnp.bfloat16)
    recept_in = mixed_inputs[2].astype(jnp.bfloat16)
    key_rows = matmul(key_in, w_key)
    value_rows = matmul(value_in, w_value)
    recept_rows = matmul(recept_in, w_recept)
    decay_rate = -jnp.exp(time_decay)
    local_len = key_rows.shape[1]
    device_span = jnp.broadcast_to(local_len * decay_rate, start_num.shape)
    own_num, own_den, own_max = local_summary(key_rows, value_rows, decay_rate)
    first_element = combine_states(
        (start_num, start_den, start_max, jnp.zeros_like(device_span)),
        (own_num, own_den, own_max, device_span),
    )
    element_num = jnp.where(is_first, first_element[0], own_num)
    element_den = jnp.where(is_first, first_element[1], own_den)
    element_max = jnp.where(is_first, first_element[2], own_max)
    zero_rows = jnp.zeros_like(start_num)
    identity = (zero_rows, zero_rows, jnp.full_like(start_num, far_below), zero_rows)
    incoming = prefix(
        (element_num, element_den, element_max, device_span), "seq", combine_states, identity, False
    )
    prior_num, prior_den, prior_max = (incoming[0], incoming[1], incoming[2])
    in_num = jnp.where(is_first, start_num, prior_num)
    in_den = jnp.where(is_first, start_den, prior_den)
    in_max = jnp.where(is_first, start_max, prior_max)
    (mixed_rows, state_out), wkv_pull = jax.vjp(
        wkv_local, key_rows, value_rows, time_decay, time_first, in_num, in_den, in_max
    )
    gated, gate_pull = jax.vjp(gate_rows, recept_rows, mixed_rows)
    gated_low = gated.astype(jnp.bfloat16)
    attended = matmul(gated_low, w_output)
    middle = input_rows + attended
    normed_ffn, norm_ffn_pull = jax.vjp(layer_norm, middle, ln2_gain, ln2_bias)
    from_left_ffn = from_behind(normed_ffn[:, -1, :], "seq", 1)
    edge_ffn = jnp.where(is_first, before_ffn, from_left_ffn)
    ffn_inputs, ffn_mix_pull = jax.vjp(
        token_mix, normed_ffn, edge_ffn, (ffn_mix_key, ffn_mix_recept)
    )
    ffn_key_in = ffn_inputs[0].astype(jnp.bfloat16)
    ffn_recept_in = ffn_inputs[1].astype(jnp.bfloat16)
    hidden_pre = matmul(ffn_key_in, w_ffn_key)
    hidden = jnp.square(jax.nn.relu(hidden_pre)).astype(jnp.bfloat16)
    ffn_values = matmul(hidden, w_ffn_value)
    gate_now = jax.nn.sigmoid(matmul(ffn_recept_in, w_ffn_recept))
    block_out = (middle + gate_now * ffn_values).astype(jnp.bfloat16)
    grad_out = cotangent.astype(jnp.float32)
    grad_values = (grad_out * gate_now).astype(jnp.bfloat16)
    grad_gate = (grad_out * ffn_values * gate_now * (1.0 - gate_now)).astype(jnp.bfloat16)
    grad_hidden = matmul_back(grad_values, w_ffn_value)
    grad_pre = (grad_hidden * 2.0 * jax.nn.relu(hidden_pre)).astype(jnp.bfloat16)
    grad_w_ffn_value = outer_sum(hidden, grad_values)
    grad_w_ffn_key = outer_sum(ffn_key_in, grad_pre)
    grad_w_ffn_recept = outer_sum(ffn_recept_in, grad_gate)
    grad_normed_ffn, grad_edge_ffn, ffn_mix_grads = ffn_mix_pull(
        (matmul_back(grad_pre, w_ffn_key), matmul_back(grad_gate, w_ffn_recept))
    )
    from_right_ffn = from_behind(grad_edge_ffn, "seq", -1)
    grad_normed_ffn = grad_normed_ffn.at[:, -1, :].add(from_right_ffn)
    grad_middle, grad_ln2_gain, grad_ln2_bias = norm_ffn_pull(grad_normed_ffn)
    grad_middle = grad_middle + grad_out
    grad_attended = grad_middle.astype(jnp.bfloat16)
    grad_w_output = outer_sum(gated_low, grad_attended)
    grad_recept_full, grad_mixed = gate_pull(matmul_back(grad_attended, w_output))
    grad_recept = grad_recept_full.astype(jnp.bfloat16)
    zero_state = (zero_rows, zero_rows, zero_rows)
    first_pass = wkv_pull((grad_mixed, zero_state))
    unscale = jnp.exp(-in_max)
    local_grad_num = first_pass[4] * unscale
    local_grad_den = first_pass[5] * unscale
    later_grads = prefix(
        (local_grad_num, local_grad_den, device_span),
        "seq",
        combine_grads,
        (zero_rows, zero_rows, zero_rows),
        True,
    )
    exit_num, exit_den = (later_grads[0], later_grads[1])
    out_num, out_den, out_max = state_out
    lifting = jnp.exp(out_max)
    exit_cotangent = (
        exit_num * lifting,
        exit_den * lifting,
        (exit_num * out_num + exit_den * out_den) * lifting,
    )
    second_pass = wkv_pull((jnp.zeros_like(grad_mixed), exit_cotangent))
    grad_key_rows = (first_pass[0] + second_pass[0]).astype(jnp.bfloat16)
    grad_value_rows = (first_pass[1] + second_pass[1]).astype(jnp.bfloat16)
    grad_time_decay = first_pass[2] + second_pass[2]
    grad_time_first = first_pass[3] + second_pass[3]
    grad_start_num = first_pass[4] + second_pass[4]
    grad_start_den = first_pass[5] + second_pass[5]
    grad_start_max = first_pass[6] + second_pass[6]
    grad_w_key = outer_sum(key_in, grad_key_rows)
    grad_w_value = outer_sum(value_in, grad_value_rows)
    grad_w_recept = outer_sum(recept_in, grad_recept)
    grad_normed, grad_edge_att, mix_grads = mix_pull(
        (
            matmul_back(grad_key_rows, w_key),
            matmul_back(grad_value_rows, w_value),
            matmul_back(grad_recept, w_recept),
        )
    )
    from_right = from_behind(grad_edge_att, "seq", -1)
    grad_normed = grad_normed.at[:, -1, :].add(from_right)
    grad_input_ln, grad_ln1_gain, grad_ln1_bias = norm_pull(grad_normed)
    input_grad = (grad_input_ln + grad_middle).astype(jnp.bfloat16)
    start_num_grad = jnp.where(is_first, grad_start_num, 0.0).T
    start_den_grad = jnp.where(is_first, grad_start_den, 0.0).T
    start_max_grad = jnp.where(is_first, grad_start_max, 0.0).T
    edge_att_grad = jnp.where(is_first, grad_edge_att, 0.0).T
    edge_ffn_grad = jnp.where(is_first, grad_edge_ffn, 0.0).T
    row_parts = (
        lax.psum_scatter(grad_w_key, "seq", scatter_dimension=0, tiled=True),
        lax.psum_scatter(grad_w_value, "seq", scatter_dimension=0, tiled=True),
        lax.psum_scatter(grad_w_recept, "seq", scatter_dimension=0, tiled=True),
        lax.psum_scatter(grad_w_output, "seq", scatter_dimension=0, tiled=True),
        lax.psum_scatter(grad_w_ffn_key, "seq", scatter_dimension=0, tiled=True),
        lax.psum_scatter(grad_w_ffn_value, "seq", scatter_dimension=0, tiled=True),
        lax.psum_scatter(grad_w_ffn_recept, "seq", scatter_dimension=0, tiled=True),
        lax.psum_scatter(grad_ln1_gain, "seq", scatter_dimension=0, tiled=True),
        lax.psum_scatter(grad_ln1_bias, "seq", scatter_dimension=0, tiled=True),
        lax.psum_scatter(mix_grads[0], "seq", scatter_dimension=0, tiled=True),
        lax.psum_scatter(mix_grads[1], "seq", scatter_dimension=0, tiled=True),
        lax.psum_scatter(mix_grads[2], "seq", scatter_dimension=0, tiled=True),
        lax.psum_scatter(grad_time_decay, "seq", scatter_dimension=0, tiled=True),
        lax.psum_scatter(grad_time_first, "seq", scatter_dimension=0, tiled=True),
        lax.psum_scatter(grad_ln2_gain, "seq", scatter_dimension=0, tiled=True),
        lax.psum_scatter(grad_ln2_bias, "seq", scatter_dimension=0, tiled=True),
        lax.psum_scatter(ffn_mix_grads[0], "seq", scatter_dimension=0, tiled=True),
        lax.psum_scatter(ffn_mix_grads[1], "seq", scatter_dimension=0, tiled=True),
        lax.psum_scatter(start_num_grad, "seq", scatter_dimension=0, tiled=True),
        lax.psum_scatter(start_den_grad, "seq", scatter_dimension=0, tiled=True),
        lax.psum_scatter(start_max_grad, "seq", scatter_dimension=0, tiled=True),
        lax.psum_scatter(edge_att_grad, "seq", scatter_dimension=0, tiled=True),
        lax.psum_scatter(edge_ffn_grad, "seq", scatter_dimension=0, tiled=True),
    )
    matrix_parts = (
        lax.psum_scatter(row_parts[0], "batch", scatter_dimension=1, tiled=True),
        lax.psum_scatter(row_parts[1], "batch", scatter_dimension=1, tiled=True),
        lax.psum_scatter(row_parts[2], "batch", scatter_dimension=1, tiled=True),
        lax.psum_scatter(row_parts[3], "batch", scatter_dimension=1, tiled=True),
        lax.psum_scatter(row_parts[4], "batch", scatter_dimension=1, tiled=True),
        lax.psum_scatter(row_parts[5], "batch", scatter_dimension=1, tiled=True),
        lax.psum_scatter(row_parts[6], "batch", scatter_dimension=1, tiled=True),
    )
    vector_parts = lax.psum(
        (
            row_parts[7],
            row_parts[8],
            row_parts[9],
            row_parts[10],
            row_parts[11],
            row_parts[12],
            row_parts[13],
            row_parts[14],
            row_parts[15],
            row_parts[16],
            row_parts[17],
        ),
        "batch",
    )
    start_parts = (row_parts[18], row_parts[19], row_parts[20], row_parts[21], row_parts[22])
    return (
        block_out,
        input_grad,
        matrix_parts[0],
        matrix_parts[1],
        matrix_parts[2],
        matrix_parts[3],
        matrix_parts[4],
        matrix_parts[5],
        matrix_parts[6],
        vector_parts[0],
        vector_parts[1],
        vector_parts[2],
        vector_parts[3],
        vector_parts[4],
        vector_parts[5],
        vector_parts[6],
        vector_parts[7],
        vector_parts[8],
        vector_parts[9],
        vector_parts[10],
        start_parts[0],
        start_parts[1],
        start_parts[2],
        start_parts[3],
        start_parts[4],
    )


def solution(mesh):
    placed = (
        P("batch", "seq", None),
        P(),
        P(),
        P(),
        P(),
        P(),
        P(),
        P(),
        P(),
        P(),
        P(),
        P(),
        P(),
        P(),
        P(),
        P(),
        P(),
        P(),
        P(),
        P(None, "batch"),
        P(None, "batch"),
        P(None, "batch"),
        P(None, "batch"),
        P(None, "batch"),
        P("batch", "seq", None),
    )
    return jax.shard_map(
        local if fits(mesh) else local_plain,
        mesh=mesh,
        in_specs=placed,
        out_specs=(
            P("batch", "seq", None),
            P("batch", "seq", None),
            P("seq", "batch"),
            P("seq", "batch"),
            P("seq", "batch"),
            P("seq", "batch"),
            P("seq", "batch"),
            P("seq", "batch"),
            P("seq", "batch"),
            P("seq"),
            P("seq"),
            P("seq"),
            P("seq"),
            P("seq"),
            P("seq"),
            P("seq"),
            P("seq"),
            P("seq"),
            P("seq"),
            P("seq"),
            P("seq", "batch"),
            P("seq", "batch"),
            P("seq", "batch"),
            P("seq", "batch"),
            P("seq", "batch"),
        ),
        check_vma=False,
    )
```
